128 devices in a mesh: row: 4 (over y), col: 4 (over z), depth: 8 (over x, core).
Axes of the slice: x: 4, y: 4, z: 4, core: 2. Of those that a mesh axis runs over, the one named last changes fastest.
Arguments:
- diag_block: float32 [512, 512], P(('row', 'col', 'depth')), as said below
- panel_rows: float32 [32256, 512], P(('row', 'col', 'depth')), may hold values from -2 to 2
- trailing: float32 [32256, 1024], P(('row', 'depth'), 'col'), may hold values from -6 to 6
Outputs:
- diag_factor: float32 [512, 512], P(('row', 'col', 'depth'))
- panel_factor: float32 [32256, 512], P(('row', 'col', 'depth'))
- updated: float32 [32256, 1024], P(('row', 'depth'), 'col')
The draws below stay inside these ranges and needn't reach their ends.
Inputs may be any that keep to these rules, and one draw needn't show every extreme that they name: `diag_block`: symmetric positive definite.
All inputs are finite; a program needn't handle non-finite values.
Results may differ from the reference program's by a relative error of at most 0.000062.
Values sent between devices are 32-bit elements; how exact they have to be, the bound alone decides.
A program may use at most 64 MiB of HBM per device.

```python
import math
import jax
import jax.numpy as jnp
from jax import lax

PANEL = 512
WIN = 1024
TRAIL = 32256


def draw_diag_block(key, part):
    first = jax.random.fold_in(key, 11)
    second = jax.random.fold_in(key, 12)
    noise = jax.random.normal(first, (PANEL, PANEL), jnp.float32)
    sym = (noise + noise.T) / math.sqrt(2.0 * PANEL)
    shift = jax.random.uniform(second, (PANEL,), jnp.float32, 3.0, 6.0)
    matrix = sym + jnp.diag(shift)
    return matrix


def block_scale(own_key, dims, shards, low, high):
    factor_of = 1.0
    for position, shards_of in shards:
        draws = jax.random.uniform(jax.random.fold_in(jax.random.fold_in(own_key, 6), position), (shards_of,), jnp.float32, low / len(shards), high / len(shards))
        factor_of = factor_of * jnp.repeat(jnp.exp(draws), dims[position] // shards_of).reshape((-1,) + (1,) * (len(dims) - 1 - position))
    return factor_of


def scatter_about(own_key, extent, scale, reach, shards=(), kind=jnp.bfloat16):
    gain = block_scale(own_key, extent, shards, -0.22, 0.18) if shards else 1.0
    result = jax.random.normal(own_key, extent, jnp.float32) * scale * gain
    return jnp.minimum(jnp.maximum(result, -reach), reach).astype(kind)


def setup_inputs(seed: int = 0) -> dict:
    seeds = jax.random.split(jax.random.key(seed), 4)
    diag_block = draw_diag_block(jax.random.fold_in(seeds[3], 71), 0)
    panel_rows = scatter_about(seeds[1], (TRAIL, PANEL), 0.25, 2.0, ((0, 128),), jnp.float32)
    trailing = scatter_about(seeds[2], (TRAIL, WIN), 1.0, 6.0, ((0, 32), (1, 4)), jnp.float32)
    return {"diag_block": diag_block, "panel_rows": panel_rows, "trailing": trailing}


def reference(diag_block, panel_rows, trailing):
    diag_factor = jnp.linalg.cholesky(diag_block)
    panel_factor = jax.scipy.linalg.solve_triangular(diag_factor, panel_rows.T, lower=True).T
    window = panel_factor[:trailing.shape[1]]
    product = lax.dot_general(panel_factor.astype(jnp.float32), window.astype(jnp.float32), (((1,), (1,)), ((), ())), precision=lax.Precision.HIGHEST, preferred_element_type=jnp.float32)
    return (diag_factor, panel_factor, trailing - product)
```

```python
import jax
import jax.numpy as jnp
from jax import lax
from jax.experimental import pallas as pl
from jax.experimental.pallas import tpu as pltpu
from jax.sharding import Mesh
from jax.sharding import PartitionSpec as P

DEPTH = ("depth_0", "depth_1")
ROW_COL_DEPTH = ("row", "col", "depth_0", "depth_1")
ROW_DEPTH = ("row", "depth_0", "depth_1")


F32 = jnp.float32
NT = (((1,), (1,)), ((), ()))
BLOCK = 128


def lane(v, j):
    return jnp.broadcast_to(v[:, j : j + 1], (8, 128))


def sub(v, k):
    return jnp.broadcast_to(v[k : k + 1, :], (8, 128))


def split(x):
    hi = x.astype(jnp.bfloat16)
    return hi, (x - hi.astype(F32)).astype(jnp.bfloat16)


def dot(a, b):
    def one(x, y):
        return lax.dot_general(x, y, NT, preferred_element_type=F32)

    return one(a[0], b[0]) + (one(a[0], b[1]) + one(a[1], b[0]))


def factor_block(rows):
    ri = lax.broadcasted_iota(jnp.int32, (8, 128), 0)
    li = lax.broadcasted_iota(jnp.int32, (8, 128), 1)
    rows = list(rows)
    unit = [jnp.where(li == ri + 8 * v, 1.0, 0.0).astype(F32) for v in range(16)]
    upper, inverse = [], []
    for p in range(16):
        n = 16 - p
        cols = [[lane(rows[p + v], 8 * p + j) for j in range(8)] for v in range(n)]
        r = [sub(rows[p], k) for k in range(8)]
        s = [sub(unit[p], k) for k in range(8)]
        for k in range(8):
            inv = lax.rsqrt(sub(cols[0][k], k))
            for v in range(n):
                cols[v][k] = cols[v][k] * inv
            r[k] = r[k] * inv
            s[k] = s[k] * inv
            for j in range(k + 1, 8):
                m = sub(cols[0][k], j)
                for v in range(n):
                    cols[v][j] = cols[v][j] - cols[v][k] * m
                r[j] = r[j] - m * r[k]
                s[j] = s[j] - m * s[k]
        u, t = r[0], s[0]
        for k in range(1, 8):
            u = jnp.where(ri == k, r[k], u)
            t = jnp.where(ri == k, s[k], t)
        upper.append(jnp.where(li >= ri + 8 * p, u, 0.0))
        inverse.append(t)
        for v in range(1, n):
            for k in range(8):
                rows[p + v] = rows[p + v] - cols[v][k] * r[k]
                unit[p + v] = unit[p + v] - cols[v][k] * s[k]
    return upper, inverse


def at(i):
    return slice(BLOCK * i, BLOCK * (i + 1))


def factor_all(a_ref, l_ref, s_ref, lows, invs):
    n = 4
    for k in range(n):
        src = a_ref if k == 0 else s_ref
        upper, inverse = factor_block(
            [src[BLOCK * k + 8 * v : BLOCK * k + 8 * v + 8, at(k)] for v in range(16)]
        )
        invs[k] = split(jnp.concatenate(inverse, 0))
        l_ref[at(k), at(k)] = jnp.concatenate(upper, 0).T
        for j in range(k + 1, n):
            l_ref[at(k), at(j)] = jnp.zeros((BLOCK, BLOCK), F32)
        for i in range(k + 1, n):
            low = dot(split(src[at(i), at(k)]), invs[k])
            l_ref[at(i), at(k)] = low
            lows[i, k] = split(low)
        for i in range(k + 1, n):
            for j in range(k + 1, i + 1):
                s_ref[at(i), at(j)] = src[at(i), at(j)] - dot(lows[i, k], lows[j, k])


def solve(x, lows, invs):
    done = []
    for k in range(4):
        acc = x[:, at(k)]
        for m in range(k):
            acc = acc - dot(done[m][1], lows[k, m])
        value = dot(split(acc), invs[k])
        done.append((value, split(value)))
    return done


def product(a, b):
    total = dot(a[0][1], b[0][1])
    for k in range(1, 4):
        total = total + dot(a[k][1], b[k][1])
    return total


def compute(diag, own, rows, window, trailing, own_l, solved, updated, l_ref, s_ref):
    lows, invs = {}, {}
    factor_all(diag, l_ref, s_ref, lows, invs)
    position = lax.axis_index("row") * 32 + lax.axis_index("col") * 8 + lax.axis_index(DEPTH)
    pair = l_ref[pl.ds(pl.multiple_of((position // 2) * 8, 8), 8), :]
    own_l[...] = jnp.where(position % 2 == 0, pair[0:4], pair[4:8])
    w = solve(window[...], lows, invs)
    for k, (value, _) in enumerate(solve(own[...], lows, invs)):
        solved[:, at(k)] = value
    size = own.shape[0]
    for j in range(4):
        span = slice(size * j, size * (j + 1))
        x = solve(rows[span, :], lows, invs)
        updated[span, :] = trailing[span, :] - product(x, w)


def all_compute(diag, own, rows, window, trailing):
    spec = pl.BlockSpec(memory_space=pltpu.VMEM)
    return pl.pallas_call(
        compute,
        out_shape=(
            jax.ShapeDtypeStruct((4, 512), F32),
            jax.ShapeDtypeStruct(own.shape, F32),
            jax.ShapeDtypeStruct(trailing.shape, F32),
        ),
        in_specs=[spec] * 5,
        out_specs=(spec,) * 3,
        scratch_shapes=[pltpu.VMEM((512, 512), F32), pltpu.VMEM((512, 512), F32)],
        compiler_params=pltpu.CompilerParams(vmem_limit_bytes=48 * 2**20),
        name="factor_solve_update",
    )(diag, own, rows, window, trailing)


def sent_to_all(value, axis):
    copies = jnp.broadcast_to(value, (lax.axis_size(axis), *value.shape))
    return lax.all_to_all(copies, axis, split_axis=0, concat_axis=0, tiled=True)


def in_order(tiles, dim):
    shape = list(tiles.shape[1:])
    shape[dim] *= tiles.shape[0]
    return jnp.moveaxis(tiles, 0, dim).reshape(shape)


def gather_directly(value, axis, dim):
    tiles = sent_to_all(value, axis)
    return in_order(tiles, dim)


def broadcast(value, axis, root):
    return lax.dynamic_index_in_dim(lax.all_gather(value, axis), root, 0, keepdims=False)


def gather_axes(value, axes, dim):
    far, near = axes
    tiles = sent_to_all(sent_to_all(value, far), near)
    return in_order(tiles.swapaxes(0, 1).reshape(-1, *value.shape), dim)


def gathered_by_axis(value, axes, dim):
    if not axes:
        return value
    nearer = lax.all_gather(value, axes[-1], axis=dim, tiled=True)
    return gathered_by_axis(nearer, axes[:-1], dim)


def split_panel(solved, win_rows):
    ranges = lax.all_to_all(solved, DEPTH, split_axis=1, concat_axis=0, tiled=True)
    row_panel = gather_directly(ranges, "col", 0)
    local_window = lax.dynamic_slice_in_dim(
        row_panel, lax.axis_index("col") * win_rows, win_rows, 0
    )
    window = broadcast(local_window, "row", 0)
    return (row_panel, window)


def body(diag_block, panel_rows, trailing):
    whole_diag = gather_axes(diag_block, (("row", "col", "depth_0"), "depth_1"), 0)
    row_panel, window = split_panel(panel_rows, trailing.shape[1])
    owned = lax.all_to_all(row_panel, DEPTH, split_axis=0, concat_axis=1, tiled=True)
    full_window = gathered_by_axis(window, DEPTH, 1)
    return all_compute(whole_diag, panel_rows, owned, full_window, trailing)


def solution(mesh):
    split = Mesh(
        mesh.devices.reshape(mesh.shape["row"], mesh.shape["col"], 4, 2),
        ("row", "col", "depth_0", "depth_1"),
    )
    return jax.shard_map(
        body,
        mesh=split,
        in_specs=(P(ROW_COL_DEPTH, None), P(ROW_COL_DEPTH, None), P(ROW_DEPTH, "col")),
        out_specs=(P(ROW_COL_DEPTH, None), P(ROW_COL_DEPTH, None), P(ROW_DEPTH, "col")),
        check_vma=False,
    )
```

```python
import jax
import jax.numpy as jnp
from jax import lax
from jax.experimental import pallas as pl
from jax.experimental.pallas import tpu as pltpu
from jax.sharding import PartitionSpec as P

ALL = ("row", "col", "depth")

F32 = jnp.float32
NT = (((1,), (1,)), ((), ()))
BLOCK = 128


def lane(v, j):
    return jnp.broadcast_to(v[:, j : j + 1], (8, 128))


def sub(v, k):
    return jnp.broadcast_to(v[k : k + 1, :], (8, 128))


def split(x):
    hi = x.astype(jnp.bfloat16)
    return hi, (x - hi.astype(F32)).astype(jnp.bfloat16)


def dot(a, b):
    def one(x, y):
        return lax.dot_general(x, y, NT, preferred_element_type=F32)

    return one(a[0], b[0]) + (one(a[0], b[1]) + one(a[1], b[0]))


def factor_block(rows):
    ri = lax.broadcasted_iota(jnp.int32, (8, 128), 0)
    li = lax.broadcasted_iota(jnp.int32, (8, 128), 1)
    rows = list(rows)
    unit = [jnp.where(li == ri + 8 * v, 1.0, 0.0).astype(F32) for v in range(16)]
    upper, inverse = [], []
    for p in range(16):
        n = 16 - p
        cols = [[lane(rows[p + v], 8 * p + j) for j in range(8)] for v in range(n)]
        r = [sub(rows[p], k) for k in range(8)]
        s = [sub(unit[p], k) for k in range(8)]
        for k in range(8):
            inv = lax.rsqrt(sub(cols[0][k], k))
            for v in range(n):
                cols[v][k] = cols[v][k] * inv
            r[k] = r[k] * inv
            s[k] = s[k] * inv
            for j in range(k + 1, 8):
                m = sub(cols[0][k], j)
                for v in range(n):
                    cols[v][j] = cols[v][j] - cols[v][k] * m
                r[j] = r[j] - m * r[k]
                s[j] = s[j] - m * s[k]
        u, t = r[0], s[0]
        for k in range(1, 8):
            u = jnp.where(ri == k, r[k], u)
            t = jnp.where(ri == k, s[k], t)
        upper.append(jnp.where(li >= ri + 8 * p, u, 0.0))
        inverse.append(t)
        for v in range(1, n):
            for k in range(8):
                rows[p + v] = rows[p + v] - cols[v][k] * r[k]
                unit[p + v] = unit[p + v] - cols[v][k] * s[k]
    return upper, inverse


def at(i):
    return slice(BLOCK * i, BLOCK * (i + 1))


def factor_all(a_ref, l_ref, s_ref, lows, invs):
    n = 4
    for k in range(n):
        src = a_ref if k == 0 else s_ref
        upper, inverse = factor_block(
            [src[BLOCK * k + 8 * v : BLOCK * k + 8 * v + 8, at(k)] for v in range(16)]
        )
        invs[k] = split(jnp.concatenate(inverse, 0))
        l_ref[at(k), at(k)] = jnp.concatenate(upper, 0).T
        for j in range(k + 1, n):
            l_ref[at(k), at(j)] = jnp.zeros((BLOCK, BLOCK), F32)
        for i in range(k + 1, n):
            low = dot(split(src[at(i), at(k)]), invs[k])
            l_ref[at(i), at(k)] = low
            lows[i, k] = split(low)
        for i in range(k + 1, n):
            for j in range(k + 1, i + 1):
                s_ref[at(i), at(j)] = src[at(i), at(j)] - dot(lows[i, k], lows[j, k])


def solve(x, lows, invs):
    done = []
    for k in range(4):
        acc = x[:, at(k)]
        for m in range(k):
            acc = acc - dot(done[m][1], lows[k, m])
        value = dot(split(acc), invs[k])
        done.append((value, split(value)))
    return done


def product(a, b):
    total = dot(a[0][1], b[0][1])
    for k in range(1, 4):
        total = total + dot(a[k][1], b[k][1])
    return total


def compute(dbuf, own, rows, win, trailing, own_l, solved, updated, diag, window, l_ref, s_ref):
    for p in range(128):
        diag[4 * p : 4 * p + 4, :] = dbuf[p]
    for s in range(8):
        for r in range(4):
            for u in range(2):
                first = 32 * s + 8 * r + 4 * u
                window[first : first + 4, :] = win[s, r, u]
    lows, invs = {}, {}
    factor_all(diag, l_ref, s_ref, lows, invs)
    position = (lax.axis_index("row") * 4 + lax.axis_index("col")) * 8 + lax.axis_index("depth")
    pair = l_ref[pl.ds(pl.multiple_of((position // 2) * 8, 8), 8), :]
    own_l[...] = jnp.where(position % 2 == 0, pair[0:4], pair[4:8])
    w = solve(window[...], lows, invs)
    for k, (value, _) in enumerate(solve(own[...], lows, invs)):
        solved[:, at(k)] = value
    size = own.shape[0]
    for j in range(4):
        span = slice(size * j, size * (j + 1))
        x = solve(rows[j], lows, invs)
        updated[span, :] = trailing[span, :] - product(x, w)


def all_compute(dbuf, own, rows, win, trailing):
    spec = pl.BlockSpec(memory_space=pltpu.VMEM)
    return pl.pallas_call(
        compute,
        out_shape=(
            jax.ShapeDtypeStruct((4, 512), F32),
            jax.ShapeDtypeStruct(own.shape, F32),
            jax.ShapeDtypeStruct(trailing.shape, F32),
        ),
        in_specs=[spec] * 5,
        out_specs=(spec,) * 3,
        scratch_shapes=[
            pltpu.VMEM((512, 512), F32),
            pltpu.VMEM((256, 512), F32),
            pltpu.VMEM((512, 512), F32),
            pltpu.VMEM((512, 512), F32),
        ],
        compiler_params=pltpu.CompilerParams(vmem_limit_bytes=36 * 2**20),
        name="factor_solve_update",
    )(dbuf, own, rows, win, trailing)


def remote(src, dst, send, recv, **device):
    return pltpu.make_async_remote_copy(
        src_ref=src,
        dst_ref=dst,
        send_sem=send,
        recv_sem=recv,
        device_id=device,
        device_id_type=pl.DeviceIdType.MESH,
    )


class Exchange:
    def __init__(self, diag, panel, dbuf, relay, rows, win, wsrc, pw, q, sems):
        self.diag, self.panel, self.dbuf, self.relay, self.rows = diag, panel, dbuf, relay, rows
        self.win, self.wsrc, self.pw, self.q = win, wsrc, pw, q
        (self.loc, self.ds, self.dr, self.cs, self.cr, self.rs, self.rr, self.zs, self.zr, self.xs, self.xr,
         self.w1s, self.w1r, self.w2s, self.w2r, self.w3s, self.w3r, self.w4s, self.w4r, self.w5s, self.w5r) = sems
        self.r, self.c, self.s = (lax.axis_index(a) for a in ("row", "col", "depth"))
        self.pos = (self.r * 4 + self.c) * 8 + self.s
        self.corner = jnp.logical_and(self.r == 0, self.c == 0)

    def enter(self):
        r, c, s = self.r, self.c, self.s
        self.own_diag = pltpu.make_async_copy(self.diag, self.dbuf.at[self.pos], self.loc.at[0])
        self.own_panel = pltpu.make_async_copy(self.panel, self.relay.at[c], self.loc.at[1])
        self.own_diag.start()
        self.own_panel.start()
        barrier = pltpu.get_barrier_semaphore()
        for axis, me, n in (("depth", s, 8), ("col", c, 4), ("row", r, 4)):
            for t in range(1, n):
                pl.semaphore_signal(
                    barrier, inc=1, device_id={axis: (me + t) % n}, device_id_type=pl.DeviceIdType.MESH
                )
        pl.semaphore_wait(barrier, 13)
        self.own_diag.wait()

    def diag_depth(self, t, pos):
        ref = self.dbuf.at[pos]
        return remote(ref, ref, self.ds.at[t], self.dr.at[t], depth=(self.s + t) % 8)

    def diag_depth_send(self):
        for t in range(1, 8):
            self.diag_depth(t, self.pos).start()

    def diag_depth_wait(self):
        for t in range(1, 8):
            self.diag_depth(t, (self.r * 4 + self.c) * 8 + (self.s - t) % 8).wait_recv()

    def diag_col(self, t, c, i):
        ref = self.dbuf.at[pl.ds(32 * i + 8 * c, 8), :, 0 : 128 * (i + 1)]
        return remote(ref, ref, self.cs.at[t], self.cr.at[t], col=(self.c + t) % 4)

    def diag_col_send(self):
        for i in range(4):

            @pl.when(self.r == i)
            def _():
                for t in range(1, 4):
                    self.diag_col(t, self.c, i).start()

    def diag_col_wait(self):
        for i in range(4):

            @pl.when(self.r == i)
            def _():
                for t in range(1, 4):
                    self.diag_col(t, (self.c - t) % 4, i).wait_recv()

    def diag_row(self, t, i):
        ref = self.dbuf.at[32 * i : 32 * i + 32, :, 0 : 128 * (i + 1)]
        return remote(ref, ref, self.rs.at[t], self.rr.at[t], row=(self.r + t) % 4)

    def diag_row_send(self):
        for i in range(4):

            @pl.when(self.r == i)
            def _():
                for t in range(1, 4):
                    self.diag_row(t, i).start()

    def diag_row_wait(self, src):
        for i in range(4):
            if i != src:

                @pl.when(self.r == i)
                def _():
                    self.diag_row((i - src) % 4, src).wait_recv()

    def rows_col(self, k, slot, step, part):
        ref = self.relay.at[slot]
        if part is not None:
            ref = self.relay.at[slot, :, 256 * part : 256 * part + 256]
        return remote(ref, ref, self.zs.at[k], self.zr.at[k], col=(self.c + step) % 4)

    def rows_col_send(self):
        self.rows_col(0, self.c, 1, None).start()
        self.rows_col(1, self.c, 3, None).start()

    def rows_col_pass(self, k):
        step = (1, 3)[k]
        slot = (self.c - step) % 4
        self.rows_col(k, slot, step, None).wait_recv()
        self.rows_col(2 + k, slot, step, k).start()
        self.rows_depth_send(1 + k, slot)

    def rows_col_last(self):
        slot = (self.c + 2) % 4
        self.rows_col(2, slot, 1, 0).wait_recv()
        self.rows_col(3, slot, 3, 1).wait_recv()
        self.rows_depth_send(3, slot)

    def rows_depth(self, k, slot):
        target = 2 * slot + self.s // 4
        return target, remote(
            self.relay.at[slot], self.rows.at[self.s % 4], self.xs.at[k], self.xr.at[self.s % 4], depth=target
        )

    def rows_depth_send(self, k, slot):
        target, copy = self.rows_depth(k, slot)

        @pl.when(target != self.s)
        def _():
            copy.start()

        @pl.when(target == self.s)
        def _():
            self.rows[self.s % 4] = self.relay[slot]

    def rows_wait(self, j):
        source = 4 * (self.s % 2) + j

        @pl.when(source != self.s)
        def _():
            remote(
                self.relay.at[0], self.rows.at[j], self.xs.at[0], self.xr.at[j], depth=source
            ).wait_recv()

    def win_main(self, i, d):
        n = 8 if d < 7 else 7 - i
        return remote(
            self.wsrc.at[i + 8 * d : i + 8 * d + n], self.pw.at[i, 0:n], self.w1s.at[d], self.w1r.at[i], depth=d
        )

    def win_head(self, c):
        return remote(self.wsrc.at[0 : c + 1], self.pw.at[c, 7 - c : 8], self.w1s.at[8], self.w1r.at[4 + c], depth=7)

    def win_scatter(self, act):
        for i in range(5):

            @pl.when(jnp.logical_and(self.corner, self.s == i))
            def _():
                if i < 4:
                    for d in range(8):
                        if d != i:
                            act(self.win_main(i, d))
                if i > 0:
                    act(self.win_head(i - 1))

    def win_scatter_send(self):
        self.own_panel.wait()

        @pl.when(jnp.logical_and(self.corner, self.s < 5))
        def _():
            for u in range(63):
                self.wsrc[u] = self.relay[0, 4 * u : 4 * u + 4, :]

        for i in range(4):

            @pl.when(jnp.logical_and(self.corner, self.s == i))
            def _():
                self.pw[i] = self.wsrc[9 * i : 9 * i + 8]

        self.win_scatter(lambda copy: copy.start())

    def win_scatter_wait(self):
        for d in range(8):

            @pl.when(jnp.logical_and(self.corner, self.s == d))
            def _():
                for i in range(4):
                    if d != i:
                        self.win_main(i, d).wait_recv()
                    if d == 7:
                        self.win_head(i).wait_recv()

    def win_col(self, t):
        return remote(self.pw.at[t], self.q, self.w2s.at[t], self.w2r.at[0], col=t)

    def win_col_send(self):
        @pl.when(self.corner)
        def _():
            for t in range(1, 4):
                self.win_col(t).start()
            self.q[...] = self.pw[0]

    def win_col_wait(self):
        @pl.when(jnp.logical_and(self.r == 0, self.c != 0))
        def _():
            self.win_col(1).wait_recv()

    def win_row(self, t, row):
        return remote(
            self.q.at[2 * t : 2 * t + 2], self.win.at[self.s, row], self.w3s.at[t], self.w3r.at[0], row=t
        )

    def win_row_send(self):
        @pl.when(self.r == 0)
        def _():
            for t in range(1, 4):
                self.win_row(t, t).start()
            self.win[self.s, 0] = self.q[0:2]

    def win_row_wait(self):
        @pl.when(self.r != 0)
        def _():
            self.win_row(1, self.r).wait_recv()

    def win_depth(self, t, d):
        ref = self.win.at[d, self.r]
        return remote(ref, ref, self.w4s.at[t], self.w4r.at[t], depth=(self.s + t) % 8)

    def win_depth_send(self):
        for t in range(1, 8):
            self.win_depth(t, self.s).start()

    def win_depth_wait(self):
        for t in range(1, 8):
            self.win_depth(t, (self.s - t) % 8).wait_recv()

    def win_all(self, t, row):
        ref = self.win.at[:, row]
        return remote(ref, ref, self.w5s.at[t], self.w5r.at[t], row=(self.r + t) % 4)

    def win_all_send(self):
        for t in range(1, 4):
            self.win_all(t, self.r).start()

    def win_all_wait(self):
        for t in range(1, 4):
            self.win_all(t, (self.r - t) % 4).wait_recv()

    def leave(self):
        for t in range(1, 8):
            self.diag_depth(t, self.pos).wait_send()
            self.win_depth(t, self.s).wait_send()
        for i in range(4):

            @pl.when(self.r == i)
            def _():
                for t in range(1, 4):
                    self.diag_col(t, self.c, i).wait_send()
                    self.diag_row(t, i).wait_send()

        for t in range(1, 4):
            self.win_all(t, self.r).wait_send()
        for k in range(2):
            step = (1, 3)[k]
            self.rows_col(k, self.c, step, None).wait_send()
            self.rows_col(2 + k, (self.c - step) % 4, step, k).wait_send()
        for k, slot in enumerate((self.c, (self.c + 3) % 4, (self.c + 1) % 4, (self.c + 2) % 4)):
            target, copy = self.rows_depth(k, slot)

            @pl.when(target != self.s)
            def _():
                copy.wait_send()

        self.win_scatter(lambda copy: copy.wait_send())

        @pl.when(self.corner)
        def _():
            for t in range(1, 4):
                self.win_col(t).wait_send()

        @pl.when(self.r == 0)
        def _():
            for t in range(1, 4):
                self.win_row(t, t).wait_send()


SEMAPHORES = (2, 8, 8, 4, 4, 4, 4, 4, 4, 4, 4, 9, 8, 4, 1, 4, 1, 8, 8, 4, 4)


def exchange(diag, panel, dbuf, rows, win, relay, wsrc, pw, q, *sems):
    e = Exchange(diag, panel, dbuf, relay, rows, win, wsrc, pw, q, sems)
    e.enter()
    e.diag_depth_send()
    e.win_scatter_send()
    e.diag_depth_wait()
    e.diag_col_send()
    e.rows_col_send()
    e.rows_depth_send(0, e.c)
    e.win_scatter_wait()
    e.win_col_send()
    e.diag_col_wait()
    e.diag_row_send()
    e.win_col_wait()
    e.win_row_send()
    e.win_row_wait()
    e.win_depth_send()
    for i in range(4):
        e.diag_row_wait(i)
    e.rows_col_pass(0)
    e.rows_col_pass(1)
    e.win_depth_wait()
    e.win_all_send()
    e.rows_col_last()
    e.win_all_wait()
    for j in range(4):
        e.rows_wait(j)
    e.leave()


def all_exchange(diag, panel):
    vmem = pl.BlockSpec(memory_space=pltpu.VMEM)
    hbm = pl.BlockSpec(memory_space=pltpu.HBM)
    return pl.pallas_call(
        exchange,
        out_shape=(
            jax.ShapeDtypeStruct((128, 4, 512), F32),
            jax.ShapeDtypeStruct((4, *panel.shape), F32),
            jax.ShapeDtypeStruct((8, 4, 2, 4, 512), F32),
        ),
        in_specs=[hbm, hbm],
        out_specs=(vmem,) * 3,
        scratch_shapes=[
            pltpu.VMEM((4, *panel.shape), F32),
            pltpu.VMEM((63, 4, 512), F32),
            pltpu.VMEM((4, 8, 4, 512), F32),
            pltpu.VMEM((8, 4, 512), F32),
        ]
        + [pltpu.SemaphoreType.DMA((n,)) for n in SEMAPHORES],
        compiler_params=pltpu.CompilerParams(
            collective_id=0, has_side_effects=True, vmem_limit_bytes=24 * 2**20
        ),
        name="exchange",
    )(diag, panel)


def body(diag_block, panel_rows, trailing):
    dbuf, rows, win = all_exchange(diag_block, panel_rows)
    return all_compute(dbuf, panel_rows, rows, win, trailing)


def solution(mesh):
    specs = (P(ALL, None), P(ALL, None), P(("row", "depth"), "col"))
    return jax.shard_map(body, mesh=mesh, in_specs=specs, out_specs=specs, check_vma=False)
```

```python
import jax
import jax.numpy as jnp
from jax import lax
from jax.experimental import pallas as pl
from jax.experimental.pallas import tpu as pltpu
from jax.sharding import PartitionSpec as P

ALL = ("row", "col", "depth")
F32 = jnp.float32
NT = (((1,), (1,)), ((), ()))
BLOCK = 128
MESH = pl.DeviceIdType.MESH


def at(i):
    return slice(BLOCK * i, BLOCK * (i + 1))


def split(x):
    hi = x.astype(jnp.bfloat16)
    return hi, (x - hi.astype(F32)).astype(jnp.bfloat16)


def dot(a, b):
    def one(x, y):
        return lax.dot_general(x, y, NT, preferred_element_type=F32)

    return one(a[0], b[0]) + (one(a[0], b[1]) + one(a[1], b[0]))


def sub(v, k):
    return jnp.broadcast_to(v[k : k + 1, :], (8, 128))


class Block:
    def __init__(self, rows):
        self.ri = lax.broadcasted_iota(jnp.int32, (8, 128), 0)
        self.li = lax.broadcasted_iota(jnp.int32, (8, 128), 1)
        self.rows = rows
        self.unit = jnp.stack([jnp.where(self.li == self.ri + 8 * v, 1.0, 0.0).astype(F32) for v in range(16)])
        self.upper, self.inverse = [], []

    def advance(self, panels):
        ri, li = self.ri, self.li
        for p in panels:
            rows, unit = self.rows, self.unit
            cols = [jnp.broadcast_to(rows[:, :, 8 * p + j : 8 * p + j + 1], rows.shape) for j in range(8)]
            r = [sub(rows[0], k) for k in range(8)]
            s = [sub(unit[0], k) for k in range(8)]
            for k in range(8):
                inv = lax.rsqrt(sub(cols[k][0], k))
                cols[k] = cols[k] * inv
                r[k] = r[k] * inv
                s[k] = s[k] * inv
                for j in range(k + 1, 8):
                    m = sub(cols[k][0], j)
                    cols[j] = cols[j] - cols[k] * m
                    r[j] = r[j] - m * r[k]
                    s[j] = s[j] - m * s[k]
            u, t = r[0], s[0]
            for k in range(1, 8):
                u = jnp.where(ri == k, r[k], u)
                t = jnp.where(ri == k, s[k], t)
            self.upper.append(jnp.where(li >= ri + 8 * p, u, 0.0))
            self.inverse.append(t)
            if p < 15:
                rows, unit = rows[1:], unit[1:]
                for k in range(8):
                    rows = rows - cols[k][1:] * r[k]
                    unit = unit - cols[k][1:] * s[k]
                self.rows, self.unit = rows, unit


class Factor:
    def __init__(self, a, l, schur):
        self.a, self.l, self.schur = a, l, schur
        self.lows, self.invs = {}, {}

    def block(self, k, between=lambda: None):
        src = self.a if k == 0 else self.schur
        b = Block(jnp.stack([src[BLOCK * k + 8 * v : BLOCK * k + 8 * v + 8, at(k)] for v in range(16)]))
        b.advance(range(8))
        between()
        b.advance(range(8, 16))
        self.invs[k] = split(jnp.concatenate(b.inverse, 0))
        self.l[at(k), at(k)] = jnp.concatenate(b.upper, 0).T
        for j in range(k + 1, 4):
            self.l[at(k), at(j)] = jnp.zeros((BLOCK, BLOCK), F32)

    def rest(self, k):
        src = self.a if k == 0 else self.schur
        for i in range(k + 1, 4):
            low = dot(split(src[at(i), at(k)]), self.invs[k])
            self.l[at(i), at(k)] = low
            self.lows[i, k] = split(low)
        for j in range(k + 1, 4):
            for i in range(j, 4):
                self.schur[at(i), at(j)] = src[at(i), at(j)] - dot(self.lows[i, k], self.lows[j, k])

    def solve_block(self, x, k, done):
        for m in range(k):
            x = x - dot(done[m][1], self.lows[k, m])
        value = dot(split(x), self.invs[k])
        done.append((value, split(value)))


def remote(src, dst, send, recv, **device):
    return pltpu.make_async_remote_copy(
        src_ref=src, dst_ref=dst, send_sem=send, recv_sem=recv, device_id=device, device_id_type=MESH
    )


class Exchange:
    def __init__(self, diag, panel, dbuf, relay, rows, win, wsrc, pw, q, sems):
        self.diag, self.panel, self.dbuf, self.relay, self.rows = diag, panel, dbuf, relay, rows
        self.win, self.wsrc, self.pw, self.q = win, wsrc, pw, q
        (self.loc, self.ds, self.dr, self.cs, self.cr, self.rs, self.rr, self.zs, self.zr, self.xs, self.xr,
         self.w1s, self.w1r, self.w2s, self.w2r, self.w3s, self.w3r, self.w4s, self.w4r, self.w5s, self.w5r) = sems
        self.r, self.c, self.s = (lax.axis_index(a) for a in ALL)
        self.corner = jnp.logical_and(self.r == 0, self.c == 0)

    def enter(self):
        r, c, s = self.r, self.c, self.s
        self.own_diag = pltpu.make_async_copy(self.diag, self.dbuf.at[r, c, s], self.loc.at[0])
        self.own_panel = pltpu.make_async_copy(self.panel, self.relay.at[c], self.loc.at[1])
        self.own_diag.start()
        self.own_panel.start()
        barrier = pltpu.get_barrier_semaphore()
        for axis, me, n in (("depth", s, 8), ("col", c, 4), ("row", r, 4)):
            for t in range(1, n):
                pl.semaphore_signal(barrier, inc=1, device_id={axis: (me + t) % n}, device_id_type=MESH)
        pl.semaphore_wait(barrier, 13)
        self.own_diag.wait()

    def diag_col(self, t, c):
        ref = self.dbuf.at[self.r, c, self.s]
        return remote(ref, ref, self.cs.at[t], self.cr.at[t], col=(self.c + t) % 4)

    def diag_col_send(self):
        for t in range(1, 4):
            self.diag_col(t, self.c).start()

    def diag_col_wait(self):
        for t in range(1, 4):
            self.diag_col(t, (self.c - t) % 4).wait_recv()

    def diag_depth(self, t, s, i):
        ref = self.dbuf.at[i, :, s, :, 0 : 128 * (i + 1)]
        return remote(ref, ref, self.ds.at[t], self.dr.at[t], depth=(self.s + t) % 8)

    def by_row(self, act):
        for i in range(4):

            @pl.when(self.r == i)
            def _():
                act(i)

    def diag_depth_send(self):
        self.by_row(lambda i: [self.diag_depth(t, self.s, i).start() for t in range(1, 8)] and None)

    def diag_depth_wait(self):
        self.by_row(lambda i: [self.diag_depth(t, (self.s - t) % 8, i).wait_recv() for t in range(1, 8)] and None)

    def diag_row(self, t, i):
        ref = self.dbuf.at[i, :, :, :, 0 : 128 * (i + 1)]
        return remote(ref, ref, self.rs.at[t], self.rr.at[t], row=(self.r + t) % 4)

    def diag_row_send(self):
        self.by_row(lambda i: [self.diag_row(t, i).start() for t in range(1, 4)] and None)

    def diag_row_wait(self, src):
        self.by_row(lambda i: None if i == src else self.diag_row((i - src) % 4, src).wait_recv())

    def rows_col(self, t, slot, b):
        ref = self.relay.at[slot, :, at(b)]
        return remote(ref, ref, self.zs.at[t, b], self.zr.at[t, b], col=(self.c + t) % 4)

    def rows_col_send(self, b):
        for t in (1, 3, 2):
            self.rows_col(t, self.c, b).start()

    def rows_pass(self, b):
        for t in (1, 3, 2):
            slot = (self.c - t) % 4
            self.rows_col(t, slot, b).wait_recv()
            self.rows_depth_send(t, slot, b)

    def rows_depth(self, t, slot, b):
        target, j = 2 * slot + self.s // 4, self.s % 4
        return target, remote(
            self.relay.at[slot, :, at(b)], self.rows.at[j, :, at(b)], self.xs.at[t, b], self.xr.at[j, b], depth=target
        )

    def rows_depth_send(self, t, slot, b):
        target, copy = self.rows_depth(t, slot, b)

        @pl.when(target != self.s)
        def _():
            copy.start()

        @pl.when(target == self.s)
        def _():
            self.rows[self.s % 4, :, at(b)] = self.relay[slot, :, at(b)]

    def rows_wait(self, b):
        for j in range(4):
            source = 4 * (self.s % 2) + j
            ref = self.rows.at[j, :, at(b)]

            @pl.when(source != self.s)
            def _():
                remote(ref, ref, self.xs.at[0, b], self.xr.at[j, b], depth=source).wait_recv()

    def win_main(self, i, d):
        n = 8 if d < 7 else 7 - i
        return remote(
            self.wsrc.at[i + 8 * d : i + 8 * d + n], self.pw.at[i, 0:n], self.w1s.at[d], self.w1r.at[i], depth=d
        )

    def win_head(self, c):
        return remote(self.wsrc.at[0 : c + 1], self.pw.at[c, 7 - c : 8], self.w1s.at[8], self.w1r.at[4 + c], depth=7)

    def win_scatter(self, act):
        for i in range(5):

            @pl.when(jnp.logical_and(self.corner, self.s == i))
            def _():
                if i < 4:
                    for d in range(8):
                        if d != i:
                            act(self.win_main(i, d))
                if i > 0:
                    act(self.win_head(i - 1))

    def win_scatter_send(self):
        @pl.when(jnp.logical_and(self.corner, self.s < 5))
        def _():
            for u in range(63):
                self.wsrc[u] = self.relay[0, 4 * u : 4 * u + 4, :]

        for i in range(4):

            @pl.when(jnp.logical_and(self.corner, self.s == i))
            def _():
                self.pw[i] = self.wsrc[9 * i : 9 * i + 8]

        self.win_scatter(lambda copy: copy.start())

    def win_scatter_wait(self):
        for d in range(8):

            @pl.when(jnp.logical_and(self.corner, self.s == d))
            def _():
                for i in range(4):
                    if d != i:
                        self.win_main(i, d).wait_recv()
                    if d == 7:
                        self.win_head(i).wait_recv()

    def win_col(self, t):
        return remote(self.pw.at[t], self.q, self.w2s.at[t], self.w2r.at[0], col=t)

    def win_col_send(self):
        @pl.when(self.corner)
        def _():
            for t in range(1, 4):
                self.win_col(t).start()
            self.q[...] = self.pw[0]

    def win_col_wait(self):
        @pl.when(jnp.logical_and(self.r == 0, self.c != 0))
        def _():
            self.win_col(1).wait_recv()

    def win_row(self, t, row):
        return remote(
            self.q.at[2 * t : 2 * t + 2], self.win.at[self.s, row], self.w3s.at[t], self.w3r.at[0], row=t
        )

    def win_row_send(self):
        @pl.when(self.r == 0)
        def _():
            for t in range(1, 4):
                self.win_row(t, t).start()
            self.win[self.s, 0] = self.q[0:2]

    def win_row_wait(self):
        @pl.when(self.r != 0)
        def _():
            self.win_row(1, self.r).wait_recv()

    def win_depth(self, t, d):
        ref = self.win.at[d, self.r]
        return remote(ref, ref, self.w4s.at[t], self.w4r.at[t], depth=(self.s + t) % 8)

    def win_depth_send(self):
        for t in range(1, 8):
            self.win_depth(t, self.s).start()

    def win_depth_wait(self):
        for t in range(1, 8):
            self.win_depth(t, (self.s - t) % 8).wait_recv()

    def win_all(self, t, row):
        ref = self.win.at[:, row]
        return remote(ref, ref, self.w5s.at[t], self.w5r.at[t], row=(self.r + t) % 4)

    def win_all_send(self):
        for t in range(1, 4):
            self.win_all(t, self.r).start()

    def win_all_wait(self):
        for t in range(1, 4):
            self.win_all(t, (self.r - t) % 4).wait_recv()

    def leave(self):
        for t in range(1, 8):
            self.win_depth(t, self.s).wait_send()
        self.by_row(
            lambda i: [self.diag_depth(t, self.s, i).wait_send() for t in range(1, 8)]
            and [self.diag_row(t, i).wait_send() for t in range(1, 4)]
            and None
        )
        for t in range(1, 4):
            self.diag_col(t, self.c).wait_send()
            self.win_all(t, self.r).wait_send()
        for b in range(4):
            for t in range(4):
                if t:
                    self.rows_col(t, self.c, b).wait_send()
                target, copy = self.rows_depth(t, (self.c - t) % 4, b)

                @pl.when(target != self.s)
                def _():
                    copy.wait_send()

        self.win_scatter(lambda copy: copy.wait_send())

        @pl.when(self.corner)
        def _():
            for t in range(1, 4):
                self.win_col(t).wait_send()

        @pl.when(self.r == 0)
        def _():
            for t in range(1, 4):
                self.win_row(t, t).wait_send()


SEMAPHORES = ((3,), (8,), (8,), (4,), (4,), (4,), (4,), (4, 4), (4, 4), (4, 4), (4, 4),
              (9,), (8,), (4,), (1,), (4,), (1,), (8,), (8,), (4,), (4,))


def kernel(
    diag_in, panel, trailing_in, own_l, solved, updated,
    dbuf, relay, rows, win, wsrc, pw, q, diag, window, l, schur, trailing, *sems,
):
    e = Exchange(diag_in, panel, dbuf, relay, rows, win, wsrc, pw, q, sems)
    f = Factor(diag, l, schur)

    def assemble(i):
        e.diag_row_wait(i)
        for c in range(4):
            for s in range(8):
                first = 128 * i + 32 * c + 4 * s
                diag[first : first + 4, 0 : 128 * (i + 1)] = dbuf[i, c, s, :, 0 : 128 * (i + 1)]

    own_trailing = pltpu.make_async_copy(trailing_in, trailing, sems[0].at[2])
    own_trailing.start()
    e.enter()
    e.diag_col_send()
    e.own_panel.wait()
    e.rows_col_send(0)
    e.rows_col_send(1)
    e.diag_col_wait()
    e.diag_depth_send()
    e.win_scatter_send()
    e.rows_depth_send(0, e.c, 0)
    e.rows_depth_send(0, e.c, 1)
    e.diag_depth_wait()
    e.diag_row_send()
    e.win_scatter_wait()
    e.win_col_send()
    e.rows_col_send(2)
    e.rows_col_send(3)
    e.rows_pass(0)
    assemble(0)
    f.block(0)
    e.win_col_wait()
    e.win_row_send()
    e.rows_depth_send(0, e.c, 2)
    e.rows_pass(1)
    for i in range(1, 4):
        assemble(i)
    f.rest(0)
    f.block(1)
    e.win_row_wait()
    e.win_depth_send()
    e.rows_depth_send(0, e.c, 3)
    e.rows_pass(2)
    f.rest(1)
    f.block(2)
    e.win_depth_wait()
    e.win_all_send()
    e.rows_pass(3)
    f.rest(2)
    f.block(3)

    position = (e.r * 4 + e.c) * 8 + e.s
    pair = l[pl.ds(pl.multiple_of((position // 2) * 8, 8), 8), :]
    own_l[...] = jnp.where(position % 2 == 0, pair[0:4], pair[4:8])
    own = []
    for k in range(4):
        f.solve_block(relay[e.c, :, at(k)], k, own)
        solved[:, at(k)] = own[k][0]
    e.win_all_wait()
    for s in range(8):
        for r in range(4):
            for u in range(2):
                first = 32 * s + 8 * r + 4 * u
                window[first : first + 4, :] = win[s, r, u]
    w = []
    for k in range(4):
        f.solve_block(window[:, at(k)], k, w)
    own_trailing.wait()
    size = panel.shape[0]
    x = [[] for _ in range(4)]
    total = [None] * 4
    for k in range(4):
        e.rows_wait(k)
        for j in range(4):
            f.solve_block(rows[j, :, at(k)], k, x[j])
            term = dot(x[j][k][1], w[k][1])
            total[j] = term if k == 0 else total[j] + term
    for j in range(4):
        span = slice(size * j, size * (j + 1))
        updated[span, :] = trailing[span, :] - total[j]
    e.leave()


def body(diag_block, panel_rows, trailing):
    vmem = pl.BlockSpec(memory_space=pltpu.VMEM)
    hbm = pl.BlockSpec(memory_space=pltpu.HBM)
    shapes = (
        (4, 4, 8, 4, 512),
        (4, *panel_rows.shape),
        (4, *panel_rows.shape),
        (8, 4, 2, 4, 512),
        (63, 4, 512),
        (4, 8, 4, 512),
        (8, 4, 512),
        (512, 512),
        (256, 512),
        (512, 512),
        (512, 512),
        trailing.shape,
    )
    return pl.pallas_call(
        kernel,
        out_shape=tuple(jax.ShapeDtypeStruct(a.shape, F32) for a in (diag_block, panel_rows, trailing)),
        in_specs=[hbm] * 3,
        out_specs=(vmem,) * 3,
        scratch_shapes=[pltpu.VMEM(shape, F32) for shape in shapes]
        + [pltpu.SemaphoreType.DMA(n) for n in SEMAPHORES],
        compiler_params=pltpu.CompilerParams(
            collective_id=0, has_side_effects=True, vmem_limit_bytes=VMEM_LIMIT
        ),
        name="panel_step",
    )(diag_block, panel_rows, trailing)


VMEM_LIMIT = 60 * 2**20


def solution(mesh):
    specs = (P(ALL, None), P(ALL, None), P(("row", "depth"), "col"))
    return jax.shard_map(body, mesh=mesh, in_specs=specs, out_specs=specs, check_vma=False)
```

```python
import jax
import jax.numpy as jnp
from jax import lax
from jax.experimental import pallas as pl
from jax.experimental.pallas import tpu as pltpu
from jax.sharding import PartitionSpec as P

ALL = ("row", "col", "depth")
F32 = jnp.float32
NT = (((1,), (1,)), ((), ()))
NN = (((1,), (0,)), ((), ()))
BLOCK = 128
MESH = pl.DeviceIdType.MESH


def at(i):
    return slice(BLOCK * i, BLOCK * (i + 1))


def split(x):
    hi = x.astype(jnp.bfloat16)
    return hi, (x - hi.astype(F32)).astype(jnp.bfloat16)


def dot(a, b, dims=NT):
    def one(x, y):
        return lax.dot_general(x, y, dims, preferred_element_type=F32)

    return one(a[0], b[0]) + (one(a[0], b[1]) + one(a[1], b[0]))


def sub(v, k):
    return jnp.broadcast_to(v[k : k + 1, :], (8, 128))


class Block:
    def __init__(self, rows):
        self.ri = lax.broadcasted_iota(jnp.int32, (8, 128), 0)
        self.li = lax.broadcasted_iota(jnp.int32, (8, 128), 1)
        self.rows = rows
        self.unit = jnp.stack([jnp.where(self.li == self.ri + 8 * v, 1.0, 0.0).astype(F32) for v in range(16)])
        self.upper, self.inverse = [], []

    def advance(self, panels):
        ri, li = self.ri, self.li
        for p in panels:
            rows, unit = self.rows, self.unit
            cols = [jnp.broadcast_to(rows[:, :, 8 * p + j : 8 * p + j + 1], rows.shape) for j in range(8)]
            r = [sub(rows[0], k) for k in range(8)]
            s = [sub(unit[0], k) for k in range(8)]
            for k in range(8):
                inv = lax.rsqrt(sub(cols[k][0], k))
                cols[k] = cols[k] * inv
                r[k] = r[k] * inv
                s[k] = s[k] * inv
                for j in range(k + 1, 8):
                    m = sub(cols[k][0], j)
                    cols[j] = cols[j] - cols[k] * m
                    r[j] = r[j] - m * r[k]
                    s[j] = s[j] - m * s[k]
            u, t = r[0], s[0]
            for k in range(1, 8):
                u = jnp.where(ri == k, r[k], u)
                t = jnp.where(ri == k, s[k], t)
            self.upper.append(jnp.where(li >= ri + 8 * p, u, 0.0))
            self.inverse.append(t)
            if p < 15:
                rows, unit = rows[1:], unit[1:]
                for k in range(8):
                    rows = rows - cols[k][1:] * r[k]
                    unit = unit - cols[k][1:] * s[k]
                self.rows, self.unit = rows, unit


class Factor:
    def __init__(self, a, l):
        self.a, self.l = a, l
        self.lows, self.invs, self.below, self.sums = {}, {}, {}, {}

    def column(self, k, i):
        value = self.a[at(i), at(k)]
        for m in range(k):
            value = value - dot(self.lows[i, m], self.lows[k, m])
        return value

    def block(self, k, tasks=(), between=lambda: None):
        value = self.column(k, k)
        b = Block(value.reshape(16, 8, 128))
        tasks = list(tasks)
        for p in range(16):
            b.advance([p])
            if p == 7:
                between()
            for _ in range(-(-len(tasks) // (16 - p))):
                tasks.pop(0)()
        self.invs[k, k] = split(jnp.concatenate(b.inverse, 0))
        self.l[at(k), at(k)] = jnp.concatenate(b.upper, 0).T
        for j in range(k + 1, 4):
            self.l[at(k), at(j)] = jnp.zeros((BLOCK, BLOCK), F32)

    def prepare(self, k, i):
        def task():
            self.below[i] = split(self.column(k, i))

        return task

    def rest(self, k):
        for i in range(k + 1, 4):
            if i not in self.below:
                self.prepare(k, i)()
            low = dot(self.below.pop(i), self.invs[k, k])
            self.l[at(i), at(k)] = low
            self.lows[i, k] = split(low)

    def inverse_sum(self, k, m):
        def task():
            total = dot(self.lows[k, m], self.invs[m, m], NN)
            for j in range(m + 1, k):
                total = total + dot(self.lows[k, j], self.invs[j, m], NN)
            self.sums[k, m] = split(total)

        return task

    def inverse(self, k, m):
        def task():
            self.invs[k, m] = split(-dot(self.invs[k, k], self.sums.pop((k, m)), NN))

        return task

    def solved(self, x, k):
        total = dot(x[0], self.invs[k, 0])
        for m in range(1, k + 1):
            total = total + dot(x[m], self.invs[k, m])
        return total


def remote(src, dst, send, recv, **device):
    return pltpu.make_async_remote_copy(
        src_ref=src, dst_ref=dst, send_sem=send, recv_sem=recv, device_id=device, device_id_type=MESH
    )


class Exchange:
    def __init__(self, diag, panel, dbuf, relay, rows, win, wsrc, wq, hq, pw, sems):
        self.diag, self.panel, self.dbuf, self.relay, self.rows = diag, panel, dbuf, relay, rows
        self.win, self.wsrc, self.wq, self.hq, self.pw = win, wsrc, wq, hq, pw
        (self.loc, self.ds, self.dr, self.cs, self.cr, self.rs, self.rr, self.zs, self.zr, self.xs, self.xr,
         self.w1s, self.w1r, self.w2s, self.w2r, self.w3s, self.w3r, self.w4s, self.w4r, self.w5s, self.w5r) = sems
        self.r, self.c, self.s = (lax.axis_index(a) for a in ALL)
        self.corner = jnp.logical_and(self.r == 0, self.c == 0)

    def enter(self):
        r, c, s = self.r, self.c, self.s
        self.own_diag = pltpu.make_async_copy(self.diag, self.dbuf.at[r, c, s], self.loc.at[0])
        self.own_panel = pltpu.make_async_copy(self.panel, self.relay.at[c], self.loc.at[1])
        self.own_diag.start()
        self.own_panel.start()
        barrier = pltpu.get_barrier_semaphore()
        for axis, me, n in (("depth", s, 8), ("col", c, 4), ("row", r, 4)):
            for t in range(1, n):
                pl.semaphore_signal(barrier, inc=1, device_id={axis: (me + t) % n}, device_id_type=MESH)
        pl.semaphore_wait(barrier, 13)
        self.own_diag.wait()

    def diag_col(self, t, c):
        ref = self.dbuf.at[self.r, c, self.s]
        return remote(ref, ref, self.cs.at[t], self.cr.at[t], col=(self.c + t) % 4)

    def diag_col_send(self):
        for t in range(1, 4):
            self.diag_col(t, self.c).start()

    def diag_col_wait(self):
        for t in range(1, 4):
            self.diag_col(t, (self.c - t) % 4).wait_recv()

    def by_row(self, act):
        for i in range(4):

            @pl.when(self.r == i)
            def _():
                act(i)

    def diag_depth(self, t, s, i, part):
        cols = slice(0, 128) if part == 0 else slice(128, 128 * (i + 1))
        ref = self.dbuf.at[i, :, s, :, cols]
        return remote(ref, ref, self.ds.at[t, part], self.dr.at[t, part], depth=(self.s + t) % 8)

    def diag_depth_each(self, part, act, receive=False):
        def at_row(i):
            if i >= part:
                for t in range(1, 8):
                    act(self.diag_depth(t, (self.s - t) % 8 if receive else self.s, i, part))

        self.by_row(at_row)

    def diag_depth_send(self, part):
        self.diag_depth_each(part, lambda copy: copy.start())

    def diag_depth_wait(self, part):
        self.diag_depth_each(part, lambda copy: copy.wait_recv(), receive=True)

    def diag_row(self, t, i, b):
        ref = self.dbuf.at[i, :, :, :, at(b)]
        return remote(ref, ref, self.rs.at[t, b], self.rr.at[t, b], row=(self.r + t) % 4)

    def diag_row_each(self, b, act):
        def at_row(i):
            if i >= b:
                for t in range(1, 4):
                    act(self.diag_row(t, i, b))

        self.by_row(at_row)

    def diag_row_send(self, b):
        self.diag_row_each(b, lambda copy: copy.start())

    def diag_row_wait(self, src, b):
        def at_row(i):
            if i != src:
                self.diag_row((i - src) % 4, src, b).wait_recv()

        self.by_row(at_row)

    def rows_col(self, t, slot, b):
        ref = self.relay.at[slot, :, at(b)]
        return remote(ref, ref, self.zs.at[t, b], self.zr.at[t, b], col=(self.c + t) % 4)

    def rows_col_send(self, b):
        for t in (1, 3, 2):
            self.rows_col(t, self.c, b).start()

    def rows_pass(self, b):
        for t in (1, 3, 2):
            slot = (self.c - t) % 4
            self.rows_col(t, slot, b).wait_recv()
            self.rows_depth_send(t, slot, b)

    def rows_depth(self, t, slot, b):
        target, j = 2 * slot + self.s // 4, self.s % 4
        return target, remote(
            self.relay.at[slot, :, at(b)], self.rows.at[j, :, at(b)], self.xs.at[t, b], self.xr.at[j, b], depth=target
        )

    def rows_depth_send(self, t, slot, b):
        target, copy = self.rows_depth(t, slot, b)

        @pl.when(target != self.s)
        def _():
            copy.start()

        @pl.when(target == self.s)
        def _():
            self.rows[self.s % 4, :, at(b)] = self.relay[slot, :, at(b)]

    def rows_wait(self, b):
        for j in range(4):
            source = 4 * (self.s % 2) + j
            ref = self.rows.at[j, :, at(b)]

            @pl.when(source != self.s)
            def _():
                remote(ref, ref, self.xs.at[0, b], self.xr.at[j, b], depth=source).wait_recv()

    def corner_case(self, rows, i, act):
        here = jnp.logical_and(self.c == 0, self.s == i)
        if rows is not None:
            here = jnp.logical_and(here, jnp.logical_and(self.r >= rows[0], self.r <= rows[-1]))

        @pl.when(here)
        def _():
            act()

    def win_main(self, i, t):
        n = 16 if t < 3 else 15 - i
        return remote(
            self.wsrc.at[i + 16 * t : i + 16 * t + n], self.wq.at[0:n], self.w1s.at[t], self.w1r.at[0], row=t
        )

    def win_head(self, i):
        return remote(self.wsrc.at[0:i], self.hq.at[0:i], self.w1s.at[4], self.w1r.at[1], row=3)

    def win_scatter(self, act):
        def copies(i):
            if i < 4:
                for t in range(1, 4):
                    act(self.win_main(i, t))
            if i > 0:
                act(self.win_head(i))

        for i in range(5):
            self.corner_case((0,), i, lambda: copies(i))

    def win_scatter_send(self):
        @pl.when(jnp.logical_and(self.corner, self.s < 5))
        def _():
            for u in range(63):
                self.wsrc[u] = self.relay[0, 4 * u : 4 * u + 4, :]

        self.win_scatter(lambda copy: copy.start())

    def win_scatter_wait(self):
        for i in range(5):
            if i < 4:
                self.corner_case((1, 2), i, lambda: self.win_main(i, 1).wait_recv())
                self.corner_case((3,), i, lambda: self.win_main(i, 3).wait_recv())
            if i > 0:
                self.corner_case((3,), i, lambda: self.win_head(i).wait_recv())

    def win_piece(self, rows, i, d):
        n = 2 if rows[0] < 3 else min(max(15 - i - 2 * d, 0), 2)
        if n == 0:
            return None
        src = self.wsrc.at[i + 2 * d : i + 2 * d + n] if rows[0] == 0 else self.wq.at[2 * d : 2 * d + n]
        dst = self.pw.at[i, 0:n]
        return src, dst, lambda: remote(src, dst, self.w2s.at[d], self.w2r.at[i], depth=d)

    def win_head_piece(self, c, d):
        first, last = max(0, 2 * d - 15 + c), min(c + 1, 2 * d - 13 + c)
        if d < 6 or first >= last:
            return None
        slot = (15 - c + first) % 2
        return remote(
            self.hq.at[first:last],
            self.pw.at[c, slot : slot + last - first],
            self.w2s.at[2 + d],
            self.w2r.at[4 + c],
            depth=d,
        )

    def win_spread(self, act, local=False):
        def copies(rows, i):
            for d in range(8):
                if i < 4:
                    piece = self.win_piece(rows, i, d)
                    if piece and d != i:
                        act(piece[2]())
                    elif piece and local:
                        piece[1][...] = piece[0][...]
                if i > 0 and rows[0] == 3:
                    copy = self.win_head_piece(i - 1, d)
                    if copy:
                        act(copy)

        for i in range(5):
            for rows in ((0,), (1, 2), (3,)):
                self.corner_case(rows, i, lambda: copies(rows, i))

    def win_spread_send(self):
        self.win_spread(lambda copy: copy.start(), local=True)

    def win_spread_wait(self):
        def waits(rows, d):
            for i in range(4):
                piece = self.win_piece(rows, i, d)
                if piece and d != i:
                    piece[2]().wait_recv()
                if rows[0] == 3:
                    copy = self.win_head_piece(i, d)
                    if copy:
                        copy.wait_recv()

        for d in range(8):
            for rows in ((0, 1, 2), (3,)):
                self.corner_case(rows, d, lambda: waits(rows, d))

    def win_col(self, t):
        return remote(self.pw.at[t], self.win.at[self.s, self.r], self.w3s.at[t], self.w3r.at[0], col=t)

    def win_col_send(self):
        @pl.when(self.c == 0)
        def _():
            for t in range(1, 4):
                self.win_col(t).start()
            self.win[self.s, self.r] = self.pw[0]

    def win_col_wait(self):
        @pl.when(self.c != 0)
        def _():
            self.win_col(1).wait_recv()

    def win_depth(self, t, d):
        ref = self.win.at[d, self.r]
        return remote(ref, ref, self.w4s.at[t], self.w4r.at[t], depth=(self.s + t) % 8)

    def win_depth_send(self):
        for t in range(1, 8):
            self.win_depth(t, self.s).start()

    def win_depth_wait(self):
        for t in range(1, 8):
            self.win_depth(t, (self.s - t) % 8).wait_recv()

    def win_all(self, t, row):
        ref = self.win.at[:, row]
        return remote(ref, ref, self.w5s.at[t], self.w5r.at[t], row=(self.r + t) % 4)

    def win_all_send(self):
        for t in range(1, 4):
            self.win_all(t, self.r).start()

    def win_all_wait(self):
        for t in range(1, 4):
            self.win_all(t, (self.r - t) % 4).wait_recv()

    def leave(self):
        for t in range(1, 8):
            self.win_depth(t, self.s).wait_send()
        for part in range(2):
            self.diag_depth_each(part, lambda copy: copy.wait_send())
        for b in range(4):
            self.diag_row_each(b, lambda copy: copy.wait_send())
        for t in range(1, 4):
            self.diag_col(t, self.c).wait_send()
            self.win_all(t, self.r).wait_send()
        for b in range(4):
            for t in range(4):
                if t:
                    self.rows_col(t, self.c, b).wait_send()
                target, copy = self.rows_depth(t, (self.c - t) % 4, b)

                @pl.when(target != self.s)
                def _():
                    copy.wait_send()

        self.win_scatter(lambda copy: copy.wait_send())
        self.win_spread(lambda copy: copy.wait_send())

        @pl.when(self.c == 0)
        def _():
            for t in range(1, 4):
                self.win_col(t).wait_send()


SEMAPHORES = ((3,), (8, 2), (8, 2), (4,), (4,), (4, 4), (4, 4), (4, 4), (4, 4), (4, 4), (4, 4),
              (5,), (2,), (10,), (8,), (4,), (1,), (8,), (8,), (4,), (4,))


def kernel(
    diag_in, panel, trailing_in, own_l, solved, updated,
    dbuf, relay, rows, win, wsrc, wq, hq, pw, diag, window, l, trailing, *sems,
):
    e = Exchange(diag_in, panel, dbuf, relay, rows, win, wsrc, wq, hq, pw, sems)
    f = Factor(diag, l)

    def assemble(i, b):
        e.diag_row_wait(i, b)
        for c in range(4):
            for s in range(8):
                first = 128 * i + 32 * c + 4 * s
                diag[first : first + 4, at(b)] = dbuf[i, c, s, :, at(b)]

    def assemble_column(b):
        for i in range(b, 4):
            if i > 0:
                assemble(i, b)

    own_trailing = pltpu.make_async_copy(trailing_in, trailing, sems[0].at[2])
    own_trailing.start()
    e.enter()
    e.diag_col_send()
    e.own_panel.wait()
    e.rows_col_send(0)
    e.win_scatter_send()
    e.rows_col_send(1)
    e.diag_col_wait()
    e.diag_depth_send(0)
    e.diag_depth_send(1)
    e.diag_depth_wait(0)
    e.diag_row_send(0)
    e.diag_depth_wait(1)
    e.diag_row_send(1)
    e.diag_row_send(2)
    e.diag_row_send(3)
    e.win_scatter_wait()
    e.win_spread_send()
    e.rows_depth_send(0, e.c, 0)
    e.rows_depth_send(0, e.c, 1)
    e.rows_pass(0)
    assemble(0, 0)
    e.win_spread_wait()
    e.win_col_send()
    e.rows_col_send(2)

    def first_hook():
        e.rows_col_send(3)

    f.block(0, between=first_hook)
    e.win_col_wait()
    e.win_depth_send()
    e.rows_depth_send(0, e.c, 2)
    e.rows_pass(1)
    assemble_column(0)
    f.rest(0)
    assemble_column(1)

    size = panel.shape[0]
    own_a, rows_a, own_x = {}, [{} for _ in range(4)], {}
    rows_x = [{} for _ in range(4)]

    def own_task(k):
        def task():
            own_a[k] = split(relay[e.c, :, at(k)])
            solved[:, at(k)] = f.solved(own_a, k)

        return task

    def row_task(j, k):
        def task():
            rows_a[j][k] = split(rows[j, :, at(k)])
            rows_x[j][k] = split(f.solved(rows_a[j], k))

        return task

    def second_hook():
        e.rows_depth_send(0, e.c, 3)

    f.block(1, [f.prepare(1, 2), f.prepare(1, 3), own_task(0)], second_hook)
    e.win_depth_wait()
    e.win_all_send()
    e.rows_pass(2)
    f.rest(1)
    assemble_column(2)

    def third_hook():
        e.rows_pass(3)

    f.block(
        2,
        [f.prepare(2, 3), f.inverse_sum(1, 0), f.inverse(1, 0), own_task(1), f.inverse_sum(2, 0), f.inverse_sum(2, 1)],
        third_hook,
    )
    f.rest(2)
    assemble_column(3)
    e.rows_wait(0)
    e.rows_wait(1)
    f.block(
        3,
        [f.inverse(2, 0), f.inverse(2, 1), own_task(2)]
        + [row_task(j, k) for k in range(2) for j in range(4)]
        + [f.inverse_sum(3, m) for m in range(3)],
    )
    for m in range(3):
        f.inverse(3, m)()

    position = (e.r * 4 + e.c) * 8 + e.s
    pair = l[pl.ds(pl.multiple_of((position // 2) * 8, 8), 8), :]
    own_l[...] = jnp.where(position % 2 == 0, pair[0:4], pair[4:8])
    own_task(3)()
    e.win_all_wait()
    for s in range(8):
        for r in range(4):
            for u in range(2):
                first = 64 * r + 8 * s + 4 * u
                window[first : first + 4, :] = win[s, r, u]
    window_a = [split(window[:, at(k)]) for k in range(4)]
    w = [split(f.solved(window_a, k)) for k in range(4)]
    e.rows_wait(2)
    e.rows_wait(3)
    own_trailing.wait()
    for j in range(4):
        row_task(j, 2)()
        row_task(j, 3)()
        total = dot(rows_x[j][0], w[0])
        for k in range(1, 4):
            total = total + dot(rows_x[j][k], w[k])
        span = slice(size * j, size * (j + 1))
        updated[span, :] = trailing[span, :] - total
    e.leave()


def deliver(own_l, solved, updated, own_l_out, solved_out, updated_out, sem):
    copies = [
        pltpu.make_async_copy(src, dst, sem.at[i])
        for i, (src, dst) in enumerate(((own_l, own_l_out), (solved, solved_out), (updated, updated_out)))
    ]
    for copy in copies:
        copy.start()
    for copy in copies:
        copy.wait()


def body(diag_block, panel_rows, trailing):
    vmem = pl.BlockSpec(memory_space=pltpu.VMEM)
    hbm = pl.BlockSpec(memory_space=pltpu.HBM)
    shapes = (
        (4, 4, 8, 4, 512),
        (4, *panel_rows.shape),
        (4, *panel_rows.shape),
        (8, 4, 2, 4, 512),
        (63, 4, 512),
        (16, 4, 512),
        (4, 4, 512),
        (4, 2, 4, 512),
        (512, 512),
        (256, 512),
        (512, 512),
        trailing.shape,
    )
    outs = tuple(jax.ShapeDtypeStruct(a.shape, F32) for a in (diag_block, panel_rows, trailing))
    results = pl.pallas_call(
        kernel,
        out_shape=outs,
        in_specs=[hbm] * 3,
        out_specs=(vmem,) * 3,
        scratch_shapes=[pltpu.VMEM(shape, F32) for shape in shapes]
        + [pltpu.SemaphoreType.DMA(n) for n in SEMAPHORES],
        compiler_params=pltpu.CompilerParams(
            collective_id=0, has_side_effects=True, vmem_limit_bytes=VMEM_LIMIT
        ),
        name="panel_step",
    )(*(pltpu.with_memory_space_constraint(x, pltpu.HBM) for x in (diag_block, panel_rows, trailing)))
    return pl.pallas_call(
        deliver,
        out_shape=outs,
        in_specs=[vmem] * 3,
        out_specs=(hbm,) * 3,
        scratch_shapes=[pltpu.SemaphoreType.DMA((3,))],
        compiler_params=pltpu.CompilerParams(vmem_limit_bytes=2 * 2**20),
        name="deliver",
    )(*results)


VMEM_LIMIT = 44 * 2**20


def solution(mesh):
    specs = (P(ALL, None), P(ALL, None), P(("row", "depth"), "col"))
    return jax.shard_map(body, mesh=mesh, in_specs=specs, out_specs=specs, check_vma=False)
```

```python
import jax
import jax.numpy as jnp
from jax import lax
from jax.experimental import pallas as pl
from jax.experimental.pallas import tpu as pltpu
from jax.sharding import PartitionSpec as P

ALL = ("row", "col", "depth")
F32 = jnp.float32
NT = (((1,), (1,)), ((), ()))
NN = (((1,), (0,)), ((), ()))
BLOCK = 128
MESH = pl.DeviceIdType.MESH


def at(i):
    return slice(BLOCK * i, BLOCK * (i + 1))


def half(h):
    return slice(256 * h, 256 * (h + 1))


def split(x):
    hi = x.astype(jnp.bfloat16)
    return hi, (x - hi.astype(F32)).astype(jnp.bfloat16)


def dot(a, b, dims=NT):
    left = jnp.concatenate([a[0], a[1], a[0]], 1)
    right = jnp.concatenate([b[0], b[0], b[1]], dims[0][1][0])
    return lax.dot_general(left, right, dims, preferred_element_type=F32)


def beside(parts, axis=1):
    return tuple(jnp.concatenate(x, axis) if len(x) > 1 else x[0] for x in zip(*parts))


def sub(v, k):
    return jnp.broadcast_to(v[k : k + 1, :], (8, 128))


class Block:
    def __init__(self, rows):
        self.ri = lax.broadcasted_iota(jnp.int32, (8, 128), 0)
        self.li = lax.broadcasted_iota(jnp.int32, (8, 128), 1)
        self.rows = rows
        self.upper, self.inverse = [], []

    def advance(self, p):
        ri, li, rows = self.ri, self.li, self.rows
        first = 8 * p
        cols = [jnp.broadcast_to(rows[:, :, first + j : first + j + 1], rows.shape) for j in range(8)]
        e = {(i, j): sub(cols[j][0], i) for j in range(8) for i in range(j, 8)}
        r = [sub(rows[0], k) for k in range(8)]
        s = [jnp.where(li < first, r[k], jnp.where(li == first + k, 1.0, 0.0)) for k in range(8)]
        for k in range(8):
            inv = lax.rsqrt(e[k, k])
            m = {j: e[j, k] * inv for j in range(k + 1, 8)}
            for j in range(k + 1, 8):
                for i in range(j, 8):
                    e[i, j] = e[i, j] - m[i] * m[j]
            cols[k] = cols[k] * inv
            r[k] = r[k] * inv
            s[k] = s[k] * inv
            for j in range(k + 1, 8):
                cols[j] = cols[j] - cols[k] * m[j]
                r[j] = r[j] - m[j] * r[k]
                s[j] = s[j] - m[j] * s[k]
        u, t = r[0], s[0]
        for k in range(1, 8):
            u = jnp.where(ri == k, r[k], u)
            t = jnp.where(ri == k, s[k], t)
        self.upper.append(jnp.where(li >= ri + first, u, 0.0))
        self.inverse.append(t)
        if p < 15:
            rows = jnp.where(((li < first) | (li >= first + 8))[None], rows[1:], 0.0)
            for k in range(8):
                rows = rows - cols[k][1:] * jnp.where(li < first + 8, s[k], r[k])
            self.rows = rows


class Factor:
    def __init__(self, a, l):
        self.a, self.l = a, l
        self.lows, self.inv, self.inv_rows, self.below, self.sums = {}, {}, {}, {}, {}

    def low_row(self, i, n):
        return beside([self.lows[i, m] for m in range(n)])

    def column(self, k, i):
        value = self.a[at(i), at(k)]
        return value - dot(self.low_row(i, k), self.low_row(k, k)) if k else value

    def block(self, k, tasks=(), between=lambda: None, late=()):
        value = self.column(k, k)
        b = Block(value.reshape(16, 8, 128))
        tasks = [list(tasks), list(late)]
        for p in range(16):
            b.advance(p)
            half = tasks[p // 8 if late else 0]
            for _ in range(-(-len(half) // ((8 if late and p < 8 else 16) - p))):
                half.pop(0)()
            if p == 7:
                between()
        self.inv[k] = split(jnp.concatenate(b.inverse, 0))
        if k == 0:
            self.inv_rows[0] = self.inv[0]
        self.l[at(k), at(k)] = jnp.concatenate(b.upper, 0).T
        for j in range(k + 1, 4):
            self.l[at(k), at(j)] = jnp.zeros((BLOCK, BLOCK), F32)

    def prepare(self, k, i):
        def task():
            self.below[i] = split(self.column(k, i))

        return task

    def rest(self, k):
        for i in range(k + 1, 4):
            if i not in self.below:
                self.prepare(k, i)()
            low = dot(self.below.pop(i), self.inv[k])
            self.l[at(i), at(k)] = low
            self.lows[i, k] = split(low)

    def inverse_rows(self, rows, width):
        parts = []
        for k in rows:
            fill = jnp.zeros((BLOCK, width - BLOCK * (k + 1)), jnp.bfloat16)
            parts.append(beside([self.inv_rows[k], (fill, fill)]) if fill.shape[1] else self.inv_rows[k])
        return beside(parts, 0)

    def inverse_sum(self, k):
        def task():
            total = dot(self.low_row(k, k), self.inverse_rows(range(k), BLOCK * k), NN)
            self.sums[k] = split(total)

        return task

    def inverse_row(self, k):
        def task():
            left = split(-dot(self.inv[k], self.sums.pop(k), NN))
            self.inv_rows[k] = beside([left, self.inv[k]])

        return task

    def solved(self, x, h):
        return dot(beside(x[: h + 1]), self.inverse_rows((2 * h, 2 * h + 1), 256 * (h + 1)))


def remote(src, dst, send, recv, **device):
    return pltpu.make_async_remote_copy(
        src_ref=src, dst_ref=dst, send_sem=send, recv_sem=recv, device_id=device, device_id_type=MESH
    )


class Exchange:
    def __init__(self, diag, panel, own, dbuf, relay, rows, win, wsrc, wq, hq, pw, sems):
        self.diag, self.panel, self.own, self.dbuf, self.relay, self.rows = diag, panel, own, dbuf, relay, rows
        self.win, self.wsrc, self.wq, self.hq, self.pw = win, wsrc, wq, hq, pw
        (self.loc, self.ds, self.dr, self.cs, self.cr, self.rs, self.rr, self.zs, self.zr, self.xs, self.xr,
         self.w1s, self.w1r, self.w2s, self.w2r, self.w3s, self.w3r, self.w4s, self.w4r, self.w5s, self.w5r,
         self.as_, self.ar, self.bs, self.br, self.es, self.er) = sems
        self.r, self.c, self.s = (lax.axis_index(a) for a in ALL)
        self.corner = jnp.logical_and(self.r == 0, self.c == 0)

    def enter(self):
        r, c, s = self.r, self.c, self.s
        self.own_diag = pltpu.make_async_copy(self.diag, self.dbuf.at[r, c, s], self.loc.at[0])
        self.own_panel = pltpu.make_async_copy(self.panel, self.own, self.loc.at[1])
        self.own_diag.start()
        self.own_panel.start()
        barrier = pltpu.get_barrier_semaphore()
        for axis, me, n in (("depth", s, 8), ("col", c, 4), ("row", r, 4)):
            for t in range(1, n):
                pl.semaphore_signal(barrier, inc=1, device_id={axis: (me + t) % n}, device_id_type=MESH)
        self.own_panel.wait()
        n = self.own.shape[0]
        self.relay[c, 0:n] = self.own[...]
        self.relay[c, n:256] = jnp.zeros((256 - n, 512), F32)
        pl.semaphore_wait(barrier, 13)
        self.own_diag.wait()

    def diag_col(self, t, c):
        ref = self.dbuf.at[self.r, c, self.s]
        return remote(ref, ref, self.cs.at[t], self.cr.at[t], col=(self.c + t) % 4)

    def diag_col_send(self):
        for t in range(1, 4):
            self.diag_col(t, self.c).start()

    def diag_col_wait(self):
        for t in range(1, 4):
            self.diag_col(t, (self.c - t) % 4).wait_recv()

    def by_row(self, act):
        for i in range(4):

            @pl.when(self.r == i)
            def _():
                act(i)

    def diag_depth(self, t, s, i, part):
        cols = slice(0, 128) if part == 0 else slice(128, 128 * (i + 1))
        ref = self.dbuf.at[i, :, s, :, cols]
        return remote(ref, ref, self.ds.at[t, part], self.dr.at[t, part], depth=(self.s + t) % 8)

    def diag_depth_each(self, part, act, receive=False):
        def at_row(i):
            if i >= part:
                for t in range(1, 8):
                    act(self.diag_depth(t, (self.s - t) % 8 if receive else self.s, i, part))

        self.by_row(at_row)

    def diag_depth_send(self, part):
        self.diag_depth_each(part, lambda copy: copy.start())

    def diag_depth_wait(self, part):
        self.diag_depth_each(part, lambda copy: copy.wait_recv(), receive=True)

    def diag_row(self, t, i, b):
        ref = self.dbuf.at[i, :, :, :, at(b)]
        return remote(ref, ref, self.rs.at[t, b], self.rr.at[t, b], row=(self.r + t) % 4)

    def diag_row_each(self, b, act):
        def at_row(i):
            if i >= b:
                for t in range(1, 4):
                    act(self.diag_row(t, i, b))

        self.by_row(at_row)

    def diag_row_send(self, b):
        self.diag_row_each(b, lambda copy: copy.start())

    def diag_row_wait(self, src, b):
        def at_row(i):
            if i != src:
                self.diag_row((i - src) % 4, src, b).wait_recv()

        self.by_row(at_row)

    def rows_col(self, t, slot, b):
        ref = self.relay.at[slot, :, at(b)]
        return remote(ref, ref, self.zs.at[t, b], self.zr.at[t, b], col=(self.c + t) % 4)

    def rows_col_send(self, b):
        for t in (1, 3, 2):
            self.rows_col(t, self.c, b).start()

    def rows_pass(self, b):
        for t in (1, 3, 2):
            slot = (self.c - t) % 4
            self.rows_col(t, slot, b).wait_recv()
            self.rows_depth_send(t, slot, b)

    def rows_depth(self, t, slot, b):
        target, j = 2 * slot + self.s // 4, self.s % 4
        return target, remote(
            self.relay.at[slot, :, at(b)], self.rows.at[j, :, at(b)], self.xs.at[t, b], self.xr.at[j, b], depth=target
        )

    def rows_depth_send(self, t, slot, b):
        target, copy = self.rows_depth(t, slot, b)

        @pl.when(target != self.s)
        def _():
            copy.start()

        @pl.when(target == self.s)
        def _():
            self.rows[self.s % 4, :, at(b)] = self.relay[slot, :, at(b)]

    def rows_wait(self, b):
        for j in range(4):
            source = 4 * (self.s % 2) + j
            ref = self.rows.at[j, :, at(b)]

            @pl.when(source != self.s)
            def _():
                remote(ref, ref, self.xs.at[0, b], self.xr.at[j, b], depth=source).wait_recv()

    def quarter(self, a):
        return pl.ds(pl.multiple_of(64 * a, 64), 64), slice(256, 512)

    def half_col(self, t, slot, a):
        ref = self.relay.at[(slot, *self.quarter(a))]
        return remote(ref, ref, self.as_.at[t], self.ar.at[t], col=(self.c + t) % 4)

    def half_col_send(self):
        for t in (1, 3, 2):
            self.half_col(t, self.c, (self.c + t) % 4).start()

    def half_depth(self, t):
        slot = (self.c - t) % 4
        target, j, part = 2 * slot + self.s // 4, self.s % 4, self.quarter(self.c)
        return target, (slot, *part), (j, *part)

    def half_depth_copy(self, t):
        target, src, dst = self.half_depth(t)
        return remote(
            self.relay.at[src], self.rows.at[dst], self.bs.at[t], self.br.at[self.s % 4], depth=target
        )

    def half_depth_send(self):
        for t in range(4):
            if t:
                self.half_col(t, (self.c - t) % 4, self.c).wait_recv()
            target, src, dst = self.half_depth(t)

            @pl.when(target != self.s)
            def _():
                self.half_depth_copy(t).start()

            @pl.when(target == self.s)
            def _():
                self.rows[dst] = self.relay[src]

    def half_all(self, t, a):
        ref = self.rows.at[(slice(None), *self.quarter(a))]
        return remote(ref, ref, self.es.at[t], self.er.at[t], col=(self.c + t) % 4)

    def half_all_send(self):
        for j in range(4):
            source = 4 * (self.s % 2) + j
            ref = self.rows.at[(j, *self.quarter(self.c))]

            @pl.when(source != self.s)
            def _():
                remote(ref, ref, self.bs.at[0], self.br.at[j], depth=source).wait_recv()

        for t in (1, 3, 2):
            self.half_all(t, self.c).start()

    def half_all_wait(self):
        for t in (1, 3, 2):
            self.half_all(t, (self.c - t) % 4).wait_recv()

    def corner_case(self, rows, i, act):
        here = jnp.logical_and(self.c == 0, self.s == i)
        if rows is not None:
            here = jnp.logical_and(here, jnp.logical_and(self.r >= rows[0], self.r <= rows[-1]))

        @pl.when(here)
        def _():
            act()

    def win_main(self, i, t):
        n = 16 if t < 3 else 15 - i
        return remote(
            self.wsrc.at[i + 16 * t : i + 16 * t + n], self.wq.at[0:n], self.w1s.at[t], self.w1r.at[0], row=t
        )

    def win_head(self, i):
        return remote(self.wsrc.at[0:i], self.hq.at[0:i], self.w1s.at[4], self.w1r.at[1], row=3)

    def win_scatter(self, act):
        def copies(i):
            if i < 4:
                for t in range(1, 4):
                    act(self.win_main(i, t))
            if i > 0:
                act(self.win_head(i))

        for i in range(5):
            self.corner_case((0,), i, lambda: copies(i))

    def win_scatter_send(self):
        @pl.when(jnp.logical_and(self.corner, self.s < 5))
        def _():
            for u in range(63):
                self.wsrc[u] = self.relay[0, 4 * u : 4 * u + 4, :]

        self.win_scatter(lambda copy: copy.start())

    def win_scatter_wait(self):
        for i in range(5):
            if i < 4:
                self.corner_case((1, 2), i, lambda: self.win_main(i, 1).wait_recv())
                self.corner_case((3,), i, lambda: self.win_main(i, 3).wait_recv())
            if i > 0:
                self.corner_case((3,), i, lambda: self.win_head(i).wait_recv())

    def win_piece(self, rows, i, d):
        n = 2 if rows[0] < 3 else min(max(15 - i - 2 * d, 0), 2)
        if n == 0:
            return None
        src = self.wsrc.at[i + 2 * d : i + 2 * d + n] if rows[0] == 0 else self.wq.at[2 * d : 2 * d + n]
        dst = self.pw.at[i, 0:n]
        return src, dst, lambda: remote(src, dst, self.w2s.at[d], self.w2r.at[i], depth=d)

    def win_head_piece(self, c, d):
        first, last = max(0, 2 * d - 15 + c), min(c + 1, 2 * d - 13 + c)
        if d < 6 or first >= last:
            return None
        slot = (15 - c + first) % 2
        return remote(
            self.hq.at[first:last],
            self.pw.at[c, slot : slot + last - first],
            self.w2s.at[2 + d],
            self.w2r.at[4 + c],
            depth=d,
        )

    def win_spread(self, act, local=False):
        def copies(rows, i):
            for d in range(8):
                if i < 4:
                    piece = self.win_piece(rows, i, d)
                    if piece and d != i:
                        act(piece[2]())
                    elif piece and local:
                        piece[1][...] = piece[0][...]
                if i > 0 and rows[0] == 3:
                    copy = self.win_head_piece(i - 1, d)
                    if copy:
                        act(copy)

        for i in range(5):
            for rows in ((0,), (1, 2), (3,)):
                self.corner_case(rows, i, lambda: copies(rows, i))

    def win_spread_send(self):
        self.win_spread(lambda copy: copy.start(), local=True)

    def win_spread_wait(self):
        def waits(rows, d):
            for i in range(4):
                piece = self.win_piece(rows, i, d)
                if piece and d != i:
                    piece[2]().wait_recv()
                if rows[0] == 3:
                    copy = self.win_head_piece(i, d)
                    if copy:
                        copy.wait_recv()

        for d in range(8):
            for rows in ((0, 1, 2), (3,)):
                self.corner_case(rows, d, lambda: waits(rows, d))

    def win_col(self, t):
        return remote(self.pw.at[t], self.win.at[self.s, self.r], self.w3s.at[t], self.w3r.at[0], col=t)

    def win_col_send(self):
        @pl.when(self.c == 0)
        def _():
            for t in range(1, 4):
                self.win_col(t).start()
            self.win[self.s, self.r] = self.pw[0]

    def win_col_wait(self):
        @pl.when(self.c != 0)
        def _():
            self.win_col(1).wait_recv()

    def win_depth(self, t, d):
        ref = self.win.at[d, self.r]
        return remote(ref, ref, self.w4s.at[t], self.w4r.at[t], depth=(self.s + t) % 8)

    def win_depth_send(self):
        for t in range(1, 8):
            self.win_depth(t, self.s).start()

    def win_depth_wait(self):
        for t in range(1, 8):
            self.win_depth(t, (self.s - t) % 8).wait_recv()

    def win_all(self, t, row):
        ref = self.win.at[:, row]
        return remote(ref, ref, self.w5s.at[t], self.w5r.at[t], row=(self.r + t) % 4)

    def win_all_send(self):
        for t in range(1, 4):
            self.win_all(t, self.r).start()

    def win_all_wait(self):
        for t in range(1, 4):
            self.win_all(t, (self.r - t) % 4).wait_recv()

    def leave(self):
        for t in range(1, 8):
            self.win_depth(t, self.s).wait_send()
        for part in range(2):
            self.diag_depth_each(part, lambda copy: copy.wait_send())
        for b in range(4):
            self.diag_row_each(b, lambda copy: copy.wait_send())
        for t in range(1, 4):
            self.diag_col(t, self.c).wait_send()
            self.win_all(t, self.r).wait_send()
        for t in range(4):
            if t:
                self.half_col(t, self.c, (self.c + t) % 4).wait_send()
                self.half_all(t, self.c).wait_send()
            target = self.half_depth(t)[0]

            @pl.when(target != self.s)
            def _():
                self.half_depth_copy(t).wait_send()

        for b in range(2):
            for t in range(4):
                if t:
                    self.rows_col(t, self.c, b).wait_send()
                target, copy = self.rows_depth(t, (self.c - t) % 4, b)

                @pl.when(target != self.s)
                def _():
                    copy.wait_send()

        self.win_scatter(lambda copy: copy.wait_send())
        self.win_spread(lambda copy: copy.wait_send())

        @pl.when(self.c == 0)
        def _():
            for t in range(1, 4):
                self.win_col(t).wait_send()


SEMAPHORES = ((3,), (8, 2), (8, 2), (4,), (4,), (4, 4), (4, 4), (4, 2), (4, 2), (4, 2), (4, 2),
              (5,), (2,), (10,), (8,), (4,), (1,), (8,), (8,), (4,), (4,),
              (4,), (4,), (4,), (4,), (4,), (4,))


def kernel(
    diag_in, panel, trailing_in, own_l, solved, updated,
    own, dbuf, relay, rows, win, wsrc, wq, hq, pw, diag, window, l, trailing, *sems,
):
    e = Exchange(diag_in, panel, own, dbuf, relay, rows, win, wsrc, wq, hq, pw, sems)
    f = Factor(diag, l)

    def assemble(i, b):
        e.diag_row_wait(i, b)
        for c in range(4):
            for s in range(8):
                first = 128 * i + 32 * c + 4 * s
                diag[first : first + 4, at(b)] = dbuf[i, c, s, :, at(b)]

    def assemble_column(b):
        for i in range(b, 4):
            if i > 0:
                assemble(i, b)

    own_trailing = pltpu.make_async_copy(trailing_in, trailing, sems[0].at[2])
    own_trailing.start()
    e.enter()
    e.diag_col_send()
    e.half_col_send()
    e.rows_col_send(0)
    e.win_scatter_send()
    e.rows_col_send(1)
    e.diag_col_wait()
    e.diag_depth_send(0)
    e.diag_depth_send(1)
    e.half_depth_send()
    e.diag_depth_wait(0)
    e.diag_row_send(0)
    e.win_scatter_wait()
    e.win_spread_send()
    e.diag_depth_wait(1)
    e.diag_row_send(1)
    e.diag_row_send(2)
    e.diag_row_send(3)
    e.rows_depth_send(0, e.c, 0)
    e.rows_pass(0)
    assemble(0, 0)
    e.win_spread_wait()
    e.win_col_send()

    def first_hook():
        e.half_all_send()

    f.block(0, between=first_hook)
    e.win_col_wait()
    e.win_depth_send()
    e.rows_depth_send(0, e.c, 1)
    e.rows_pass(1)
    assemble_column(0)
    f.rest(0)
    assemble_column(1)

    size = panel.shape[0]
    own_a, window_a, w, total = [], [], [], [None] * 4
    rows_a, rows_x = [[] for _ in range(4)], [[] for _ in range(4)]

    def own_task(h):
        def task():
            own_a.append(split(own[:, half(h)]))
            solved[:, half(h)] = f.solved(own_a, h)

        return task

    def row_load(j, h):
        return lambda: rows_a[j].append(split(rows[j, 0:size, half(h)]))

    def row_task(j, h):
        return lambda: rows_x[j].append(split(f.solved(rows_a[j], h)))

    def window_load():
        for s in range(8):
            for r in range(4):
                for u in range(2):
                    first = 64 * r + 8 * s + 4 * u
                    window[first : first + 4, :] = win[s, r, u]
        for h in range(2):
            window_a.append(split(window[:, half(h)]))

    def window_task(h):
        return lambda: w.append(split(f.solved(window_a, h)))

    def product_task(j, h):
        def task():
            term = dot(rows_x[j][h], w[h])
            total[j] = term if total[j] is None else total[j] + term

        return task

    f.block(1, [f.prepare(1, 2), f.prepare(1, 3)])
    e.win_depth_wait()
    e.win_all_send()
    f.rest(1)
    assemble_column(2)
    f.block(2, [f.prepare(2, 3), f.inverse_sum(1), f.inverse_row(1), f.inverse_sum(2), own_task(0)])
    f.rest(2)
    assemble_column(3)

    def last_hook():
        e.rows_wait(0)
        e.rows_wait(1)
        e.half_all_wait()
        e.win_all_wait()

    f.block(
        3,
        [f.inverse_row(2), f.inverse_sum(3)],
        last_hook,
        [window_load, window_task(0)]
        + [t(j, 0) for j in range(4) for t in (row_load, row_task)]
        + [product_task(j, 0) for j in range(4)]
        + [row_load(j, 1) for j in range(4)],
    )
    f.inverse_row(3)()
    window_task(1)()
    own_trailing.wait()
    for j in range(4):
        row_task(j, 1)()
        product_task(j, 1)()
        span = slice(size * j, size * (j + 1))
        updated[span, :] = trailing[span, :] - total[j]
    own_task(1)()
    position = (e.r * 4 + e.c) * 8 + e.s
    pair = l[pl.ds(pl.multiple_of((position // 2) * 8, 8), 8), :]
    own_l[...] = jnp.where(position % 2 == 0, pair[0:4], pair[4:8])
    e.leave()


def deliver(own_l, solved, updated, own_l_out, solved_out, updated_out, sem):
    copies = [
        pltpu.make_async_copy(src, dst, sem.at[i])
        for i, (src, dst) in enumerate(((own_l, own_l_out), (solved, solved_out), (updated, updated_out)))
    ]
    for copy in copies:
        copy.start()
    for copy in copies:
        copy.wait()


def body(diag_block, panel_rows, trailing):
    vmem = pl.BlockSpec(memory_space=pltpu.VMEM)
    hbm = pl.BlockSpec(memory_space=pltpu.HBM)
    shapes = (
        panel_rows.shape,
        (4, 4, 8, 4, 512),
        (4, 256, 512),
        (4, 256, 512),
        (8, 4, 2, 4, 512),
        (63, 4, 512),
        (16, 4, 512),
        (4, 4, 512),
        (4, 2, 4, 512),
        (512, 512),
        (256, 512),
        (512, 512),
        trailing.shape,
    )
    outs = tuple(jax.ShapeDtypeStruct(a.shape, F32) for a in (diag_block, panel_rows, trailing))
    results = pl.pallas_call(
        kernel,
        out_shape=outs,
        in_specs=[hbm] * 3,
        out_specs=(vmem,) * 3,
        scratch_shapes=[pltpu.VMEM(shape, F32) for shape in shapes]
        + [pltpu.SemaphoreType.DMA(n) for n in SEMAPHORES],
        compiler_params=pltpu.CompilerParams(
            collective_id=0, has_side_effects=True, vmem_limit_bytes=VMEM_LIMIT
        ),
        name="panel_step",
    )(*(pltpu.with_memory_space_constraint(x, pltpu.HBM) for x in (diag_block, panel_rows, trailing)))
    return pl.pallas_call(
        deliver,
        out_shape=outs,
        in_specs=[vmem] * 3,
        out_specs=(hbm,) * 3,
        scratch_shapes=[pltpu.SemaphoreType.DMA((3,))],
        compiler_params=pltpu.CompilerParams(vmem_limit_bytes=2 * 2**20),
        name="deliver",
    )(*results)


VMEM_LIMIT = 44 * 2**20


def solution(mesh):
    specs = (P(ALL, None), P(ALL, None), P(("row", "depth"), "col"))
    return jax.shard_map(body, mesh=mesh, in_specs=specs, out_specs=specs, check_vma=False)
```

```python
import jax
import jax.numpy as jnp
from jax import lax
from jax.experimental import pallas as pl
from jax.experimental.pallas import tpu as pltpu
from jax.sharding import PartitionSpec as P

ALL = ("row", "col", "depth")
F32 = jnp.float32
NT = (((1,), (1,)), ((), ()))
NN = (((1,), (0,)), ((), ()))
BLOCK = 128
NEAR = 4
MESH = pl.DeviceIdType.MESH


def at(i):
    return slice(BLOCK * i, BLOCK * (i + 1))


PIECES = (((0, 1), slice(0, 256)), ((2,), slice(256, 384)), ((3,), slice(384, 512)))


def split(x):
    hi = x.astype(jnp.bfloat16)
    return hi, (x - hi.astype(F32)).astype(jnp.bfloat16)


def dot(a, b, dims=NT):
    left = jnp.concatenate([a[0], a[1], a[0]], 1)
    right = jnp.concatenate([b[0], b[0], b[1]], dims[0][1][0])
    return lax.dot_general(left, right, dims, preferred_element_type=F32)


def beside(parts, axis=1):
    return tuple(jnp.concatenate(x, axis) if len(x) > 1 else x[0] for x in zip(*parts))


def sub(v, k):
    return jnp.broadcast_to(v[k : k + 1, :], (8, 128))


class Block:
    def __init__(self, rows):
        self.ri = lax.broadcasted_iota(jnp.int32, (8, 128), 0)
        self.li = lax.broadcasted_iota(jnp.int32, (8, 128), 1)
        self.rows = rows
        self.upper, self.inverse = [], []

    def advance(self, p):
        ri, li, rows = self.ri, self.li, self.rows
        first = 8 * p
        raw = [jnp.broadcast_to(rows[:, :, first + j : first + j + 1], rows.shape) for j in range(8)]
        e = {(i, j): sub(raw[j][0], i) for j in range(8) for i in range(j, 8)}
        near = min(NEAR + 1, rows.shape[0])
        cols = [x[1:near] for x in raw]
        scales, factors = [], []
        r = [sub(rows[0], k) for k in range(8)]
        s = [jnp.where(li < first, r[k], jnp.where(li == first + k, 1.0, 0.0)) for k in range(8)]
        for k in range(8):
            inv = lax.rsqrt(e[k, k])
            m = {j: e[j, k] * inv for j in range(k + 1, 8)}
            for j in range(k + 1, 8):
                for i in range(j, 8):
                    e[i, j] = e[i, j] - m[i] * m[j]
            scales.append(inv)
            factors.append(m)
            if near > 1:
                cols[k] = cols[k] * inv
            r[k] = r[k] * inv
            s[k] = s[k] * inv
            for j in range(k + 1, 8):
                if near > 1:
                    cols[j] = cols[j] - cols[k] * m[j]
                r[j] = r[j] - m[j] * r[k]
                s[j] = s[j] - m[j] * s[k]
        u, t = r[0], s[0]
        for k in range(1, 8):
            u = jnp.where(ri == k, r[k], u)
            t = jnp.where(ri == k, s[k], t)
        self.upper.append(jnp.where(li >= ri + first, u, 0.0))
        self.inverse.append(t)
        if p < 15:
            rows = jnp.where(((li < first) | (li >= first + 8))[None], rows[1:], 0.0)
            both = [jnp.where(li < first + 8, s[k], r[k]) for k in range(8)]
            close, parts = rows[: near - 1], []
            for k in range(8):
                close = close - cols[k] * both[k]
            parts.append(close)
            if rows.shape[0] > near - 1:
                for k in range(7, -1, -1):
                    for j in range(k + 1, 8):
                        both[k] = both[k] - factors[k][j] * both[j]
                    both[k] = both[k] * scales[k]
                far = rows[near - 1 :]
                for k in range(8):
                    far = far - raw[k][near:] * both[k]
                parts.append(far)
            rows = jnp.concatenate(parts, 0) if len(parts) > 1 else close
            self.rows = rows


class Factor:
    def __init__(self, a, l):
        self.a, self.l = a, l
        self.lows, self.inv, self.inv_rows, self.below, self.sums = {}, {}, {}, {}, {}

    def low_row(self, i, n):
        return beside([self.lows[i, m] for m in range(n)])

    def column(self, k, i):
        value = self.a[at(i), at(k)]
        return value - dot(self.low_row(i, k), self.low_row(k, k)) if k else value

    def block(self, k, tasks=(), between=lambda: None, late=()):
        value = self.column(k, k)
        b = Block(value.reshape(16, 8, 128))
        tasks = [list(tasks), list(late)]
        for p in range(16):
            b.advance(p)
            half = tasks[p // 8 if late else 0]
            for _ in range(-(-len(half) // ((8 if late and p < 8 else 16) - p))):
                half.pop(0)()
            if p == 7:
                between()
        self.inv[k] = split(jnp.concatenate(b.inverse, 0))
        if k == 0:
            self.inv_rows[0] = self.inv[0]
        self.l[at(k), at(k)] = jnp.concatenate(b.upper, 0).T
        for j in range(k + 1, 4):
            self.l[at(k), at(j)] = jnp.zeros((BLOCK, BLOCK), F32)

    def prepare(self, k, i):
        def task():
            self.below[i] = split(self.column(k, i))

        return task

    def rest(self, k):
        for i in range(k + 1, 4):
            if i not in self.below:
                self.prepare(k, i)()
            low = dot(self.below.pop(i), self.inv[k])
            self.l[at(i), at(k)] = low
            self.lows[i, k] = split(low)

    def inverse_rows(self, rows, width):
        parts = []
        for k in rows:
            fill = jnp.zeros((BLOCK, width - BLOCK * (k + 1)), jnp.bfloat16)
            parts.append(beside([self.inv_rows[k], (fill, fill)]) if fill.shape[1] else self.inv_rows[k])
        return beside(parts, 0)

    def inverse_sum(self, k):
        def task():
            total = dot(self.low_row(k, k), self.inverse_rows(range(k), BLOCK * k), NN)
            self.sums[k] = split(total)

        return task

    def inverse_row(self, k):
        def task():
            left = split(-dot(self.inv[k], self.sums.pop(k), NN))
            self.inv_rows[k] = beside([left, self.inv[k]])

        return task

    def solved(self, x, g):
        blocks = PIECES[g][0]
        return dot(beside(x[: g + 1]), self.inverse_rows(blocks, BLOCK * (blocks[-1] + 1)))


def remote(src, dst, send, recv, **device):
    return pltpu.make_async_remote_copy(
        src_ref=src, dst_ref=dst, send_sem=send, recv_sem=recv, device_id=device, device_id_type=MESH
    )


class Exchange:
    def __init__(self, diag, panel, own, dbuf, relay, rows, win, wsrc, wq, hq, pw, sems):
        self.diag, self.panel, self.own, self.dbuf, self.relay, self.rows = diag, panel, own, dbuf, relay, rows
        self.win, self.wsrc, self.wq, self.hq, self.pw = win, wsrc, wq, hq, pw
        (self.loc, self.ds, self.dr, self.cs, self.cr, self.rs, self.rr, self.zs, self.zr, self.xs, self.xr,
         self.w1s, self.w1r, self.w2s, self.w2r, self.w3s, self.w3r, self.w4s, self.w4r, self.w5s, self.w5r,
         self.as_, self.ar, self.bs, self.br, self.es, self.er) = sems
        self.r, self.c, self.s = (lax.axis_index(a) for a in ALL)
        self.corner = jnp.logical_and(self.r == 0, self.c == 0)

    def enter(self):
        r, c, s = self.r, self.c, self.s
        self.own_diag = pltpu.make_async_copy(self.diag, self.dbuf.at[r, c, s], self.loc.at[0])
        self.own_panel = pltpu.make_async_copy(self.panel, self.own, self.loc.at[1])
        self.own_diag.start()
        self.own_panel.start()
        barrier = pltpu.get_barrier_semaphore()
        for axis, me, n in (("depth", s, 8), ("col", c, 4), ("row", r, 4)):
            for t in range(1, n):
                pl.semaphore_signal(barrier, inc=1, device_id={axis: (me + t) % n}, device_id_type=MESH)
        self.own_panel.wait()
        n = self.own.shape[0]
        self.relay[c, 0:n] = self.own[...]
        self.relay[c, n:256] = jnp.zeros((256 - n, 512), F32)
        pl.semaphore_wait(barrier, 13)
        self.own_diag.wait()

    def diag_col(self, t, c):
        ref = self.dbuf.at[self.r, c, self.s]
        return remote(ref, ref, self.cs.at[t], self.cr.at[t], col=(self.c + t) % 4)

    def diag_col_send(self):
        for t in range(1, 4):
            self.diag_col(t, self.c).start()

    def diag_col_wait(self):
        for t in range(1, 4):
            self.diag_col(t, (self.c - t) % 4).wait_recv()

    def by_row(self, act):
        for i in range(4):

            @pl.when(self.r == i)
            def _():
                act(i)

    def diag_depth(self, t, s, i, part):
        cols = slice(0, 128) if part == 0 else slice(128, 128 * (i + 1))
        ref = self.dbuf.at[i, :, s, :, cols]
        return remote(ref, ref, self.ds.at[t, part], self.dr.at[t, part], depth=(self.s + t) % 8)

    def diag_depth_each(self, part, act, receive=False):
        def at_row(i):
            if i >= part:
                for t in range(1, 8):
                    act(self.diag_depth(t, (self.s - t) % 8 if receive else self.s, i, part))

        self.by_row(at_row)

    def diag_depth_send(self, part):
        self.diag_depth_each(part, lambda copy: copy.start())

    def diag_depth_wait(self, part):
        self.diag_depth_each(part, lambda copy: copy.wait_recv(), receive=True)

    def diag_row(self, t, i, b):
        ref = self.dbuf.at[i, :, :, :, at(b)]
        return remote(ref, ref, self.rs.at[t, b], self.rr.at[t, b], row=(self.r + t) % 4)

    def diag_row_each(self, b, act):
        def at_row(i):
            if i >= b:
                for t in range(1, 4):
                    act(self.diag_row(t, i, b))

        self.by_row(at_row)

    def diag_row_send(self, b):
        self.diag_row_each(b, lambda copy: copy.start())

    def diag_first_send(self, rows):
        for i in rows:

            @pl.when(self.r == i)
            def _():
                for t in range(1, 4):
                    self.diag_row(t, i, 0).start()

    def diag_row_wait(self, src, b):
        def at_row(i):
            if i != src:
                self.diag_row((i - src) % 4, src, b).wait_recv()

        self.by_row(at_row)

    def rows_col(self, t, slot, b):
        ref = self.relay.at[slot, :, at(b)]
        return remote(ref, ref, self.zs.at[t, b], self.zr.at[t, b], col=(self.c + t) % 4)

    def rows_far_half(self, t, slot, b):
        ref = self.relay.at[slot, at((t - 1) // 2), at(b)]
        return remote(ref, ref, self.zs.at[t - 1, b], self.zr.at[t - 1, b], col=(self.c + t) % 4)

    def rows_col_send(self, b):
        for t in (1, 3):
            self.rows_col(t, self.c, b).start()

    def rows_near(self, b):
        for t in (1, 3):
            slot = (self.c - t) % 4
            self.rows_col(t, slot, b).wait_recv()
            self.rows_far_half(t, slot, b).start()

    def rows_near_pass(self, b):
        for t in (1, 3):
            self.rows_depth_send(t, (self.c - t) % 4, b)

    def rows_far_pass(self, b):
        slot = (self.c + 2) % 4
        for t in (1, 3):
            self.rows_far_half(t, slot, b).wait_recv()
        self.rows_depth_send(2, slot, b)

    def rows_depth(self, t, slot, b):
        target, j = 2 * slot + self.s // 4, self.s % 4
        return target, remote(
            self.relay.at[slot, :, at(b)], self.rows.at[j, :, at(b)], self.xs.at[t, b], self.xr.at[j, b], depth=target
        )

    def rows_depth_send(self, t, slot, b):
        target, copy = self.rows_depth(t, slot, b)

        @pl.when(target != self.s)
        def _():
            copy.start()

        @pl.when(target == self.s)
        def _():
            self.rows[self.s % 4, :, at(b)] = self.relay[slot, :, at(b)]

    def rows_wait(self, b):
        for j in range(4):
            source = 4 * (self.s % 2) + j
            ref = self.rows.at[j, :, at(b)]

            @pl.when(source != self.s)
            def _():
                remote(ref, ref, self.xs.at[0, b], self.xr.at[j, b], depth=source).wait_recv()

    def quarter(self, a):
        return pl.ds(pl.multiple_of(64 * a, 64), 64), slice(256, 512)

    def half_col(self, t, slot, a):
        ref = self.relay.at[(slot, *self.quarter(a))]
        return remote(ref, ref, self.as_.at[t], self.ar.at[t], col=(self.c + t) % 4)

    def half_col_send(self):
        for t in (1, 3, 2):
            self.half_col(t, self.c, (self.c + t) % 4).start()

    def half_depth(self, t):
        slot = (self.c - t) % 4
        target, j, part = 2 * slot + self.s // 4, self.s % 4, self.quarter(self.c)
        return target, (slot, *part), (j, *part)

    def half_depth_copy(self, t):
        target, src, dst = self.half_depth(t)
        return remote(
            self.relay.at[src], self.rows.at[dst], self.bs.at[t], self.br.at[self.s % 4], depth=target
        )

    def half_depth_send(self):
        for t in range(4):
            if t:
                self.half_col(t, (self.c - t) % 4, self.c).wait_recv()
            target, src, dst = self.half_depth(t)

            @pl.when(target != self.s)
            def _():
                self.half_depth_copy(t).start()

            @pl.when(target == self.s)
            def _():
                self.rows[dst] = self.relay[src]

    def half_all(self, t, a):
        ref = self.rows.at[(slice(None), *self.quarter(a))]
        return remote(ref, ref, self.es.at[t], self.er.at[t], col=(self.c + t) % 4)

    def half_all_send(self):
        for j in range(4):
            source = 4 * (self.s % 2) + j
            ref = self.rows.at[(j, *self.quarter(self.c))]

            @pl.when(source != self.s)
            def _():
                remote(ref, ref, self.bs.at[0], self.br.at[j], depth=source).wait_recv()

        for t in (1, 3):
            self.half_all(t, self.c).start()

    def half_far_half(self, t, a):
        ref = self.rows.at[(slice(t - 1, t + 1), *self.quarter(a))]
        return remote(ref, ref, self.es.at[t - 1], self.er.at[t - 1], col=(self.c + t) % 4)

    def half_all_near(self):
        for t in (1, 3):
            a = (self.c - t) % 4
            self.half_all(t, a).wait_recv()
            self.half_far_half(t, a).start()

    def half_all_far(self):
        for t in (1, 3):
            self.half_far_half(t, (self.c + 2) % 4).wait_recv()

    def corner_case(self, rows, i, act):
        here = jnp.logical_and(self.c == 0, self.s == i)
        if rows is not None:
            here = jnp.logical_and(here, jnp.logical_and(self.r >= rows[0], self.r <= rows[-1]))

        @pl.when(here)
        def _():
            act()

    def win_main(self, i, t):
        n = 16 if t < 3 else 15 - i
        return remote(
            self.wsrc.at[i + 16 * t : i + 16 * t + n], self.wq.at[0:n], self.w1s.at[t], self.w1r.at[0], row=t
        )

    def win_head(self, i):
        return remote(self.wsrc.at[0:i], self.hq.at[0:i], self.w1s.at[4], self.w1r.at[1], row=3)

    def win_scatter(self, act):
        def copies(i):
            if i < 4:
                for t in range(1, 4):
                    act(self.win_main(i, t))
            if i > 0:
                act(self.win_head(i))

        for i in range(5):
            self.corner_case((0,), i, lambda: copies(i))

    def win_scatter_send(self):
        @pl.when(jnp.logical_and(self.corner, self.s < 5))
        def _():
            for u in range(63):
                self.wsrc[u] = self.relay[0, 4 * u : 4 * u + 4, :]

        self.win_scatter(lambda copy: copy.start())

    def win_scatter_wait(self):
        for i in range(5):
            if i < 4:
                self.corner_case((1, 2), i, lambda: self.win_main(i, 1).wait_recv())
                self.corner_case((3,), i, lambda: self.win_main(i, 3).wait_recv())
            if i > 0:
                self.corner_case((3,), i, lambda: self.win_head(i).wait_recv())

    def win_piece(self, rows, i, d):
        n = 2 if rows[0] < 3 else min(max(15 - i - 2 * d, 0), 2)
        if n == 0:
            return None
        src = self.wsrc.at[i + 2 * d : i + 2 * d + n] if rows[0] == 0 else self.wq.at[2 * d : 2 * d + n]
        dst = self.pw.at[i, 0:n]
        return src, dst, lambda: remote(src, dst, self.w2s.at[d], self.w2r.at[i], depth=d)

    def win_head_piece(self, c, d):
        first, last = max(0, 2 * d - 15 + c), min(c + 1, 2 * d - 13 + c)
        if d < 6 or first >= last:
            return None
        slot = (15 - c + first) % 2
        return remote(
            self.hq.at[first:last],
            self.pw.at[c, slot : slot + last - first],
            self.w2s.at[2 + d],
            self.w2r.at[4 + c],
            depth=d,
        )

    def win_spread(self, act, local=False):
        def copies(rows, i):
            for d in range(8):
                if i < 4:
                    piece = self.win_piece(rows, i, d)
                    if piece and d != i:
                        act(piece[2]())
                    elif piece and local:
                        piece[1][...] = piece[0][...]
                if i > 0 and rows[0] == 3:
                    copy = self.win_head_piece(i - 1, d)
                    if copy:
                        act(copy)

        for i in range(5):
            for rows in ((0,), (1, 2), (3,)):
                self.corner_case(rows, i, lambda: copies(rows, i))

    def win_spread_send(self):
        self.win_spread(lambda copy: copy.start(), local=True)

    def win_spread_wait(self):
        def waits(rows, d):
            for i in range(4):
                piece = self.win_piece(rows, i, d)
                if piece and d != i:
                    piece[2]().wait_recv()
                if rows[0] == 3:
                    copy = self.win_head_piece(i, d)
                    if copy:
                        copy.wait_recv()

        for d in range(8):
            for rows in ((0, 1, 2), (3,)):
                self.corner_case(rows, d, lambda: waits(rows, d))

    def win_col(self, t):
        return remote(self.pw.at[t], self.win.at[self.s, self.r], self.w3s.at[t], self.w3r.at[0], col=t)

    def win_col_send(self):
        @pl.when(self.c == 0)
        def _():
            for t in range(1, 4):
                self.win_col(t).start()
            self.win[self.s, self.r] = self.pw[0]

    def win_col_wait(self):
        @pl.when(self.c != 0)
        def _():
            self.win_col(1).wait_recv()

    def win_depth(self, t, d):
        ref = self.win.at[d, self.r]
        return remote(ref, ref, self.w4s.at[t], self.w4r.at[t], depth=(self.s + t) % 8)

    def win_depth_send(self):
        for t in range(1, 8):
            self.win_depth(t, self.s).start()

    def win_depth_wait(self):
        for t in range(1, 8):
            self.win_depth(t, (self.s - t) % 8).wait_recv()

    def win_all(self, t, row):
        ref = self.win.at[:, row]
        return remote(ref, ref, self.w5s.at[t], self.w5r.at[t], row=(self.r + t) % 4)

    def win_all_send(self):
        for t in range(1, 4):
            self.win_all(t, self.r).start()

    def win_all_wait(self):
        for t in range(1, 4):
            self.win_all(t, (self.r - t) % 4).wait_recv()

    def leave(self):
        for t in range(1, 8):
            self.win_depth(t, self.s).wait_send()
        for part in range(2):
            self.diag_depth_each(part, lambda copy: copy.wait_send())
        for b in range(4):
            self.diag_row_each(b, lambda copy: copy.wait_send())
        for t in range(1, 4):
            self.diag_col(t, self.c).wait_send()
            self.win_all(t, self.r).wait_send()
        for t in range(4):
            if t:
                self.half_col(t, self.c, (self.c + t) % 4).wait_send()
            if t % 2:
                self.half_all(t, self.c).wait_send()
                self.half_far_half(t, (self.c - t) % 4).wait_send()
            target = self.half_depth(t)[0]

            @pl.when(target != self.s)
            def _():
                self.half_depth_copy(t).wait_send()

        for b in range(2):
            for t in range(4):
                if t % 2:
                    self.rows_col(t, self.c, b).wait_send()
                    self.rows_far_half(t, (self.c - t) % 4, b).wait_send()
                target, copy = self.rows_depth(t, (self.c - t) % 4, b)

                @pl.when(target != self.s)
                def _():
                    copy.wait_send()

        self.win_scatter(lambda copy: copy.wait_send())
        self.win_spread(lambda copy: copy.wait_send())

        @pl.when(self.c == 0)
        def _():
            for t in range(1, 4):
                self.win_col(t).wait_send()


SEMAPHORES = ((3,), (8, 2), (8, 2), (4,), (4,), (4, 4), (4, 4), (4, 2), (4, 2), (4, 2), (4, 2),
              (5,), (2,), (10,), (8,), (4,), (1,), (8,), (8,), (4,), (4,),
              (4,), (4,), (4,), (4,), (4,), (4,))


def kernel(
    diag_in, panel, trailing_in, own_l, solved, updated,
    own, dbuf, relay, rows, win, wsrc, wq, hq, pw, diag, window, l, trailing, *sems,
):
    e = Exchange(diag_in, panel, own, dbuf, relay, rows, win, wsrc, wq, hq, pw, sems)
    f = Factor(diag, l)

    def assemble(i, b):
        e.diag_row_wait(i, b)
        for c in range(4):
            for s in range(8):
                first = 128 * i + 32 * c + 4 * s
                diag[first : first + 4, at(b)] = dbuf[i, c, s, :, at(b)]

    def assemble_column(b):
        for i in range(b, 4):
            if i > 0:
                assemble(i, b)

    own_trailing = pltpu.make_async_copy(trailing_in, trailing, sems[0].at[2])
    own_trailing.start()
    e.enter()
    e.diag_col_send()
    e.half_col_send()
    e.rows_col_send(0)
    e.win_scatter_send()
    e.rows_col_send(1)
    e.diag_col_wait()
    e.diag_depth_send(0)
    e.diag_depth_send(1)
    e.half_depth_send()
    e.diag_depth_wait(0)
    e.diag_first_send((0,))
    e.win_scatter_wait()
    e.win_spread_send()
    e.diag_depth_wait(1)
    e.rows_depth_send(0, e.c, 0)
    e.rows_near(0)
    e.rows_near_pass(0)
    e.diag_first_send((1, 2, 3))
    e.diag_row_send(1)
    e.diag_row_send(2)
    e.diag_row_send(3)
    assemble(0, 0)
    e.win_spread_wait()
    e.win_col_send()
    e.rows_near(1)
    e.half_all_send()
    f.block(0)
    e.win_col_wait()
    e.win_depth_send()
    e.rows_far_pass(0)
    e.rows_depth_send(0, e.c, 1)
    e.rows_near_pass(1)
    assemble_column(0)
    f.rest(0)
    assemble_column(1)

    size = panel.shape[0]
    own_a, window_a, w, total = [], [], [], [None] * 4
    rows_a, rows_x = [[] for _ in range(4)], [[] for _ in range(4)]

    def own_task(g):
        def task():
            own_a.append(split(own[:, PIECES[g][1]]))
            solved[:, PIECES[g][1]] = f.solved(own_a, g)

        return task

    def row_load(j, g):
        return lambda: rows_a[j].append(split(rows[j, 0:size, PIECES[g][1]]))

    def row_task(j, g):
        return lambda: rows_x[j].append(split(f.solved(rows_a[j], g)))

    def window_load():
        for s in range(8):
            for r in range(4):
                for u in range(2):
                    first = 64 * r + 8 * s + 4 * u
                    window[first : first + 4, :] = win[s, r, u]
        for _, columns in PIECES:
            window_a.append(split(window[:, columns]))

    def window_task(g):
        return lambda: w.append(split(f.solved(window_a, g)))

    def product_task(j, g):
        def task():
            term = dot(rows_x[j][g], w[g])
            total[j] = term if total[j] is None else total[j] + term

        return task

    def second_hook():
        e.rows_far_pass(1)

    f.block(1, [f.prepare(1, 2), f.prepare(1, 3)], second_hook)
    e.win_depth_wait()
    e.win_all_send()
    e.half_all_near()
    f.rest(1)
    assemble_column(2)
    f.block(2, [f.prepare(2, 3), f.inverse_sum(1), f.inverse_row(1), f.inverse_sum(2), own_task(0)])
    f.rest(2)
    assemble_column(3)

    e.rows_wait(0)
    e.rows_wait(1)

    def last_hook():
        e.half_all_far()
        e.win_all_wait()

    f.block(
        3,
        [f.inverse_row(2), f.inverse_sum(3), own_task(1)] + [t(j, 0) for j in range(4) for t in (row_load, row_task)],
        last_hook,
        [window_load, window_task(0), window_task(1)]
        + [t(j, 1) for j in range(4) for t in (row_load, row_task)]
        + [product_task(j, g) for g in range(2) for j in range(4)]
        + [row_load(j, 2) for j in range(4)],
    )
    f.inverse_row(3)()
    window_task(2)()
    own_trailing.wait()
    for j in range(4):
        row_task(j, 2)()
        product_task(j, 2)()
        span = slice(size * j, size * (j + 1))
        updated[span, :] = trailing[span, :] - total[j]
    own_task(2)()
    position = (e.r * 4 + e.c) * 8 + e.s
    pair = l[pl.ds(pl.multiple_of((position // 2) * 8, 8), 8), :]
    own_l[...] = jnp.where(position % 2 == 0, pair[0:4], pair[4:8])
    e.leave()


def deliver(own_l, solved, updated, own_l_out, solved_out, updated_out, sem):
    copies = [
        pltpu.make_async_copy(src, dst, sem.at[i])
        for i, (src, dst) in enumerate(((own_l, own_l_out), (solved, solved_out), (updated, updated_out)))
    ]
    for copy in copies:
        copy.start()
    for copy in copies:
        copy.wait()


def body(diag_block, panel_rows, trailing):
    vmem = pl.BlockSpec(memory_space=pltpu.VMEM)
    hbm = pl.BlockSpec(memory_space=pltpu.HBM)
    shapes = (
        panel_rows.shape,
        (4, 4, 8, 4, 512),
        (4, 256, 512),
        (4, 256, 512),
        (8, 4, 2, 4, 512),
        (63, 4, 512),
        (16, 4, 512),
        (4, 4, 512),
        (4, 2, 4, 512),
        (512, 512),
        (256, 512),
        (512, 512),
        trailing.shape,
    )
    outs = tuple(jax.ShapeDtypeStruct(a.shape, F32) for a in (diag_block, panel_rows, trailing))
    results = pl.pallas_call(
        kernel,
        out_shape=outs,
        in_specs=[hbm] * 3,
        out_specs=(vmem,) * 3,
        scratch_shapes=[pltpu.VMEM(shape, F32) for shape in shapes]
        + [pltpu.SemaphoreType.DMA(n) for n in SEMAPHORES],
        compiler_params=pltpu.CompilerParams(
            collective_id=0, has_side_effects=True, vmem_limit_bytes=VMEM_LIMIT
        ),
        name="panel_step",
    )(*(pltpu.with_memory_space_constraint(x, pltpu.HBM) for x in (diag_block, panel_rows, trailing)))
    return pl.pallas_call(
        deliver,
        out_shape=outs,
        in_specs=[vmem] * 3,
        out_specs=(hbm,) * 3,
        scratch_shapes=[pltpu.SemaphoreType.DMA((3,))],
        compiler_params=pltpu.CompilerParams(vmem_limit_bytes=2 * 2**20),
        name="deliver",
    )(*results)


VMEM_LIMIT = 44 * 2**20


def solution(mesh):
    specs = (P(ALL, None), P(ALL, None), P(("row", "depth"), "col"))
    return jax.shard_map(body, mesh=mesh, in_specs=specs, out_specs=specs, check_vma=False)
```

```python
import jax
import jax.numpy as jnp
from jax import lax
from jax.experimental import pallas as pl
from jax.experimental.pallas import tpu as pltpu
from jax.sharding import PartitionSpec as P

ALL = ("row", "col", "depth")
F32 = jnp.float32
NT = (((1,), (1,)), ((), ()))
NN = (((1,), (0,)), ((), ()))
BLOCK = 128
NEAR = 4
ROWS_AT, LAST_AT = 4, 8
MESH = pl.DeviceIdType.MESH


def at(i):
    return slice(BLOCK * i, BLOCK * (i + 1))


PIECES = (((0, 1), slice(0, 256)), ((2,), slice(256, 384)), ((3,), slice(384, 512)))


def split(x):
    hi = x.astype(jnp.bfloat16)
    return hi, (x - hi.astype(F32)).astype(jnp.bfloat16)


def dot(a, b, dims=NT):
    left = jnp.concatenate([a[0], a[1], a[0]], 1)
    right = jnp.concatenate([b[0], b[0], b[1]], dims[0][1][0])
    return lax.dot_general(left, right, dims, preferred_element_type=F32)


def beside(parts, axis=1):
    return tuple(jnp.concatenate(x, axis) if len(x) > 1 else x[0] for x in zip(*parts))


def sub(v, k):
    return jnp.broadcast_to(v[k : k + 1, :], (8, 128))


class Block:
    def __init__(self, rows):
        self.ri = lax.broadcasted_iota(jnp.int32, (8, 128), 0)
        self.li = lax.broadcasted_iota(jnp.int32, (8, 128), 1)
        self.rows = rows
        self.upper, self.inverse = [], []

    def advance(self, p):
        ri, li, rows = self.ri, self.li, self.rows
        first = 8 * p
        raw = [jnp.broadcast_to(rows[:, :, first + j : first + j + 1], rows.shape) for j in range(8)]
        e = {(i, j): sub(raw[j][0], i) for j in range(8) for i in range(j, 8)}
        near = min(NEAR + 1, rows.shape[0])
        cols = [x[1:near] for x in raw]
        scales, factors = [], []
        r = [sub(rows[0], k) for k in range(8)]
        s = [jnp.where(li < first, r[k], jnp.where(li == first + k, 1.0, 0.0)) for k in range(8)]
        for k in range(8):
            inv = lax.rsqrt(e[k, k])
            m = {j: e[j, k] * inv for j in range(k + 1, 8)}
            for j in range(k + 1, 8):
                for i in range(j, 8):
                    e[i, j] = e[i, j] - m[i] * m[j]
            scales.append(inv)
            factors.append(m)
            if near > 1:
                cols[k] = cols[k] * inv
            r[k] = r[k] * inv
            s[k] = s[k] * inv
            for j in range(k + 1, 8):
                if near > 1:
                    cols[j] = cols[j] - cols[k] * m[j]
                r[j] = r[j] - m[j] * r[k]
                s[j] = s[j] - m[j] * s[k]
        u, t = r[0], s[0]
        for k in range(1, 8):
            u = jnp.where(ri == k, r[k], u)
            t = jnp.where(ri == k, s[k], t)
        self.upper.append(jnp.where(li >= ri + first, u, 0.0))
        self.inverse.append(t)
        if p < 15:
            rows = jnp.where(((li < first) | (li >= first + 8))[None], rows[1:], 0.0)
            both = [jnp.where(li < first + 8, s[k], r[k]) for k in range(8)]
            close, parts = rows[: near - 1], []
            for k in range(8):
                close = close - cols[k] * both[k]
            parts.append(close)
            if rows.shape[0] > near - 1:
                for k in range(7, -1, -1):
                    for j in range(k + 1, 8):
                        both[k] = both[k] - factors[k][j] * both[j]
                    both[k] = both[k] * scales[k]
                far = rows[near - 1 :]
                for k in range(8):
                    far = far - raw[k][near:] * both[k]
                parts.append(far)
            rows = jnp.concatenate(parts, 0) if len(parts) > 1 else close
            self.rows = rows


class Factor:
    def __init__(self, a, l):
        self.a, self.l = a, l
        self.lows, self.inv, self.inv_rows, self.below, self.sums = {}, {}, {}, {}, {}

    def low_row(self, i, n):
        return beside([self.lows[i, m] for m in range(n)])

    def column(self, k, i):
        value = self.a[at(i), at(k)]
        return value - dot(self.low_row(i, k), self.low_row(k, k)) if k else value

    def block(self, k, tasks=(), hooks=()):
        value = self.column(k, k)
        b = Block(value.reshape(16, 8, 128))
        stages = [(0, lambda: None, tasks), *hooks, (16, None, ())]
        for (start, wait, work), (end, _, _) in zip(stages, stages[1:]):
            wait()
            work = list(work)
            for p in range(start, end):
                b.advance(p)
                for _ in range(-(-len(work) // (end - p))):
                    work.pop(0)()
        self.inv[k] = split(jnp.concatenate(b.inverse, 0))
        if k == 0:
            self.inv_rows[0] = self.inv[0]
        self.l[at(k), at(k)] = jnp.concatenate(b.upper, 0).T
        for j in range(k + 1, 4):
            self.l[at(k), at(j)] = jnp.zeros((BLOCK, BLOCK), F32)

    def prepare(self, k, i):
        def task():
            self.below[i] = split(self.column(k, i))

        return task

    def rest(self, k):
        for i in range(k + 1, 4):
            if i not in self.below:
                self.prepare(k, i)()
            low = dot(self.below.pop(i), self.inv[k])
            self.l[at(i), at(k)] = low
            self.lows[i, k] = split(low)

    def inverse_rows(self, rows, width):
        parts = []
        for k in rows:
            fill = jnp.zeros((BLOCK, width - BLOCK * (k + 1)), jnp.bfloat16)
            parts.append(beside([self.inv_rows[k], (fill, fill)]) if fill.shape[1] else self.inv_rows[k])
        return beside(parts, 0)

    def inverse_sum(self, k):
        def task():
            total = dot(self.low_row(k, k), self.inverse_rows(range(k), BLOCK * k), NN)
            self.sums[k] = split(total)

        return task

    def inverse_row(self, k):
        def task():
            left = split(-dot(self.inv[k], self.sums.pop(k), NN))
            self.inv_rows[k] = beside([left, self.inv[k]])

        return task

    def solved(self, x, g):
        blocks = PIECES[g][0]
        return dot(beside(x[: g + 1]), self.inverse_rows(blocks, BLOCK * (blocks[-1] + 1)))


def remote(src, dst, send, recv, **device):
    return pltpu.make_async_remote_copy(
        src_ref=src, dst_ref=dst, send_sem=send, recv_sem=recv, device_id=device, device_id_type=MESH
    )


class Exchange:
    def __init__(self, diag, panel, own, dbuf, relay, rows, win, wsrc, wq, hq, pw, sems):
        self.diag, self.panel, self.own, self.dbuf, self.relay, self.rows = diag, panel, own, dbuf, relay, rows
        self.win, self.wsrc, self.wq, self.hq, self.pw = win, wsrc, wq, hq, pw
        (self.loc, self.ds, self.dr, self.cs, self.cr, self.rs, self.rr, self.zs, self.zr, self.xs, self.xr,
         self.w1s, self.w1r, self.w2s, self.w2r, self.w3s, self.w3r, self.w4s, self.w4r, self.w5s, self.w5r, self.w6s, self.w6r,
         self.as_, self.ar, self.bs, self.br, self.es, self.er) = sems
        self.r, self.c, self.s = (lax.axis_index(a) for a in ALL)
        self.corner = jnp.logical_and(self.r == 0, self.c == 0)

    def enter(self):
        r, c, s = self.r, self.c, self.s
        self.own_diag = pltpu.make_async_copy(self.diag, self.dbuf.at[r, c, s], self.loc.at[0])
        self.own_panel = pltpu.make_async_copy(self.panel, self.own, self.loc.at[1])
        self.own_diag.start()
        self.own_panel.start()
        barrier = pltpu.get_barrier_semaphore()
        for axis, me, n in (("depth", s, 8), ("col", c, 4), ("row", r, 4)):
            for t in range(1, n):
                pl.semaphore_signal(barrier, inc=1, device_id={axis: (me + t) % n}, device_id_type=MESH)
        self.own_panel.wait()
        n = self.own.shape[0]
        self.relay[c, 0:n] = self.own[...]
        self.relay[c, n:256] = jnp.zeros((256 - n, 512), F32)
        pl.semaphore_wait(barrier, 13)
        self.own_diag.wait()

    def diag_col(self, t, c):
        ref = self.dbuf.at[self.r, c, self.s]
        return remote(ref, ref, self.cs.at[t], self.cr.at[t], col=(self.c + t) % 4)

    def diag_col_send(self):
        for t in range(1, 4):
            self.diag_col(t, self.c).start()

    def diag_col_wait(self):
        for t in range(1, 4):
            self.diag_col(t, (self.c - t) % 4).wait_recv()

    def by_row(self, act):
        for i in range(4):

            @pl.when(self.r == i)
            def _():
                act(i)

    def diag_depth(self, t, s, i, part):
        cols = slice(0, 128) if part == 0 else slice(128, 128 * (i + 1))
        ref = self.dbuf.at[i, :, s, :, cols]
        return remote(ref, ref, self.ds.at[t, part], self.dr.at[t, part], depth=(self.s + t) % 8)

    def diag_depth_each(self, part, act, receive=False):
        def at_row(i):
            if i >= part:
                for t in range(1, 8):
                    act(self.diag_depth(t, (self.s - t) % 8 if receive else self.s, i, part))

        self.by_row(at_row)

    def diag_depth_send(self, part):
        self.diag_depth_each(part, lambda copy: copy.start())

    def diag_depth_wait(self, part):
        self.diag_depth_each(part, lambda copy: copy.wait_recv(), receive=True)

    def diag_row(self, t, i, b):
        ref = self.dbuf.at[i, :, :, :, at(b)]
        return remote(ref, ref, self.rs.at[t, b], self.rr.at[t, b], row=(self.r + t) % 4)

    def diag_row_each(self, b, act):
        def at_row(i):
            if i >= b:
                for t in range(1, 4):
                    act(self.diag_row(t, i, b))

        self.by_row(at_row)

    def diag_row_send(self, b):
        self.diag_row_each(b, lambda copy: copy.start())

    def diag_first_send(self, rows):
        for i in rows:

            @pl.when(self.r == i)
            def _():
                for t in range(1, 4):
                    self.diag_row(t, i, 0).start()

    def diag_row_wait(self, src, b):
        def at_row(i):
            if i != src:
                self.diag_row((i - src) % 4, src, b).wait_recv()

        self.by_row(at_row)

    def rows_col(self, t, slot, b):
        ref = self.relay.at[slot, :, at(b)]
        return remote(ref, ref, self.zs.at[t, b], self.zr.at[t, b], col=(self.c + t) % 4)

    def rows_far_half(self, t, slot, b):
        ref = self.relay.at[slot, at((t - 1) // 2), at(b)]
        return remote(ref, ref, self.zs.at[t - 1, b], self.zr.at[t - 1, b], col=(self.c + t) % 4)

    def rows_col_send(self, b):
        for t in (1, 3):
            self.rows_col(t, self.c, b).start()

    def rows_near(self, b):
        for t in (1, 3):
            slot = (self.c - t) % 4
            self.rows_col(t, slot, b).wait_recv()
            self.rows_far_half(t, slot, b).start()

    def rows_near_pass(self, b):
        for t in (1, 3):
            self.rows_depth_send(t, (self.c - t) % 4, b)

    def rows_far_pass(self, b):
        slot = (self.c + 2) % 4
        for t in (1, 3):
            self.rows_far_half(t, slot, b).wait_recv()
        self.rows_depth_send(2, slot, b)

    def rows_depth(self, t, slot, b):
        target, j = 2 * slot + self.s // 4, self.s % 4
        return target, remote(
            self.relay.at[slot, :, at(b)], self.rows.at[j, :, at(b)], self.xs.at[t, b], self.xr.at[j, b], depth=target
        )

    def rows_depth_send(self, t, slot, b):
        target, copy = self.rows_depth(t, slot, b)

        @pl.when(target != self.s)
        def _():
            copy.start()

        @pl.when(target == self.s)
        def _():
            self.rows[self.s % 4, :, at(b)] = self.relay[slot, :, at(b)]

    def rows_wait(self, b):
        for j in range(4):
            source = 4 * (self.s % 2) + j
            ref = self.rows.at[j, :, at(b)]

            @pl.when(source != self.s)
            def _():
                remote(ref, ref, self.xs.at[0, b], self.xr.at[j, b], depth=source).wait_recv()

    def quarter(self, a):
        return pl.ds(pl.multiple_of(64 * a, 64), 64), slice(256, 512)

    def half_col(self, t, slot, a):
        ref = self.relay.at[(slot, *self.quarter(a))]
        return remote(ref, ref, self.as_.at[t], self.ar.at[t], col=(self.c + t) % 4)

    def half_col_send(self):
        for t in (1, 3, 2):
            self.half_col(t, self.c, (self.c + t) % 4).start()

    def half_depth(self, t):
        slot = (self.c - t) % 4
        target, j, part = 2 * slot + self.s // 4, self.s % 4, self.quarter(self.c)
        return target, (slot, *part), (j, *part)

    def half_depth_copy(self, t):
        target, src, dst = self.half_depth(t)
        return remote(
            self.relay.at[src], self.rows.at[dst], self.bs.at[t], self.br.at[self.s % 4], depth=target
        )

    def half_depth_send(self):
        for t in range(4):
            if t:
                self.half_col(t, (self.c - t) % 4, self.c).wait_recv()
            target, src, dst = self.half_depth(t)

            @pl.when(target != self.s)
            def _():
                self.half_depth_copy(t).start()

            @pl.when(target == self.s)
            def _():
                self.rows[dst] = self.relay[src]

    def half_all(self, t, a):
        ref = self.rows.at[(slice(None), *self.quarter(a))]
        return remote(ref, ref, self.es.at[t], self.er.at[t], col=(self.c + t) % 4)

    def half_all_send(self):
        for j in range(4):
            source = 4 * (self.s % 2) + j
            ref = self.rows.at[(j, *self.quarter(self.c))]

            @pl.when(source != self.s)
            def _():
                remote(ref, ref, self.bs.at[0], self.br.at[j], depth=source).wait_recv()

        for t in (1, 3):
            self.half_all(t, self.c).start()

    def half_far_half(self, t, a):
        ref = self.rows.at[(slice(t - 1, t + 1), *self.quarter(a))]
        return remote(ref, ref, self.es.at[t - 1], self.er.at[t - 1], col=(self.c + t) % 4)

    def half_all_near(self):
        for t in (1, 3):
            a = (self.c - t) % 4
            self.half_all(t, a).wait_recv()
            self.half_far_half(t, a).start()

    def half_all_far(self):
        for t in (1, 3):
            self.half_far_half(t, (self.c + 2) % 4).wait_recv()

    def corner_case(self, rows, i, act):
        here = jnp.logical_and(self.c == 0, self.s == i)
        if rows is not None:
            here = jnp.logical_and(here, jnp.logical_and(self.r >= rows[0], self.r <= rows[-1]))

        @pl.when(here)
        def _():
            act()

    def win_main(self, i, t):
        n = 16 if t < 3 else 15 - i
        return remote(
            self.wsrc.at[i + 16 * t : i + 16 * t + n], self.wq.at[0:n], self.w1s.at[t], self.w1r.at[0], row=t
        )

    def win_head(self, i):
        return remote(self.wsrc.at[0:i], self.hq.at[0:i], self.w1s.at[4], self.w1r.at[1], row=3)

    def win_scatter(self, act):
        def copies(i):
            if i < 4:
                for t in range(1, 4):
                    act(self.win_main(i, t))
            if i > 0:
                act(self.win_head(i))

        for i in range(5):
            self.corner_case((0,), i, lambda: copies(i))

    def win_scatter_send(self):
        @pl.when(jnp.logical_and(self.corner, self.s < 5))
        def _():
            for u in range(63):
                self.wsrc[u] = self.relay[0, 4 * u : 4 * u + 4, :]

        self.win_scatter(lambda copy: copy.start())

    def win_scatter_wait(self):
        for i in range(5):
            if i < 4:
                self.corner_case((1, 2), i, lambda: self.win_main(i, 1).wait_recv())
                self.corner_case((3,), i, lambda: self.win_main(i, 3).wait_recv())
            if i > 0:
                self.corner_case((3,), i, lambda: self.win_head(i).wait_recv())

    def win_piece(self, rows, i, d):
        n = 2 if rows[0] < 3 else min(max(15 - i - 2 * d, 0), 2)
        if n == 0:
            return None
        src = self.wsrc.at[i + 2 * d : i + 2 * d + n] if rows[0] == 0 else self.wq.at[2 * d : 2 * d + n]
        dst = self.pw.at[i, 0:n]
        return src, dst, lambda: remote(src, dst, self.w2s.at[d], self.w2r.at[i], depth=d)

    def win_head_piece(self, c, d):
        first, last = max(0, 2 * d - 15 + c), min(c + 1, 2 * d - 13 + c)
        if d < 6 or first >= last:
            return None
        slot = (15 - c + first) % 2
        return remote(
            self.hq.at[first:last],
            self.pw.at[c, slot : slot + last - first],
            self.w2s.at[2 + d],
            self.w2r.at[4 + c],
            depth=d,
        )

    def win_spread(self, act, local=False):
        def copies(rows, i):
            for d in range(8):
                if i < 4:
                    piece = self.win_piece(rows, i, d)
                    if piece and d != i:
                        act(piece[2]())
                    elif piece and local:
                        piece[1][...] = piece[0][...]
                if i > 0 and rows[0] == 3:
                    copy = self.win_head_piece(i - 1, d)
                    if copy:
                        act(copy)

        for i in range(5):
            for rows in ((0,), (1, 2), (3,)):
                self.corner_case(rows, i, lambda: copies(rows, i))

    def win_spread_send(self):
        self.win_spread(lambda copy: copy.start(), local=True)

    def win_spread_wait(self):
        def waits(rows, d):
            for i in range(4):
                piece = self.win_piece(rows, i, d)
                if piece and d != i:
                    piece[2]().wait_recv()
                if rows[0] == 3:
                    copy = self.win_head_piece(i, d)
                    if copy:
                        copy.wait_recv()

        for d in range(8):
            for rows in ((0, 1, 2), (3,)):
                self.corner_case(rows, d, lambda: waits(rows, d))

    def win_col(self, t):
        return remote(self.pw.at[t], self.win_at(self.s), self.w3s.at[t], self.w3r.at[0], col=t)

    def win_col_send(self):
        @pl.when(self.c == 0)
        def _():
            for t in range(1, 4):
                self.win_col(t).start()
            self.win[self.s // 2, self.s % 2, self.r] = self.pw[0]

    def win_col_wait(self):
        @pl.when(self.c != 0)
        def _():
            self.win_col(1).wait_recv()

    def win_at(self, d):
        return self.win.at[d // 2, d % 2, self.r]

    def win_depth(self, t, d):
        ref = self.win_at(d)
        return remote(ref, ref, self.w4s.at[t], self.w4r.at[t], depth=(self.s + t) % 8)

    def win_depth_send(self):
        for t in (2, 4, 6):
            self.win_depth(t, self.s).start()

    def win_depth_wait(self):
        for t in (2, 4, 6):
            self.win_depth(t, (self.s - t) % 8).wait_recv()

    def win_all(self, t, row):
        ref = self.win.at[:, self.s % 2, row]
        return remote(ref, ref, self.w5s.at[t], self.w5r.at[t], row=(self.r + t) % 4)

    def win_all_send(self):
        for t in range(1, 4):
            self.win_all(t, self.r).start()

    def win_all_wait(self):
        for t in range(1, 4):
            self.win_all(t, (self.r - t) % 4).wait_recv()

    def win_pair(self, core):
        ref = self.win.at[:, core]
        return remote(ref, ref, self.w6s.at[0], self.w6r.at[0], depth=self.s + 1 - 2 * (self.s % 2))

    def win_pair_send(self):
        self.win_pair(self.s % 2).start()

    def win_pair_wait(self):
        self.win_pair(1 - self.s % 2).wait_recv()

    def leave_early(self):
        for t in (2, 4, 6):
            self.win_depth(t, self.s).wait_send()
        for part in range(2):
            self.diag_depth_each(part, lambda copy: copy.wait_send())
        for b in range(4):
            self.diag_row_each(b, lambda copy: copy.wait_send())
        for t in range(1, 4):
            self.diag_col(t, self.c).wait_send()
            self.half_col(t, self.c, (self.c + t) % 4).wait_send()
        for t in range(4):
            target = self.half_depth(t)[0]

            @pl.when(target != self.s)
            def _():
                self.half_depth_copy(t).wait_send()

        for b in range(2):
            for t in (1, 3):
                self.rows_col(t, self.c, b).wait_send()
                self.rows_far_half(t, (self.c - t) % 4, b).wait_send()
        self.win_scatter(lambda copy: copy.wait_send())
        self.win_spread(lambda copy: copy.wait_send())

        @pl.when(self.c == 0)
        def _():
            for t in range(1, 4):
                self.win_col(t).wait_send()

    def leave(self):
        self.win_pair(self.s % 2).wait_send()
        for t in range(1, 4):
            self.win_all(t, self.r).wait_send()
        for t in (1, 3):
            self.half_all(t, self.c).wait_send()
            self.half_far_half(t, (self.c - t) % 4).wait_send()
        for b in range(2):
            for t in range(4):
                target, copy = self.rows_depth(t, (self.c - t) % 4, b)

                @pl.when(target != self.s)
                def _():
                    copy.wait_send()


SEMAPHORES = ((3,), (8, 2), (8, 2), (4,), (4,), (4, 4), (4, 4), (4, 2), (4, 2), (4, 2), (4, 2),
              (5,), (2,), (10,), (8,), (4,), (1,), (8,), (8,), (4,), (4,), (1,), (1,),
              (4,), (4,), (4,), (4,), (4,), (4,))


def kernel(
    diag_in, panel, trailing_in, own_l, solved, updated,
    own, dbuf, relay, rows, win, wsrc, wq, hq, pw, diag, window, l, trailing, *sems,
):
    e = Exchange(diag_in, panel, own, dbuf, relay, rows, win, wsrc, wq, hq, pw, sems)
    f = Factor(diag, l)

    def assemble(i, b):
        e.diag_row_wait(i, b)
        for c in range(4):
            for s in range(8):
                first = 128 * i + 32 * c + 4 * s
                diag[first : first + 4, at(b)] = dbuf[i, c, s, :, at(b)]

    def assemble_column(b):
        for i in range(b, 4):
            if i > 0:
                assemble(i, b)

    own_trailing = pltpu.make_async_copy(trailing_in, trailing, sems[0].at[2])
    own_trailing.start()
    e.enter()
    e.diag_col_send()
    e.half_col_send()
    e.rows_col_send(0)
    e.win_scatter_send()
    e.rows_col_send(1)
    e.diag_col_wait()
    e.diag_depth_send(0)
    e.diag_depth_send(1)
    e.half_depth_send()
    e.diag_depth_wait(0)
    e.diag_first_send((0,))
    e.win_scatter_wait()
    e.win_spread_send()
    e.diag_depth_wait(1)
    e.rows_depth_send(0, e.c, 0)
    e.rows_near(0)
    e.rows_near_pass(0)
    e.diag_first_send((1, 2, 3))
    e.diag_row_send(1)
    e.diag_row_send(2)
    e.diag_row_send(3)
    assemble(0, 0)
    e.win_spread_wait()
    e.win_col_send()
    e.rows_near(1)
    e.half_all_send()
    f.block(0)
    e.win_col_wait()
    e.win_depth_send()
    e.rows_far_pass(0)
    e.rows_depth_send(0, e.c, 1)
    e.rows_near_pass(1)
    assemble_column(0)
    f.rest(0)
    assemble_column(1)

    size = panel.shape[0]
    own_a, window_a, w, total = [], [], [], [None] * 4
    rows_a, rows_x = [[] for _ in range(4)], [[] for _ in range(4)]

    def own_task(g):
        def task():
            own_a.append(split(own[:, PIECES[g][1]]))
            solved[:, PIECES[g][1]] = f.solved(own_a, g)

        return task

    def row_load(j, g):
        return lambda: rows_a[j].append(split(rows[j, 0:size, PIECES[g][1]]))

    def row_task(j, g):
        return lambda: rows_x[j].append(split(f.solved(rows_a[j], g)))

    def window_load():
        for s in range(8):
            for r in range(4):
                for u in range(2):
                    first = 64 * r + 8 * s + 4 * u
                    window[first : first + 4, :] = win[s // 2, s % 2, r, u]
        for _, columns in PIECES:
            window_a.append(split(window[:, columns]))

    def window_task(g):
        return lambda: w.append(split(f.solved(window_a, g)))

    def product_task(j, g):
        def task():
            term = dot(rows_x[j][g], w[g])
            total[j] = term if total[j] is None else total[j] + term

        return task

    def second_hook():
        e.rows_far_pass(1)

    f.block(1, [f.prepare(1, 2), f.prepare(1, 3)], [(8, second_hook, ())])
    e.win_depth_wait()
    e.win_all_send()
    e.half_all_near()
    f.rest(1)
    assemble_column(2)
    f.block(2, [f.prepare(2, 3), f.inverse_sum(1), f.inverse_row(1), f.inverse_sum(2), own_task(0)])
    f.rest(2)
    assemble_column(3)


    e.win_all_wait()
    e.win_pair_send()

    def rows_hook():
        e.rows_wait(0)
        e.rows_wait(1)

    def last_hook():
        e.leave_early()
        e.half_all_far()
        e.win_pair_wait()

    f.block(
        3,
        [f.inverse_row(2), f.inverse_sum(3), own_task(1)],
        [
            (ROWS_AT, rows_hook, [t(j, 0) for j in range(4) for t in (row_load, row_task)]),
            (
                LAST_AT,
                last_hook,
                [window_load, window_task(0), window_task(1)]
                + [t(j, 1) for j in range(4) for t in (row_load, row_task)]
                + [product_task(j, g) for g in range(2) for j in range(4)]
                + [row_load(j, 2) for j in range(4)],
            ),
        ],
    )
    f.inverse_row(3)()
    window_task(2)()
    own_trailing.wait()
    for j in range(4):
        row_task(j, 2)()
        product_task(j, 2)()
        span = slice(size * j, size * (j + 1))
        updated[span, :] = trailing[span, :] - total[j]
    own_task(2)()
    position = (e.r * 4 + e.c) * 8 + e.s
    pair = l[pl.ds(pl.multiple_of((position // 2) * 8, 8), 8), :]
    own_l[...] = jnp.where(position % 2 == 0, pair[0:4], pair[4:8])
    e.leave()


def deliver(own_l, solved, updated, own_l_out, solved_out, updated_out, sem):
    copies = [
        pltpu.make_async_copy(src, dst, sem.at[i])
        for i, (src, dst) in enumerate(((own_l, own_l_out), (solved, solved_out), (updated, updated_out)))
    ]
    for copy in copies:
        copy.start()
    for copy in copies:
        copy.wait()


def body(diag_block, panel_rows, trailing):
    vmem = pl.BlockSpec(memory_space=pltpu.VMEM)
    hbm = pl.BlockSpec(memory_space=pltpu.HBM)
    shapes = (
        panel_rows.shape,
        (4, 4, 8, 4, 512),
        (4, 256, 512),
        (4, 256, 512),
        (4, 2, 4, 2, 4, 512),
        (63, 4, 512),
        (16, 4, 512),
        (4, 4, 512),
        (4, 2, 4, 512),
        (512, 512),
        (256, 512),
        (512, 512),
        trailing.shape,
    )
    outs = tuple(jax.ShapeDtypeStruct(a.shape, F32) for a in (diag_block, panel_rows, trailing))
    results = pl.pallas_call(
        kernel,
        out_shape=outs,
        in_specs=[hbm] * 3,
        out_specs=(vmem,) * 3,
        scratch_shapes=[pltpu.VMEM(shape, F32) for shape in shapes]
        + [pltpu.SemaphoreType.DMA(n) for n in SEMAPHORES],
        compiler_params=pltpu.CompilerParams(
            collective_id=0, has_side_effects=True, vmem_limit_bytes=VMEM_LIMIT
        ),
        name="panel_step",
    )(*(pltpu.with_memory_space_constraint(x, pltpu.HBM) for x in (diag_block, panel_rows, trailing)))
    return pl.pallas_call(
        deliver,
        out_shape=outs,
        in_specs=[vmem] * 3,
        out_specs=(hbm,) * 3,
        scratch_shapes=[pltpu.SemaphoreType.DMA((3,))],
        compiler_params=pltpu.CompilerParams(vmem_limit_bytes=2 * 2**20),
        name="deliver",
    )(*results)


VMEM_LIMIT = 44 * 2**20


def solution(mesh):
    specs = (P(ALL, None), P(ALL, None), P(("row", "depth"), "col"))
    return jax.shard_map(body, mesh=mesh, in_specs=specs, out_specs=specs, check_vma=False)
```

```python
import jax
import jax.numpy as jnp
from jax import lax
from jax.experimental import pallas as pl
from jax.experimental.pallas import tpu as pltpu
from jax.sharding import PartitionSpec as P

ALL = ("row", "col", "depth")
F32 = jnp.float32
NT = (((1,), (1,)), ((), ()))
NN = (((1,), (0,)), ((), ()))
BLOCK = 128
NEAR = 4
ROWS_AT, LAST_AT = 3, 9
MESH = pl.DeviceIdType.MESH


def at(i):
    return slice(BLOCK * i, BLOCK * (i + 1))


PIECES = (((0, 1), slice(0, 256)), ((2,), slice(256, 384)), ((3,), slice(384, 512)))


def split(x):
    hi = x.astype(jnp.bfloat16)
    return hi, (x - hi.astype(F32)).astype(jnp.bfloat16)


def dot(a, b, dims=NT):
    left = jnp.concatenate([a[0], a[1], a[0]], 1)
    right = jnp.concatenate([b[0], b[0], b[1]], dims[0][1][0])
    return lax.dot_general(left, right, dims, preferred_element_type=F32)


def beside(parts, axis=1):
    return tuple(jnp.concatenate(x, axis) if len(x) > 1 else x[0] for x in zip(*parts))


def sub(v, k):
    return jnp.broadcast_to(v[k : k + 1, :], (8, 128))


class Block:
    def __init__(self, rows):
        self.ri = lax.broadcasted_iota(jnp.int32, (8, 128), 0)
        self.li = lax.broadcasted_iota(jnp.int32, (8, 128), 1)
        self.rows = rows
        self.upper, self.inverse = [], []

    def advance(self, p):
        ri, li, rows = self.ri, self.li, self.rows
        first = 8 * p
        raw = [jnp.broadcast_to(rows[:, :, first + j : first + j + 1], rows.shape) for j in range(8)]
        e = {(i, j): sub(raw[j][0], i) for j in range(8) for i in range(j, 8)}
        near = min(NEAR + 1, rows.shape[0])
        cols = [x[1:near] for x in raw]
        scales, factors = [], []
        r = [sub(rows[0], k) for k in range(8)]
        s = [jnp.where(li < first, r[k], jnp.where(li == first + k, 1.0, 0.0)) for k in range(8)]
        for k in range(8):
            inv = lax.rsqrt(e[k, k])
            m = {j: e[j, k] * inv for j in range(k + 1, 8)}
            for j in range(k + 1, 8):
                for i in range(j, 8):
                    e[i, j] = e[i, j] - m[i] * m[j]
            scales.append(inv)
            factors.append(m)
            if near > 1:
                cols[k] = cols[k] * inv
            r[k] = r[k] * inv
            s[k] = s[k] * inv
            for j in range(k + 1, 8):
                if near > 1:
                    cols[j] = cols[j] - cols[k] * m[j]
                r[j] = r[j] - m[j] * r[k]
                s[j] = s[j] - m[j] * s[k]
        u, t = r[0], s[0]
        for k in range(1, 8):
            u = jnp.where(ri == k, r[k], u)
            t = jnp.where(ri == k, s[k], t)
        self.upper.append(jnp.where(li >= ri + first, u, 0.0))
        self.inverse.append(t)
        if p < 15:
            rows = jnp.where(((li < first) | (li >= first + 8))[None], rows[1:], 0.0)
            both = [jnp.where(li < first + 8, s[k], r[k]) for k in range(8)]
            close, parts = rows[: near - 1], []
            for k in range(8):
                close = close - cols[k] * both[k]
            parts.append(close)
            if rows.shape[0] > near - 1:
                for k in range(7, -1, -1):
                    for j in range(k + 1, 8):
                        both[k] = both[k] - factors[k][j] * both[j]
                    both[k] = both[k] * scales[k]
                far = rows[near - 1 :]
                for k in range(8):
                    far = far - raw[k][near:] * both[k]
                parts.append(far)
            rows = jnp.concatenate(parts, 0) if len(parts) > 1 else close
            self.rows = rows


class Factor:
    def __init__(self, a, l):
        self.a, self.l = a, l
        self.lows, self.inv, self.inv_rows, self.below, self.sums = {}, {}, {}, {}, {}

    def low_row(self, i, n):
        return beside([self.lows[i, m] for m in range(n)])

    def column(self, k, i):
        value = self.a[at(i), at(k)]
        return value - dot(self.low_row(i, k), self.low_row(k, k)) if k else value

    def block(self, k, tasks=(), hooks=()):
        value = self.column(k, k)
        b = Block(value.reshape(16, 8, 128))
        stages = [(0, lambda: None, tasks), *hooks, (16, None, ())]
        for (start, wait, work), (end, _, _) in zip(stages, stages[1:]):
            wait()
            work = list(work)
            for p in range(start, end):
                b.advance(p)
                for _ in range(-(-len(work) // (end - p))):
                    work.pop(0)()
        self.inv[k] = split(jnp.concatenate(b.inverse, 0))
        if k == 0:
            self.inv_rows[0] = self.inv[0]
        self.l[at(k), at(k)] = jnp.concatenate(b.upper, 0).T
        for j in range(k + 1, 4):
            self.l[at(k), at(j)] = jnp.zeros((BLOCK, BLOCK), F32)

    def prepare(self, k, i):
        def task():
            self.below[i] = split(self.column(k, i))

        return task

    def rest(self, k):
        for i in range(k + 1, 4):
            if i not in self.below:
                self.prepare(k, i)()
            low = dot(self.below.pop(i), self.inv[k])
            self.l[at(i), at(k)] = low
            self.lows[i, k] = split(low)

    def inverse_rows(self, rows, width):
        parts = []
        for k in rows:
            fill = jnp.zeros((BLOCK, width - BLOCK * (k + 1)), jnp.bfloat16)
            parts.append(beside([self.inv_rows[k], (fill, fill)]) if fill.shape[1] else self.inv_rows[k])
        return beside(parts, 0)

    def inverse_sum(self, k):
        def task():
            total = dot(self.low_row(k, k), self.inverse_rows(range(k), BLOCK * k), NN)
            self.sums[k] = split(total)

        return task

    def inverse_row(self, k):
        def task():
            left = split(-dot(self.inv[k], self.sums.pop(k), NN))
            self.inv_rows[k] = beside([left, self.inv[k]])

        return task

    def solved(self, x, g):
        blocks = PIECES[g][0]
        return dot(beside(x[: g + 1]), self.inverse_rows(blocks, BLOCK * (blocks[-1] + 1)))


def remote(src, dst, send, recv, **device):
    return pltpu.make_async_remote_copy(
        src_ref=src, dst_ref=dst, send_sem=send, recv_sem=recv, device_id=device, device_id_type=MESH
    )


class Exchange:
    def __init__(self, diag, panel, own, dbuf, relay, rows, win, wsrc, wq, hq, pw, sems):
        self.diag, self.panel, self.own, self.dbuf, self.relay, self.rows = diag, panel, own, dbuf, relay, rows
        self.win, self.wsrc, self.wq, self.hq, self.pw = win, wsrc, wq, hq, pw
        (self.loc, self.ds, self.dr, self.cs, self.cr, self.rs, self.rr, self.zs, self.zr, self.xs, self.xr,
         self.w1s, self.w1r, self.w2s, self.w2r, self.w3s, self.w3r, self.w4s, self.w4r, self.w5s, self.w5r, self.w6s, self.w6r,
         self.as_, self.ar, self.bs, self.br, self.es, self.er) = sems
        self.r, self.c, self.s = (lax.axis_index(a) for a in ALL)
        self.corner = jnp.logical_and(self.r == 0, self.c == 0)

    def enter(self):
        r, c, s = self.r, self.c, self.s
        self.own_diag = pltpu.make_async_copy(self.diag, self.dbuf.at[r, c, s], self.loc.at[0])
        self.own_panel = pltpu.make_async_copy(self.panel, self.own, self.loc.at[1])
        self.own_diag.start()
        self.own_panel.start()
        barrier = pltpu.get_barrier_semaphore()
        for axis, me, n in (("depth", s, 8), ("col", c, 4), ("row", r, 4)):
            for t in range(1, n):
                pl.semaphore_signal(barrier, inc=1, device_id={axis: (me + t) % n}, device_id_type=MESH)
        pl.semaphore_wait(barrier, 13)
        self.own_diag.wait()

    def load_panel(self):
        self.own_panel.wait()
        n = self.own.shape[0]
        self.relay[self.c, 0:n] = self.own[...]
        self.relay[self.c, n:256] = jnp.zeros((256 - n, 512), F32)

    def diag_col(self, t, c):
        ref = self.dbuf.at[self.r, c, self.s]
        return remote(ref, ref, self.cs.at[t], self.cr.at[t], col=(self.c + t) % 4)

    def diag_col_send(self):
        for t in range(1, 4):
            self.diag_col(t, self.c).start()

    def diag_col_wait(self):
        for t in range(1, 4):
            self.diag_col(t, (self.c - t) % 4).wait_recv()

    def by_row(self, act):
        for i in range(4):

            @pl.when(self.r == i)
            def _():
                act(i)

    def diag_depth(self, t, s, i, part):
        cols = slice(0, 128) if part == 0 else slice(128, 128 * (i + 1))
        ref = self.dbuf.at[i, :, s, :, cols]
        return remote(ref, ref, self.ds.at[t, part], self.dr.at[t, part], depth=(self.s + t) % 8)

    def diag_depth_each(self, part, act, receive=False):
        def at_row(i):
            if i >= part:
                for t in range(1, 8):
                    act(self.diag_depth(t, (self.s - t) % 8 if receive else self.s, i, part))

        self.by_row(at_row)

    def diag_depth_send(self, part):
        self.diag_depth_each(part, lambda copy: copy.start())

    def diag_depth_wait(self, part):
        self.diag_depth_each(part, lambda copy: copy.wait_recv(), receive=True)

    def diag_row(self, t, i, b):
        ref = self.dbuf.at[i, :, :, :, at(b)]
        return remote(ref, ref, self.rs.at[t, b], self.rr.at[t, b], row=(self.r + t) % 4)

    def diag_row_each(self, b, act):
        def at_row(i):
            if i >= b:
                for t in range(1, 4):
                    act(self.diag_row(t, i, b))

        self.by_row(at_row)

    def diag_row_send(self, b):
        self.diag_row_each(b, lambda copy: copy.start())

    def diag_first_send(self, rows):
        for i in rows:

            @pl.when(self.r == i)
            def _():
                for t in range(1, 4):
                    self.diag_row(t, i, 0).start()

    def diag_row_wait(self, src, b):
        def at_row(i):
            if i != src:
                self.diag_row((i - src) % 4, src, b).wait_recv()

        self.by_row(at_row)

    def rows_col(self, t, slot, b):
        ref = self.relay.at[slot, :, at(b)]
        return remote(ref, ref, self.zs.at[t, b], self.zr.at[t, b], col=(self.c + t) % 4)

    def rows_far_half(self, t, slot, b):
        ref = self.relay.at[slot, at((t - 1) // 2), at(b)]
        return remote(ref, ref, self.zs.at[t - 1, b], self.zr.at[t - 1, b], col=(self.c + t) % 4)

    def rows_col_send(self, b):
        for t in (1, 3):
            self.rows_col(t, self.c, b).start()

    def rows_near(self, b):
        for t in (1, 3):
            slot = (self.c - t) % 4
            self.rows_col(t, slot, b).wait_recv()
            self.rows_far_half(t, slot, b).start()

    def rows_near_pass(self, b):
        for t in (1, 3):
            self.rows_depth_send(t, (self.c - t) % 4, b)

    def rows_far_pass(self, b):
        slot = (self.c + 2) % 4
        for t in (1, 3):
            self.rows_far_half(t, slot, b).wait_recv()
        self.rows_depth_send(2, slot, b)

    def rows_depth(self, t, slot, b):
        target, j = 2 * slot + self.s // 4, self.s % 4
        return target, remote(
            self.relay.at[slot, :, at(b)], self.rows.at[j, :, at(b)], self.xs.at[t, b], self.xr.at[j, b], depth=target
        )

    def rows_depth_send(self, t, slot, b):
        target, copy = self.rows_depth(t, slot, b)

        @pl.when(target != self.s)
        def _():
            copy.start()

        @pl.when(target == self.s)
        def _():
            self.rows[self.s % 4, :, at(b)] = self.relay[slot, :, at(b)]

    def rows_wait(self, b):
        for j in range(4):
            source = 4 * (self.s % 2) + j
            ref = self.rows.at[j, :, at(b)]

            @pl.when(source != self.s)
            def _():
                remote(ref, ref, self.xs.at[0, b], self.xr.at[j, b], depth=source).wait_recv()

    def quarter(self, a):
        return pl.ds(pl.multiple_of(64 * a, 64), 64), slice(256, 512)

    def half_col(self, t, slot, a):
        ref = self.relay.at[(slot, *self.quarter(a))]
        return remote(ref, ref, self.as_.at[t], self.ar.at[t], col=(self.c + t) % 4)

    def half_col_send(self):
        for t in (1, 3, 2):
            self.half_col(t, self.c, (self.c + t) % 4).start()

    def half_depth(self, t):
        slot = (self.c - t) % 4
        target, j, part = 2 * slot + self.s // 4, self.s % 4, self.quarter(self.c)
        return target, (slot, *part), (j, *part)

    def half_depth_copy(self, t):
        target, src, dst = self.half_depth(t)
        return remote(
            self.relay.at[src], self.rows.at[dst], self.bs.at[t], self.br.at[self.s % 4], depth=target
        )

    def half_depth_send(self):
        for t in range(4):
            if t:
                self.half_col(t, (self.c - t) % 4, self.c).wait_recv()
            target, src, dst = self.half_depth(t)

            @pl.when(target != self.s)
            def _():
                self.half_depth_copy(t).start()

            @pl.when(target == self.s)
            def _():
                self.rows[dst] = self.relay[src]

    def half_all(self, t, a):
        ref = self.rows.at[(slice(None), *self.quarter(a))]
        return remote(ref, ref, self.es.at[t], self.er.at[t], col=(self.c + t) % 4)

    def half_all_send(self):
        for j in range(4):
            source = 4 * (self.s % 2) + j
            ref = self.rows.at[(j, *self.quarter(self.c))]

            @pl.when(source != self.s)
            def _():
                remote(ref, ref, self.bs.at[0], self.br.at[j], depth=source).wait_recv()

        for t in (1, 3):
            self.half_all(t, self.c).start()

    def half_far_half(self, t, a):
        ref = self.rows.at[(slice(t - 1, t + 1), *self.quarter(a))]
        return remote(ref, ref, self.es.at[t - 1], self.er.at[t - 1], col=(self.c + t) % 4)

    def half_all_near(self):
        for t in (1, 3):
            a = (self.c - t) % 4
            self.half_all(t, a).wait_recv()
            self.half_far_half(t, a).start()

    def half_all_far(self):
        for t in (1, 3):
            self.half_far_half(t, (self.c + 2) % 4).wait_recv()

    def corner_case(self, rows, i, act):
        here = jnp.logical_and(self.c == 0, self.s == i)
        if rows is not None:
            here = jnp.logical_and(here, jnp.logical_and(self.r >= rows[0], self.r <= rows[-1]))

        @pl.when(here)
        def _():
            act()

    def win_main(self, i, t):
        n = 16 if t < 3 else 15 - i
        return remote(
            self.wsrc.at[i + 16 * t : i + 16 * t + n], self.wq.at[0:n], self.w1s.at[t], self.w1r.at[0], row=t
        )

    def win_head(self, i):
        return remote(self.wsrc.at[0:i], self.hq.at[0:i], self.w1s.at[4], self.w1r.at[1], row=3)

    def win_scatter(self, act):
        def copies(i):
            if i < 4:
                for t in range(1, 4):
                    act(self.win_main(i, t))
            if i > 0:
                act(self.win_head(i))

        for i in range(5):
            self.corner_case((0,), i, lambda: copies(i))

    def win_scatter_send(self):
        @pl.when(jnp.logical_and(self.corner, self.s < 5))
        def _():
            for u in range(63):
                self.wsrc[u] = self.relay[0, 4 * u : 4 * u + 4, :]

        self.win_scatter(lambda copy: copy.start())

    def win_scatter_wait(self):
        for i in range(5):
            if i < 4:
                self.corner_case((1, 2), i, lambda: self.win_main(i, 1).wait_recv())
                self.corner_case((3,), i, lambda: self.win_main(i, 3).wait_recv())
            if i > 0:
                self.corner_case((3,), i, lambda: self.win_head(i).wait_recv())

    def win_piece(self, rows, i, d):
        n = 2 if rows[0] < 3 else min(max(15 - i - 2 * d, 0), 2)
        if n == 0:
            return None
        src = self.wsrc.at[i + 2 * d : i + 2 * d + n] if rows[0] == 0 else self.wq.at[2 * d : 2 * d + n]
        dst = self.pw.at[i, 0:n]
        return src, dst, lambda: remote(src, dst, self.w2s.at[d], self.w2r.at[i], depth=d)

    def win_head_piece(self, c, d):
        first, last = max(0, 2 * d - 15 + c), min(c + 1, 2 * d - 13 + c)
        if d < 6 or first >= last:
            return None
        slot = (15 - c + first) % 2
        return remote(
            self.hq.at[first:last],
            self.pw.at[c, slot : slot + last - first],
            self.w2s.at[2 + d],
            self.w2r.at[4 + c],
            depth=d,
        )

    def win_spread(self, act, local=False):
        def copies(rows, i):
            for d in range(8):
                if i < 4:
                    piece = self.win_piece(rows, i, d)
                    if piece and d != i:
                        act(piece[2]())
                    elif piece and local:
                        piece[1][...] = piece[0][...]
                if i > 0 and rows[0] == 3:
                    copy = self.win_head_piece(i - 1, d)
                    if copy:
                        act(copy)

        for i in range(5):
            for rows in ((0,), (1, 2), (3,)):
                self.corner_case(rows, i, lambda: copies(rows, i))

    def win_spread_send(self):
        self.win_spread(lambda copy: copy.start(), local=True)

    def win_spread_wait(self):
        def waits(rows, d):
            for i in range(4):
                piece = self.win_piece(rows, i, d)
                if piece and d != i:
                    piece[2]().wait_recv()
                if rows[0] == 3:
                    copy = self.win_head_piece(i, d)
                    if copy:
                        copy.wait_recv()

        for d in range(8):
            for rows in ((0, 1, 2), (3,)):
                self.corner_case(rows, d, lambda: waits(rows, d))

    def win_col(self, t):
        return remote(self.pw.at[t], self.win_at(self.s), self.w3s.at[t], self.w3r.at[0], col=t)

    def win_col_send(self):
        @pl.when(self.c == 0)
        def _():
            for t in range(1, 4):
                self.win_col(t).start()
            self.win[self.s // 2, self.s % 2, self.r] = self.pw[0]

    def win_col_wait(self):
        @pl.when(self.c != 0)
        def _():
            self.win_col(1).wait_recv()

    def win_at(self, d):
        return self.win.at[d // 2, d % 2, self.r]

    def win_depth(self, t, d):
        ref = self.win_at(d)
        return remote(ref, ref, self.w4s.at[t], self.w4r.at[t], depth=(self.s + t) % 8)

    def win_depth_send(self):
        for t in (2, 4, 6):
            self.win_depth(t, self.s).start()

    def win_depth_wait(self):
        for t in (2, 4, 6):
            self.win_depth(t, (self.s - t) % 8).wait_recv()

    def win_all(self, t, row):
        ref = self.win.at[:, self.s % 2, row]
        return remote(ref, ref, self.w5s.at[t], self.w5r.at[t], row=(self.r + t) % 4)

    def win_all_send(self):
        for t in range(1, 4):
            self.win_all(t, self.r).start()

    def win_all_wait(self):
        for t in range(1, 4):
            self.win_all(t, (self.r - t) % 4).wait_recv()

    def win_pair(self, core):
        ref = self.win.at[:, core]
        return remote(ref, ref, self.w6s.at[0], self.w6r.at[0], depth=self.s + 1 - 2 * (self.s % 2))

    def win_pair_send(self):
        self.win_pair(self.s % 2).start()

    def win_pair_wait(self):
        self.win_pair(1 - self.s % 2).wait_recv()

    def leave_early(self):
        for t in (2, 4, 6):
            self.win_depth(t, self.s).wait_send()
        for part in range(2):
            self.diag_depth_each(part, lambda copy: copy.wait_send())
        for b in range(4):
            self.diag_row_each(b, lambda copy: copy.wait_send())
        for t in range(1, 4):
            self.diag_col(t, self.c).wait_send()
            self.half_col(t, self.c, (self.c + t) % 4).wait_send()
        for t in range(4):
            target = self.half_depth(t)[0]

            @pl.when(target != self.s)
            def _():
                self.half_depth_copy(t).wait_send()

        for b in range(2):
            for t in (1, 3):
                self.rows_col(t, self.c, b).wait_send()
                self.rows_far_half(t, (self.c - t) % 4, b).wait_send()
        self.win_scatter(lambda copy: copy.wait_send())
        self.win_spread(lambda copy: copy.wait_send())

        @pl.when(self.c == 0)
        def _():
            for t in range(1, 4):
                self.win_col(t).wait_send()

    def leave(self):
        self.win_pair(self.s % 2).wait_send()
        for t in range(1, 4):
            self.win_all(t, self.r).wait_send()
        for t in (1, 3):
            self.half_all(t, self.c).wait_send()
            self.half_far_half(t, (self.c - t) % 4).wait_send()
        for b in range(2):
            for t in range(4):
                target, copy = self.rows_depth(t, (self.c - t) % 4, b)

                @pl.when(target != self.s)
                def _():
                    copy.wait_send()


SEMAPHORES = ((3,), (8, 2), (8, 2), (4,), (4,), (4, 4), (4, 4), (4, 2), (4, 2), (4, 2), (4, 2),
              (5,), (2,), (10,), (8,), (4,), (1,), (8,), (8,), (4,), (4,), (1,), (1,),
              (4,), (4,), (4,), (4,), (4,), (4,))


def kernel(
    diag_in, panel, trailing_in, own_l, solved, updated,
    own, dbuf, relay, rows, win, wsrc, wq, hq, pw, diag, window, l, trailing, *sems,
):
    e = Exchange(diag_in, panel, own, dbuf, relay, rows, win, wsrc, wq, hq, pw, sems)
    f = Factor(diag, l)

    def assemble(i, b):
        e.diag_row_wait(i, b)
        for c in range(4):
            for s in range(8):
                first = 128 * i + 32 * c + 4 * s
                diag[first : first + 4, at(b)] = dbuf[i, c, s, :, at(b)]

    def assemble_column(b):
        for i in range(b, 4):
            if i > 0:
                assemble(i, b)

    own_trailing = pltpu.make_async_copy(trailing_in, trailing, sems[0].at[2])
    e.enter()
    e.diag_col_send()
    own_trailing.start()
    e.load_panel()
    e.half_col_send()
    e.rows_col_send(0)
    e.win_scatter_send()
    e.rows_col_send(1)
    e.diag_col_wait()
    e.diag_depth_send(0)
    e.diag_depth_send(1)
    e.half_depth_send()
    e.diag_depth_wait(0)
    e.diag_first_send((0,))
    e.win_scatter_wait()
    e.win_spread_send()
    e.diag_depth_wait(1)
    e.rows_depth_send(0, e.c, 0)
    e.rows_near(0)
    e.rows_near_pass(0)
    e.diag_first_send((1, 2, 3))
    e.diag_row_send(1)
    e.diag_row_send(2)
    e.diag_row_send(3)
    assemble(0, 0)
    e.win_spread_wait()
    e.win_col_send()
    e.rows_near(1)
    e.half_all_send()
    f.block(0)
    e.win_col_wait()
    e.win_depth_send()
    e.rows_far_pass(0)
    e.rows_depth_send(0, e.c, 1)
    e.rows_near_pass(1)
    assemble_column(0)
    f.rest(0)
    assemble_column(1)

    size = panel.shape[0]
    own_a, window_a, w, total = [], [], [], [None] * 4
    rows_a, rows_x = [[] for _ in range(4)], [[] for _ in range(4)]

    def own_task(g):
        def task():
            own_a.append(split(own[:, PIECES[g][1]]))
            solved[:, PIECES[g][1]] = f.solved(own_a, g)

        return task

    def row_load(j, g):
        return lambda: rows_a[j].append(split(rows[j, 0:size, PIECES[g][1]]))

    def row_task(j, g):
        return lambda: rows_x[j].append(split(f.solved(rows_a[j], g)))

    def window_load():
        for s in range(8):
            for r in range(4):
                for u in range(2):
                    first = 64 * r + 8 * s + 4 * u
                    window[first : first + 4, :] = win[s // 2, s % 2, r, u]
        for _, columns in PIECES:
            window_a.append(split(window[:, columns]))

    def window_task(g):
        return lambda: w.append(split(f.solved(window_a, g)))

    def product_task(j, g):
        def task():
            term = dot(rows_x[j][g], w[g])
            total[j] = term if total[j] is None else total[j] + term

        return task

    def second_hook():
        e.rows_far_pass(1)

    f.block(1, [f.prepare(1, 2), f.prepare(1, 3)], [(8, second_hook, ())])
    e.win_depth_wait()
    e.win_all_send()
    e.half_all_near()
    f.rest(1)
    assemble_column(2)
    f.block(2, [f.prepare(2, 3), f.inverse_sum(1), f.inverse_row(1), f.inverse_sum(2), own_task(0)])
    f.rest(2)
    assemble_column(3)


    def rows_hook():
        e.win_all_wait()
        e.win_pair_send()
        e.rows_wait(0)
        e.rows_wait(1)

    def last_hook():
        e.leave_early()
        e.half_all_far()
        e.win_pair_wait()

    f.block(
        3,
        [f.inverse_row(2), f.inverse_sum(3), own_task(1)],
        [
            (ROWS_AT, rows_hook, [t(j, 0) for j in range(4) for t in (row_load, row_task)]),
            (
                LAST_AT,
                last_hook,
                [window_load, window_task(0), window_task(1)]
                + [t(j, 1) for j in range(4) for t in (row_load, row_task)]
                + [product_task(j, g) for g in range(2) for j in range(4)]
                + [row_load(j, 2) for j in range(4)],
            ),
        ],
    )
    f.inverse_row(3)()
    window_task(2)()
    own_trailing.wait()
    for j in range(4):
        row_task(j, 2)()
        product_task(j, 2)()
        span = slice(size * j, size * (j + 1))
        updated[span, :] = trailing[span, :] - total[j]
    own_task(2)()
    position = (e.r * 4 + e.c) * 8 + e.s
    pair = l[pl.ds(pl.multiple_of((position // 2) * 8, 8), 8), :]
    own_l[...] = jnp.where(position % 2 == 0, pair[0:4], pair[4:8])
    e.leave()


def deliver(own_l, solved, updated, own_l_out, solved_out, updated_out, sem):
    rows = updated.shape[0]
    parts = [(own_l, own_l_out), (solved, solved_out)]
    for first in range(0, rows, 256):
        part = pl.ds(first, min(256, rows - first))
        parts.append((updated.at[part], updated_out.at[part]))
    copies = [pltpu.make_async_copy(src, dst, sem.at[i]) for i, (src, dst) in enumerate(parts)]
    for copy in copies:
        copy.start()
    for copy in copies:
        copy.wait()


def body(diag_block, panel_rows, trailing):
    vmem = pl.BlockSpec(memory_space=pltpu.VMEM)
    hbm = pl.BlockSpec(memory_space=pltpu.HBM)
    shapes = (
        panel_rows.shape,
        (4, 4, 8, 4, 512),
        (4, 256, 512),
        (4, 256, 512),
        (4, 2, 4, 2, 4, 512),
        (63, 4, 512),
        (16, 4, 512),
        (4, 4, 512),
        (4, 2, 4, 512),
        (512, 512),
        (256, 512),
        (512, 512),
        trailing.shape,
    )
    outs = tuple(jax.ShapeDtypeStruct(a.shape, F32) for a in (diag_block, panel_rows, trailing))
    results = pl.pallas_call(
        kernel,
        out_shape=outs,
        in_specs=[hbm] * 3,
        out_specs=(vmem,) * 3,
        scratch_shapes=[pltpu.VMEM(shape, F32) for shape in shapes]
        + [pltpu.SemaphoreType.DMA(n) for n in SEMAPHORES],
        compiler_params=pltpu.CompilerParams(
            collective_id=0, has_side_effects=True, vmem_limit_bytes=VMEM_LIMIT
        ),
        name="panel_step",
    )(*(pltpu.with_memory_space_constraint(x, pltpu.HBM) for x in (diag_block, panel_rows, trailing)))
    return pl.pallas_call(
        deliver,
        out_shape=outs,
        in_specs=[vmem] * 3,
        out_specs=(hbm,) * 3,
        scratch_shapes=[pltpu.SemaphoreType.DMA((6,))],
        compiler_params=pltpu.CompilerParams(vmem_limit_bytes=2 * 2**20),
        name="deliver",
    )(*results)


VMEM_LIMIT = 44 * 2**20


def solution(mesh):
    specs = (P(ALL, None), P(ALL, None), P(("row", "depth"), "col"))
    return jax.shard_map(body, mesh=mesh, in_specs=specs, out_specs=specs, check_vma=False)
```

```python
import jax
import jax.numpy as jnp
from jax import lax
from jax.experimental import pallas as pl
from jax.experimental.pallas import tpu as pltpu
from jax.sharding import PartitionSpec as P

ALL = ("row", "col", "depth")
F32 = jnp.float32
NT = (((1,), (1,)), ((), ()))
NN = (((1,), (0,)), ((), ()))
BLOCK = 128
NEAR = 4
FIRST_AT, ROWS_AT, LAST_AT = 6, 3, 9
MESH = pl.DeviceIdType.MESH


def at(i):
    return slice(BLOCK * i, BLOCK * (i + 1))


PIECES = (((0, 1), slice(0, 256)), ((2,), slice(256, 384)), ((3,), slice(384, 512)))


def split(x):
    hi = x.astype(jnp.bfloat16)
    return hi, (x - hi.astype(F32)).astype(jnp.bfloat16)


def dot(a, b, dims=NT):
    left = jnp.concatenate([a[0], a[1], a[0]], 1)
    right = jnp.concatenate([b[0], b[0], b[1]], dims[0][1][0])
    return lax.dot_general(left, right, dims, preferred_element_type=F32)


def beside(parts, axis=1):
    return tuple(jnp.concatenate(x, axis) if len(x) > 1 else x[0] for x in zip(*parts))


def sub(v, k):
    return jnp.broadcast_to(v[k : k + 1, :], (8, 128))


class Block:
    def __init__(self, rows):
        self.ri = lax.broadcasted_iota(jnp.int32, (8, 128), 0)
        self.li = lax.broadcasted_iota(jnp.int32, (8, 128), 1)
        self.rows = rows
        self.upper, self.inverse = [], []

    def advance(self, p):
        ri, li, rows = self.ri, self.li, self.rows
        first = 8 * p
        raw = [jnp.broadcast_to(rows[:, :, first + j : first + j + 1], rows.shape) for j in range(8)]
        e = {(i, j): sub(raw[j][0], i) for j in range(8) for i in range(j, 8)}
        near = min(NEAR + 1, rows.shape[0])
        cols = [x[1:near] for x in raw]
        scales, factors = [], []
        r = [sub(rows[0], k) for k in range(8)]
        s = [jnp.where(li < first, r[k], jnp.where(li == first + k, 1.0, 0.0)) for k in range(8)]
        for k in range(8):
            inv = lax.rsqrt(e[k, k])
            m = {j: e[j, k] * inv for j in range(k + 1, 8)}
            for j in range(k + 1, 8):
                for i in range(j, 8):
                    e[i, j] = e[i, j] - m[i] * m[j]
            scales.append(inv)
            factors.append(m)
            if near > 1:
                cols[k] = cols[k] * inv
            r[k] = r[k] * inv
            s[k] = s[k] * inv
            for j in range(k + 1, 8):
                if near > 1:
                    cols[j] = cols[j] - cols[k] * m[j]
                r[j] = r[j] - m[j] * r[k]
                s[j] = s[j] - m[j] * s[k]
        u, t = r[0], s[0]
        for k in range(1, 8):
            u = jnp.where(ri == k, r[k], u)
            t = jnp.where(ri == k, s[k], t)
        self.upper.append(jnp.where(li >= ri + first, u, 0.0))
        self.inverse.append(t)
        if p < 15:
            rows = jnp.where(((li < first) | (li >= first + 8))[None], rows[1:], 0.0)
            both = [jnp.where(li < first + 8, s[k], r[k]) for k in range(8)]
            close, parts = rows[: near - 1], []
            for k in range(8):
                close = close - cols[k] * both[k]
            parts.append(close)
            if rows.shape[0] > near - 1:
                for k in range(7, -1, -1):
                    for j in range(k + 1, 8):
                        both[k] = both[k] - factors[k][j] * both[j]
                    both[k] = both[k] * scales[k]
                far = rows[near - 1 :]
                for k in range(8):
                    far = far - raw[k][near:] * both[k]
                parts.append(far)
            rows = jnp.concatenate(parts, 0) if len(parts) > 1 else close
            self.rows = rows


class Factor:
    def __init__(self, a, l):
        self.a, self.l = a, l
        self.lows, self.inv, self.inv_rows, self.below, self.sums = {}, {}, {}, {}, {}

    def low_row(self, i, n):
        return beside([self.lows[i, m] for m in range(n)])

    def column(self, k, i):
        value = self.a[at(i), at(k)]
        return value - dot(self.low_row(i, k), self.low_row(k, k)) if k else value

    def block(self, k, tasks=(), hooks=()):
        value = self.column(k, k)
        b = Block(value.reshape(16, 8, 128))
        stages = [(0, lambda: None, tasks), *hooks, (16, None, ())]
        for (start, wait, work), (end, _, _) in zip(stages, stages[1:]):
            wait()
            work = list(work)
            for p in range(start, end):
                b.advance(p)
                for _ in range(-(-len(work) // (end - p))):
                    work.pop(0)()
        self.inv[k] = split(jnp.concatenate(b.inverse, 0))
        if k == 0:
            self.inv_rows[0] = self.inv[0]
        self.l[at(k), at(k)] = jnp.concatenate(b.upper, 0).T
        for j in range(k + 1, 4):
            self.l[at(k), at(j)] = jnp.zeros((BLOCK, BLOCK), F32)

    def prepare(self, k, i):
        def task():
            self.below[i] = split(self.column(k, i))

        return task

    def rest(self, k):
        for i in range(k + 1, 4):
            if i not in self.below:
                self.prepare(k, i)()
            low = dot(self.below.pop(i), self.inv[k])
            self.l[at(i), at(k)] = low
            self.lows[i, k] = split(low)

    def inverse_rows(self, rows, width):
        parts = []
        for k in rows:
            fill = jnp.zeros((BLOCK, width - BLOCK * (k + 1)), jnp.bfloat16)
            parts.append(beside([self.inv_rows[k], (fill, fill)]) if fill.shape[1] else self.inv_rows[k])
        return beside(parts, 0)

    def inverse_sum(self, k):
        def task():
            total = dot(self.low_row(k, k), self.inverse_rows(range(k), BLOCK * k), NN)
            self.sums[k] = split(total)

        return task

    def inverse_row(self, k):
        def task():
            left = split(-dot(self.inv[k], self.sums.pop(k), NN))
            self.inv_rows[k] = beside([left, self.inv[k]])

        return task

    def solved(self, x, g):
        blocks = PIECES[g][0]
        return dot(beside(x[: g + 1]), self.inverse_rows(blocks, BLOCK * (blocks[-1] + 1)))


def remote(src, dst, send, recv, **device):
    return pltpu.make_async_remote_copy(
        src_ref=src, dst_ref=dst, send_sem=send, recv_sem=recv, device_id=device, device_id_type=MESH
    )


class Exchange:
    def __init__(self, diag, panel, own, dbuf, relay, rows, win, wsrc, wq, hq, pw, sems):
        self.diag, self.panel, self.own, self.dbuf, self.relay, self.rows = diag, panel, own, dbuf, relay, rows
        self.win, self.wsrc, self.wq, self.hq, self.pw = win, wsrc, wq, hq, pw
        (self.loc, self.ds, self.dr, self.cs, self.cr, self.rs, self.rr, self.zs, self.zr, self.xs, self.xr,
         self.w1s, self.w1r, self.w2s, self.w2r, self.w3s, self.w3r, self.w4s, self.w4r, self.w5s, self.w5r, self.w6s, self.w6r,
         self.as_, self.ar, self.bs, self.br, self.es, self.er) = sems
        self.r, self.c, self.s = (lax.axis_index(a) for a in ALL)
        self.corner = jnp.logical_and(self.r == 0, self.c == 0)

    def enter(self):
        r, c, s = self.r, self.c, self.s
        self.own_diag = pltpu.make_async_copy(self.diag, self.dbuf.at[r, c, s], self.loc.at[0])
        self.own_panel = pltpu.make_async_copy(self.panel, self.own, self.loc.at[1])
        self.own_diag.start()
        self.own_panel.start()
        barrier = pltpu.get_barrier_semaphore()
        for axis, me, n in (("depth", s, 8), ("col", c, 4), ("row", r, 4)):
            for t in range(1, n):
                pl.semaphore_signal(barrier, inc=1, device_id={axis: (me + t) % n}, device_id_type=MESH)
        pl.semaphore_wait(barrier, 13)
        self.own_diag.wait()

    def load_panel(self):
        self.own_panel.wait()
        n = self.own.shape[0]
        self.relay[self.c, 0:n] = self.own[...]
        self.relay[self.c, n:256] = jnp.zeros((256 - n, 512), F32)

    def diag_col(self, t, c):
        ref = self.dbuf.at[self.r, c, self.s]
        return remote(ref, ref, self.cs.at[t], self.cr.at[t], col=(self.c + t) % 4)

    def diag_col_send(self):
        for t in range(1, 4):
            self.diag_col(t, self.c).start()

    def diag_col_wait(self):
        for t in range(1, 4):
            self.diag_col(t, (self.c - t) % 4).wait_recv()

    def by_row(self, act):
        for i in range(4):

            @pl.when(self.r == i)
            def _():
                act(i)

    def diag_depth(self, t, s, i, part):
        cols = slice(0, 128) if part == 0 else slice(128, 128 * (i + 1))
        ref = self.dbuf.at[i, :, s, :, cols]
        return remote(ref, ref, self.ds.at[t, part], self.dr.at[t, part], depth=(self.s + t) % 8)

    def diag_depth_each(self, part, act, receive=False):
        def at_row(i):
            if i >= part:
                for t in range(1, 8):
                    act(self.diag_depth(t, (self.s - t) % 8 if receive else self.s, i, part))

        self.by_row(at_row)

    def diag_depth_send(self, part):
        self.diag_depth_each(part, lambda copy: copy.start())

    def diag_depth_wait(self, part):
        self.diag_depth_each(part, lambda copy: copy.wait_recv(), receive=True)

    def diag_row(self, t, i, b):
        ref = self.dbuf.at[i, :, :, :, at(b)]
        return remote(ref, ref, self.rs.at[t, b], self.rr.at[t, b], row=(self.r + t) % 4)

    def diag_row_each(self, b, act):
        def at_row(i):
            if i >= b:
                for t in range(1, 4):
                    act(self.diag_row(t, i, b))

        self.by_row(at_row)

    def diag_row_send(self, b):
        self.diag_row_each(b, lambda copy: copy.start())

    def diag_first_send(self, rows):
        for i in rows:

            @pl.when(self.r == i)
            def _():
                for t in range(1, 4):
                    self.diag_row(t, i, 0).start()

    def diag_row_wait(self, src, b):
        def at_row(i):
            if i != src:
                self.diag_row((i - src) % 4, src, b).wait_recv()

        self.by_row(at_row)

    def rows_col(self, t, slot, b):
        ref = self.relay.at[slot, :, at(b)]
        return remote(ref, ref, self.zs.at[t, b], self.zr.at[t, b], col=(self.c + t) % 4)

    def rows_far_half(self, t, slot, b):
        ref = self.relay.at[slot, at((t - 1) // 2), at(b)]
        return remote(ref, ref, self.zs.at[t - 1, b], self.zr.at[t - 1, b], col=(self.c + t) % 4)

    def rows_col_send(self, b):
        for t in (1, 3):
            self.rows_col(t, self.c, b).start()

    def rows_near(self, b):
        for t in (1, 3):
            slot = (self.c - t) % 4
            self.rows_col(t, slot, b).wait_recv()
            self.rows_far_half(t, slot, b).start()

    def rows_near_pass(self, b):
        for t in (1, 3):
            self.rows_depth_send(t, (self.c - t) % 4, b)

    def rows_far_pass(self, b):
        slot = (self.c + 2) % 4
        for t in (1, 3):
            self.rows_far_half(t, slot, b).wait_recv()
        self.rows_depth_send(2, slot, b)

    def rows_depth(self, t, slot, b):
        target, j = 2 * slot + self.s // 4, self.s % 4
        return target, remote(
            self.relay.at[slot, :, at(b)], self.rows.at[j, :, at(b)], self.xs.at[t, b], self.xr.at[j, b], depth=target
        )

    def rows_depth_send(self, t, slot, b):
        target, copy = self.rows_depth(t, slot, b)

        @pl.when(target != self.s)
        def _():
            copy.start()

        @pl.when(target == self.s)
        def _():
            self.rows[self.s % 4, :, at(b)] = self.relay[slot, :, at(b)]

    def rows_wait(self, b):
        for j in range(4):
            source = 4 * (self.s % 2) + j
            ref = self.rows.at[j, :, at(b)]

            @pl.when(source != self.s)
            def _():
                remote(ref, ref, self.xs.at[0, b], self.xr.at[j, b], depth=source).wait_recv()

    def quarter(self, a):
        return pl.ds(pl.multiple_of(64 * a, 64), 64), slice(256, 512)

    def half_col(self, t, slot, a):
        ref = self.relay.at[(slot, *self.quarter(a))]
        return remote(ref, ref, self.as_.at[t], self.ar.at[t], col=(self.c + t) % 4)

    def half_col_send(self):
        for t in (1, 3, 2):
            self.half_col(t, self.c, (self.c + t) % 4).start()

    def half_depth(self, t):
        slot = (self.c - t) % 4
        target, j, part = 2 * slot + self.s // 4, self.s % 4, self.quarter(self.c)
        return target, (slot, *part), (j, *part)

    def half_depth_copy(self, t):
        target, src, dst = self.half_depth(t)
        return remote(
            self.relay.at[src], self.rows.at[dst], self.bs.at[t], self.br.at[self.s % 4], depth=target
        )

    def half_depth_send(self):
        for t in range(4):
            if t:
                self.half_col(t, (self.c - t) % 4, self.c).wait_recv()
            target, src, dst = self.half_depth(t)

            @pl.when(target != self.s)
            def _():
                self.half_depth_copy(t).start()

            @pl.when(target == self.s)
            def _():
                self.rows[dst] = self.relay[src]

    def half_all(self, t, a):
        ref = self.rows.at[(slice(None), *self.quarter(a))]
        return remote(ref, ref, self.es.at[t], self.er.at[t], col=(self.c + t) % 4)

    def half_all_send(self):
        for j in range(4):
            source = 4 * (self.s % 2) + j
            ref = self.rows.at[(j, *self.quarter(self.c))]

            @pl.when(source != self.s)
            def _():
                remote(ref, ref, self.bs.at[0], self.br.at[j], depth=source).wait_recv()

        for t in (1, 3):
            self.half_all(t, self.c).start()

    def half_far_half(self, t, a):
        ref = self.rows.at[(slice(t - 1, t + 1), *self.quarter(a))]
        return remote(ref, ref, self.es.at[t - 1], self.er.at[t - 1], col=(self.c + t) % 4)

    def half_all_near(self):
        for t in (1, 3):
            a = (self.c - t) % 4
            self.half_all(t, a).wait_recv()
            self.half_far_half(t, a).start()

    def half_all_far(self):
        for t in (1, 3):
            self.half_far_half(t, (self.c + 2) % 4).wait_recv()

    def corner_case(self, rows, i, act):
        here = jnp.logical_and(self.c == 0, self.s == i)
        if rows is not None:
            here = jnp.logical_and(here, jnp.logical_and(self.r >= rows[0], self.r <= rows[-1]))

        @pl.when(here)
        def _():
            act()

    def win_main(self, i, t):
        n = 16 if t < 3 else 15 - i
        return remote(
            self.wsrc.at[i + 16 * t : i + 16 * t + n], self.wq.at[0:n], self.w1s.at[t], self.w1r.at[0], row=t
        )

    def win_head(self, i):
        return remote(self.wsrc.at[0:i], self.hq.at[0:i], self.w1s.at[4], self.w1r.at[1], row=3)

    def win_scatter(self, act):
        def copies(i):
            if i < 4:
                for t in range(1, 4):
                    act(self.win_main(i, t))
            if i > 0:
                act(self.win_head(i))

        for i in range(5):
            self.corner_case((0,), i, lambda: copies(i))

    def win_scatter_send(self):
        @pl.when(jnp.logical_and(self.corner, self.s < 5))
        def _():
            for u in range(63):
                self.wsrc[u] = self.relay[0, 4 * u : 4 * u + 4, :]

        self.win_scatter(lambda copy: copy.start())

    def win_scatter_wait(self):
        for i in range(5):
            if i < 4:
                self.corner_case((1, 2), i, lambda: self.win_main(i, 1).wait_recv())
                self.corner_case((3,), i, lambda: self.win_main(i, 3).wait_recv())
            if i > 0:
                self.corner_case((3,), i, lambda: self.win_head(i).wait_recv())

    def win_piece(self, rows, i, d):
        n = 2 if rows[0] < 3 else min(max(15 - i - 2 * d, 0), 2)
        if n == 0:
            return None
        src = self.wsrc.at[i + 2 * d : i + 2 * d + n] if rows[0] == 0 else self.wq.at[2 * d : 2 * d + n]
        dst = self.pw.at[i, 0:n]
        return src, dst, lambda: remote(src, dst, self.w2s.at[d], self.w2r.at[i], depth=d)

    def win_head_piece(self, c, d):
        first, last = max(0, 2 * d - 15 + c), min(c + 1, 2 * d - 13 + c)
        if d < 6 or first >= last:
            return None
        slot = (15 - c + first) % 2
        return remote(
            self.hq.at[first:last],
            self.pw.at[c, slot : slot + last - first],
            self.w2s.at[2 + d],
            self.w2r.at[4 + c],
            depth=d,
        )

    def win_spread(self, act, local=False):
        def copies(rows, i):
            for d in range(8):
                if i < 4:
                    piece = self.win_piece(rows, i, d)
                    if piece and d != i:
                        act(piece[2]())
                    elif piece and local:
                        piece[1][...] = piece[0][...]
                if i > 0 and rows[0] == 3:
                    copy = self.win_head_piece(i - 1, d)
                    if copy:
                        act(copy)

        for i in range(5):
            for rows in ((0,), (1, 2), (3,)):
                self.corner_case(rows, i, lambda: copies(rows, i))

    def win_spread_send(self):
        self.win_spread(lambda copy: copy.start(), local=True)

    def win_spread_wait(self):
        def waits(rows, d):
            for i in range(4):
                piece = self.win_piece(rows, i, d)
                if piece and d != i:
                    piece[2]().wait_recv()
                if rows[0] == 3:
                    copy = self.win_head_piece(i, d)
                    if copy:
                        copy.wait_recv()

        for d in range(8):
            for rows in ((0, 1, 2), (3,)):
                self.corner_case(rows, d, lambda: waits(rows, d))

    def win_col(self, t):
        return remote(self.pw.at[t], self.win_at(self.s), self.w3s.at[t], self.w3r.at[0], col=t)

    def win_col_send(self):
        @pl.when(self.c == 0)
        def _():
            for t in range(1, 4):
                self.win_col(t).start()
            self.win[self.s // 2, self.s % 2, self.r] = self.pw[0]

    def win_col_wait(self):
        @pl.when(self.c != 0)
        def _():
            self.win_col(1).wait_recv()

    def win_at(self, d):
        return self.win.at[d // 2, d % 2, self.r]

    def win_depth(self, t, d):
        ref = self.win_at(d)
        return remote(ref, ref, self.w4s.at[t], self.w4r.at[t], depth=(self.s + t) % 8)

    def win_depth_send(self):
        for t in (2, 4, 6):
            self.win_depth(t, self.s).start()

    def win_depth_wait(self):
        for t in (2, 4, 6):
            self.win_depth(t, (self.s - t) % 8).wait_recv()

    def win_all(self, t, row):
        ref = self.win.at[:, self.s % 2, row]
        return remote(ref, ref, self.w5s.at[t], self.w5r.at[t], row=(self.r + t) % 4)

    def win_all_send(self):
        for t in range(1, 4):
            self.win_all(t, self.r).start()

    def win_all_wait(self):
        for t in range(1, 4):
            self.win_all(t, (self.r - t) % 4).wait_recv()

    def win_pair(self, core):
        ref = self.win.at[:, core]
        return remote(ref, ref, self.w6s.at[0], self.w6r.at[0], depth=self.s + 1 - 2 * (self.s % 2))

    def win_pair_send(self):
        self.win_pair(self.s % 2).start()

    def win_pair_wait(self):
        self.win_pair(1 - self.s % 2).wait_recv()

    def leave_early(self):
        for t in (2, 4, 6):
            self.win_depth(t, self.s).wait_send()
        for part in range(2):
            self.diag_depth_each(part, lambda copy: copy.wait_send())
        for b in range(4):
            self.diag_row_each(b, lambda copy: copy.wait_send())
        for t in range(1, 4):
            self.diag_col(t, self.c).wait_send()
            self.half_col(t, self.c, (self.c + t) % 4).wait_send()
        for t in range(4):
            target = self.half_depth(t)[0]

            @pl.when(target != self.s)
            def _():
                self.half_depth_copy(t).wait_send()

        for b in range(2):
            for t in (1, 3):
                self.rows_col(t, self.c, b).wait_send()
                self.rows_far_half(t, (self.c - t) % 4, b).wait_send()
        self.win_scatter(lambda copy: copy.wait_send())
        self.win_spread(lambda copy: copy.wait_send())

        @pl.when(self.c == 0)
        def _():
            for t in range(1, 4):
                self.win_col(t).wait_send()

    def leave(self):
        self.win_pair(self.s % 2).wait_send()
        for t in range(1, 4):
            self.win_all(t, self.r).wait_send()
        for t in (1, 3):
            self.half_all(t, self.c).wait_send()
            self.half_far_half(t, (self.c - t) % 4).wait_send()
        for b in range(2):
            for t in range(4):
                target, copy = self.rows_depth(t, (self.c - t) % 4, b)

                @pl.when(target != self.s)
                def _():
                    copy.wait_send()


SEMAPHORES = ((3,), (8, 2), (8, 2), (4,), (4,), (4, 4), (4, 4), (4, 2), (4, 2), (4, 2), (4, 2),
              (5,), (2,), (10,), (8,), (4,), (1,), (8,), (8,), (4,), (4,), (1,), (1,),
              (4,), (4,), (4,), (4,), (4,), (4,))


def kernel(
    diag_in, panel, trailing_in, own_l, solved, updated,
    own, dbuf, relay, rows, win, wsrc, wq, hq, pw, diag, window, l, trailing, *sems,
):
    e = Exchange(diag_in, panel, own, dbuf, relay, rows, win, wsrc, wq, hq, pw, sems)
    f = Factor(diag, l)

    def assemble(i, b):
        e.diag_row_wait(i, b)
        for c in range(4):
            for s in range(8):
                first = 128 * i + 32 * c + 4 * s
                diag[first : first + 4, at(b)] = dbuf[i, c, s, :, at(b)]

    def assemble_column(b):
        for i in range(b, 4):
            if i > 0:
                assemble(i, b)

    own_trailing = pltpu.make_async_copy(trailing_in, trailing, sems[0].at[2])
    e.enter()
    e.diag_col_send()
    own_trailing.start()
    e.load_panel()
    e.half_col_send()
    e.rows_col_send(0)
    e.win_scatter_send()
    e.rows_col_send(1)
    e.diag_col_wait()
    e.diag_depth_send(0)
    e.diag_depth_send(1)
    e.half_depth_send()
    e.diag_depth_wait(0)
    e.diag_first_send((0,))
    e.win_scatter_wait()
    e.win_spread_send()
    e.diag_depth_wait(1)
    e.rows_depth_send(0, e.c, 0)
    e.rows_near(0)
    e.rows_near_pass(0)
    e.diag_first_send((1, 2, 3))
    e.diag_row_send(1)
    e.diag_row_send(2)
    e.diag_row_send(3)
    assemble(0, 0)
    e.win_spread_wait()
    e.win_col_send()
    e.rows_near(1)
    e.half_all_send()

    def first_hook():
        e.rows_far_pass(0)

    f.block(0, hooks=[(FIRST_AT, first_hook, ())])
    e.win_col_wait()
    e.win_depth_send()
    e.rows_depth_send(0, e.c, 1)
    e.rows_near_pass(1)
    assemble_column(0)
    f.rest(0)
    assemble_column(1)

    size = panel.shape[0]
    own_a, window_a, w, total = [], [], [], [None] * 4
    rows_a, rows_x = [[] for _ in range(4)], [[] for _ in range(4)]

    def own_task(g):
        def task():
            own_a.append(split(own[:, PIECES[g][1]]))
            solved[:, PIECES[g][1]] = f.solved(own_a, g)

        return task

    def row_load(j, g):
        return lambda: rows_a[j].append(split(rows[j, 0:size, PIECES[g][1]]))

    def row_task(j, g):
        return lambda: rows_x[j].append(split(f.solved(rows_a[j], g)))

    def window_load():
        for s in range(8):
            for r in range(4):
                for u in range(2):
                    first = 64 * r + 8 * s + 4 * u
                    window[first : first + 4, :] = win[s // 2, s % 2, r, u]
        for _, columns in PIECES:
            window_a.append(split(window[:, columns]))

    def window_task(g):
        return lambda: w.append(split(f.solved(window_a, g)))

    def product_task(j, g):
        def task():
            term = dot(rows_x[j][g], w[g])
            total[j] = term if total[j] is None else total[j] + term

        return task

    def second_hook():
        e.rows_far_pass(1)

    f.block(1, [f.prepare(1, 2), f.prepare(1, 3)], [(8, second_hook, ())])
    e.win_depth_wait()
    e.win_all_send()
    e.half_all_near()
    f.rest(1)
    assemble_column(2)
    f.block(2, [f.prepare(2, 3), f.inverse_sum(1), f.inverse_row(1), f.inverse_sum(2), own_task(0)])
    f.rest(2)
    assemble_column(3)


    def rows_hook():
        e.win_all_wait()
        e.win_pair_send()
        e.rows_wait(0)
        e.rows_wait(1)

    def last_hook():
        e.leave_early()
        e.half_all_far()
        e.win_pair_wait()

    f.block(
        3,
        [f.inverse_row(2), f.inverse_sum(3), own_task(1)],
        [
            (ROWS_AT, rows_hook, [t(j, 0) for j in range(4) for t in (row_load, row_task)]),
            (
                LAST_AT,
                last_hook,
                [window_load, window_task(0), window_task(1)]
                + [t(j, 1) for j in range(4) for t in (row_load, row_task)]
                + [product_task(j, g) for g in range(2) for j in range(4)]
                + [row_load(j, 2) for j in range(4)],
            ),
        ],
    )
    f.inverse_row(3)()
    window_task(2)()
    own_trailing.wait()
    for j in range(4):
        row_task(j, 2)()
        product_task(j, 2)()
        span = slice(size * j, size * (j + 1))
        updated[span, :] = trailing[span, :] - total[j]
    own_task(2)()
    position = (e.r * 4 + e.c) * 8 + e.s
    pair = l[pl.ds(pl.multiple_of((position // 2) * 8, 8), 8), :]
    own_l[...] = jnp.where(position % 2 == 0, pair[0:4], pair[4:8])
    e.leave()


def deliver(own_l, solved, updated, own_l_out, solved_out, updated_out, sem):
    rows = updated.shape[0]
    parts = [(own_l, own_l_out), (solved, solved_out)]
    for first in range(0, rows, 256):
        part = pl.ds(first, min(256, rows - first))
        parts.append((updated.at[part], updated_out.at[part]))
    copies = [pltpu.make_async_copy(src, dst, sem.at[i]) for i, (src, dst) in enumerate(parts)]
    for copy in copies:
        copy.start()
    for copy in copies:
        copy.wait()


def body(diag_block, panel_rows, trailing):
    vmem = pl.BlockSpec(memory_space=pltpu.VMEM)
    hbm = pl.BlockSpec(memory_space=pltpu.HBM)
    shapes = (
        panel_rows.shape,
        (4, 4, 8, 4, 512),
        (4, 256, 512),
        (4, 256, 512),
        (4, 2, 4, 2, 4, 512),
        (63, 4, 512),
        (16, 4, 512),
        (4, 4, 512),
        (4, 2, 4, 512),
        (512, 512),
        (256, 512),
        (512, 512),
        trailing.shape,
    )
    outs = tuple(jax.ShapeDtypeStruct(a.shape, F32) for a in (diag_block, panel_rows, trailing))
    results = pl.pallas_call(
        kernel,
        out_shape=outs,
        in_specs=[hbm] * 3,
        out_specs=(vmem,) * 3,
        scratch_shapes=[pltpu.VMEM(shape, F32) for shape in shapes]
        + [pltpu.SemaphoreType.DMA(n) for n in SEMAPHORES],
        compiler_params=pltpu.CompilerParams(
            collective_id=0, has_side_effects=True, vmem_limit_bytes=VMEM_LIMIT
        ),
        name="panel_step",
    )(*(pltpu.with_memory_space_constraint(x, pltpu.HBM) for x in (diag_block, panel_rows, trailing)))
    return pl.pallas_call(
        deliver,
        out_shape=outs,
        in_specs=[vmem] * 3,
        out_specs=(hbm,) * 3,
        scratch_shapes=[pltpu.SemaphoreType.DMA((6,))],
        compiler_params=pltpu.CompilerParams(vmem_limit_bytes=2 * 2**20),
        name="deliver",
    )(*results)


VMEM_LIMIT = 44 * 2**20


def solution(mesh):
    specs = (P(ALL, None), P(ALL, None), P(("row", "depth"), "col"))
    return jax.shard_map(body, mesh=mesh, in_specs=specs, out_specs=specs, check_vma=False)
```
